256 devices in a mesh: group: 2 (over y), temp: 4 (over x), gz: 32 (over z, core).
Axes of the slice: x: 4, y: 2, z: 16, core: 2. Of those that a mesh axis runs over, the one named last changes fastest.
The devices are a block of a 4x16x16 slice.
Arguments:
- spin_state: float32 [16, 3, 128, 128, 128], P(('group', 'temp'), None, 'gz'), parts along dimension 0, may hold values from -1 to 1, as said below
- couplings: float32 [3, 256, 128, 128], P(None, ('group', 'gz')), parts along dimension 1, may hold values from -12 to 12
- inverse_temps: float32 [16], P(('group', 'temp')), parts along dimension 0, may hold values from 0.3 to 3
- colour_order: int32 [16], P(('group', 'temp')), parts along dimension 0, may hold values 0 or 1
- heat_level: float32 [16, 128, 128, 128], P(('group', 'temp'), 'gz'), parts along dimension 0, may hold values from 0.001 to 0.999
- heat_height: float32 [16, 128, 128, 128], P(('group', 'temp'), 'gz'), parts along dimension 0, may hold values from -1 to 1
- heat_angle: float32 [16, 128, 128, 128], P(('group', 'temp'), 'gz'), parts along dimension 0, may hold values from -3.140625 to 3.140625
- swap_bits: int32 [16], P(('group', 'temp')), parts along dimension 0, may hold values 0 or 1
Outputs:
- spin_final: float32 [16, 3, 128, 128, 128], P(('group', 'temp'), None, 'gz'), parts along dimension 0
- energies: float32 [16], P(('group', 'temp')), parts along dimension 0
The draws below stay inside these ranges and needn't reach their ends.
There are 2 independent parts, one for each index of `group`. The reference program is written for one: setup_inputs(seed, part) draws one part's arguments, and reference() takes and returns one part's arrays. A program takes and returns all parts, laid end to end along the dimension named above; each array names one. Nothing has to cross between parts.
Inputs may be any that keep to these rules, and one draw needn't show every extreme that they name: `spin_state`: every site's three components form a vector of unit length.
All inputs are finite; a program needn't handle non-finite values. No bound on the sum of `colour_order` or of `swap_bits` on one device may be relied on, other than what follows from the above.
Results may differ from the reference program's by a relative error of at most 0.0003.
Values sent between devices are 32-bit elements; how exact they have to be, the bound alone decides.
A program may use at most 64 MiB of HBM per device.

```python
import math
import jax
import jax.numpy as jnp
from jax import lax

LX = 128
LY = 128
OR_SWEEPS = 2
REPLICAS = 8
NZ = 128


def draw_spin_state(key, part):
    first_key, second_key = jax.random.split(jax.random.fold_in(key, 11))
    array_shape = (REPLICAS, NZ, LY, LX)
    height = jax.random.uniform(first_key, array_shape, jnp.float32, -1.0, 1.0)
    azimuth = jax.random.uniform(second_key, array_shape, jnp.float32, -math.pi, math.pi)
    side = jnp.sqrt(jnp.maximum(1.0 - height * height, 0.0))
    return jnp.stack([side * jnp.cos(azimuth), side * jnp.sin(azimuth), height], axis=1)


def draw_couplings(key, part):
    first_key = jax.random.fold_in(key, 23)
    array_shape = (3, NZ, LY, LX)
    position = jnp.arange(NZ, dtype=jnp.float32) / max(NZ - 1, 1)
    values = jnp.clip(jax.random.normal(first_key, array_shape, jnp.float32), -4.0, 4.0)
    factor = 1.0 + 2.0 * position
    return values * factor[None, :, None, None]


def place_ends(array, rng, smallest, largest):
    longest = array.shape.index(max(array.shape))
    spots = []
    for shift in (0, 1):
        where = [jax.random.randint(jax.random.fold_in(rng, axis), (), 0, length) for axis, length in enumerate(array.shape)]
        where[longest] = (where[longest] + shift) % array.shape[longest]
        spots.append(tuple(where))
    return array.at[spots[0]].set(smallest).at[spots[1]].set(largest)


def steps_of(rng, dims, shards, low, largest):
    level = 1.0
    for dim, blocks in shards:
        draws = jax.random.uniform(jax.random.fold_in(jax.random.fold_in(rng, 6), dim), (blocks,), jnp.float32, low / len(shards), largest / len(shards))
        level = level * jnp.repeat(jnp.exp(draws), dims[dim] // blocks).reshape((-1,) + (1,) * (len(dims) - 1 - dim))
    return level


def setup_inputs(seed: int = 0, part: int = 0) -> dict:
    streams_of = jax.random.split(jax.random.key(seed), 9)
    part_splits = jax.random.split(jax.random.fold_in(streams_of[8], part), 9)
    return {
        "spin_state": draw_spin_state(jax.random.fold_in(jax.random.fold_in(streams_of[8], part), 71), part),
        "couplings": draw_couplings(jax.random.fold_in(jax.random.fold_in(streams_of[8], part), 71), part),
        "inverse_temps": jnp.clip(jnp.exp(math.log(3.0) - 2.3025851 * jax.random.uniform(part_splits[2], (REPLICAS,), jnp.float32) ** steps_of(part_splits[2], (REPLICAS,), ((0, 4),), -0.2, 0.2)), 0.3, 3.0),
        "colour_order": place_ends((jax.random.randint(part_splits[3], (REPLICAS,), 0, 2) < 1).astype(jnp.int32), jax.random.fold_in(part_splits[3], 1), 0, 1),
        "heat_level": jnp.clip(0.001 + 0.998 * jax.random.uniform(part_splits[4], (REPLICAS, NZ, LY, LX), jnp.float32) ** steps_of(part_splits[4], (REPLICAS, NZ, LY, LX), ((0, 4), (1, 32)), -0.2, 0.2), 0.001, 0.999),
        "heat_height": jnp.clip(jax.random.uniform(part_splits[5], (REPLICAS, NZ, LY, LX), jnp.float32, -1.0, 1.0) * steps_of(part_splits[5], (REPLICAS, NZ, LY, LX), ((0, 4), (1, 32)), -0.4, 0.0), -1.0, 1.0),
        "heat_angle": jnp.clip(jax.random.uniform(part_splits[6], (REPLICAS, NZ, LY, LX), jnp.float32, -3.140625, 3.140625), -3.140625, 3.140625),
        "swap_bits": place_ends((jax.random.randint(part_splits[7], (REPLICAS,), 0, 4) < 3).astype(jnp.int32), jax.random.fold_in(part_splits[7], 1), 0, 1),
    }


def neighbour_sum(current, bonds):
    east_bond, north_bond, upper_bond = (bonds[0], bonds[1], bonds[2])
    summed = east_bond * jnp.roll(current, -1, 3) + jnp.roll(east_bond, 1, 2) * jnp.roll(current, 1, 3)
    summed = summed + north_bond * jnp.roll(current, -1, 2) + jnp.roll(north_bond, 1, 1) * jnp.roll(current, 1, 2)
    summed = summed + upper_bond * jnp.roll(current, -1, 1) + jnp.roll(upper_bond, 1, 0) * jnp.roll(current, 1, 1)
    return summed

def reflect(current, pulled, component_axis):
    projection = lax.optimization_barrier(jnp.sum(current * pulled, axis=component_axis, keepdims=True))
    square = lax.optimization_barrier(jnp.sum(pulled * pulled, axis=component_axis, keepdims=True))
    return 2.0 * projection / jnp.maximum(square, 0.01) * pulled - current

def heat_bath(pulled, beta_value, uniform_level, cosine_draw, angle_draw, component_axis):
    square = lax.optimization_barrier(jnp.sum(pulled * pulled, axis=component_axis, keepdims=True))
    strength = jnp.sqrt(jnp.maximum(square, 0.01))
    unit_axis = pulled / strength
    reach = beta_value * strength
    cosine = 1.0 + jnp.log1p(uniform_level * jnp.expm1(-2.0 * reach)) / reach
    side = jnp.sqrt(jnp.maximum(1.0 - cosine_draw * cosine_draw, 0.0))
    proposal = jnp.concatenate([side * jnp.cos(angle_draw), side * jnp.sin(angle_draw), cosine_draw], axis=component_axis)
    along_axis = lax.optimization_barrier(jnp.sum(proposal * unit_axis, axis=component_axis, keepdims=True))
    tangent = proposal - along_axis * unit_axis
    tangent = tangent / jnp.sqrt(jnp.maximum(lax.optimization_barrier(jnp.sum(tangent * tangent, axis=component_axis, keepdims=True)), 0.0001))
    return cosine * unit_axis + jnp.sqrt(jnp.maximum(1.0 - cosine * cosine, 0.0)) * tangent

def pair_swap(stacked, decisions):
    flipped = stacked[:, ::-1]
    taking = (decisions != 0).reshape((-1,) + (1,) * (stacked.ndim - 1))
    return jnp.where(taking, flipped, stacked)

def reference(spin_state, couplings, inverse_temps, colour_order, heat_level, heat_height, heat_angle, swap_bits):
    plane_index = jnp.arange(NZ, dtype=jnp.int32)
    row_index = jnp.arange(LY, dtype=jnp.int32)
    column_index = jnp.arange(LX, dtype=jnp.int32)
    site_sum = plane_index[:, None, None] + row_index[None, :, None] + column_index[None, None, :]

    def one_replica(packed):
        current, beta_value, start_colour, uniform_level, cosine_draw, angle_draw = packed
        parity = (site_sum + start_colour) % 2
        colours = ((parity == 0)[None], (parity == 1)[None])
        for sweep_index in range(OR_SWEEPS):
            for chosen in colours:
                pulled = neighbour_sum(current, couplings)
                current = jnp.where(chosen, reflect(current, pulled, 0), current)
        for chosen in colours:
            pulled = neighbour_sum(current, couplings)
            renewed = heat_bath(pulled, beta_value, uniform_level[None], cosine_draw[None], angle_draw[None], 0)
            current = jnp.where(chosen, renewed, current)
        bond_sum = couplings[0] * jnp.roll(current, -1, 3) + couplings[1] * jnp.roll(current, -1, 2) + couplings[2] * jnp.roll(current, -1, 1)
        energy = -jnp.sum(current * bond_sum) / (LX * LY * NZ)
        return (current, energy)
    swept, energy_all = lax.map(one_replica, (spin_state, inverse_temps, colour_order, heat_level, heat_height, heat_angle))
    count = REPLICAS
    tail_shape = swept.shape[1:]
    swept = pair_swap(swept.reshape((count // 2, 2) + tail_shape), swap_bits[0::2]).reshape(swept.shape)
    energy_all = pair_swap(energy_all.reshape((count // 2, 2)), swap_bits[0::2]).reshape((count,))
    middle = pair_swap(swept[1:count - 1].reshape(((count - 2) // 2, 2) + tail_shape), swap_bits[1:count - 1:2])
    swept = jnp.concatenate([swept[:1], middle.reshape((count - 2,) + tail_shape), swept[count - 1:]], axis=0)
    middle_energy = pair_swap(energy_all[1:count - 1].reshape(((count - 2) // 2, 2)), swap_bits[1:count - 1:2])
    energy_all = jnp.concatenate([energy_all[:1], middle_energy.reshape((count - 2,)), energy_all[count - 1:]], axis=0)
    return (swept, energy_all)
```

```python
import functools

import jax
import jax.numpy as jnp
from jax import lax
from jax.experimental import pallas as pl
from jax.experimental.pallas import tpu as pltpu
from jax.sharding import PartitionSpec as P

OR_SWEEPS = 2
OR_HALVES = 2 * OR_SWEEPS
HALVES = OR_HALVES + 2
PAD = 8
MESH = pl.DeviceIdType.MESH

SIN_TERMS = (
    1.0,
    -1.0 / 6,
    1.0 / 120,
    -1.0 / 5040,
    1.0 / 362880,
    -1.0 / 39916800,
    1.0 / 6227020800,
)
COS_TERMS = (
    1.0,
    -1.0 / 2,
    1.0 / 24,
    -1.0 / 720,
    1.0 / 40320,
    -1.0 / 3628800,
    1.0 / 479001600,
    -1.0 / 87178291200,
)


def series(terms, square):
    total = jnp.full_like(square, terms[-1])
    for term in terms[-2::-1]:
        total = total * square + term
    return total


def cos_sin(angle):
    half = 0.5 * angle
    square = half * half
    sine = half * series(SIN_TERMS, square)
    cosine = series(COS_TERMS, square)
    return 1.0 - 2.0 * sine * sine, 2.0 * sine * cosine


def sweep_kernel(
    spin_hbm,
    bond_hbm,
    level_hbm,
    height_hbm,
    angle_hbm,
    beta_ref,
    order_ref,
    bits_ref,
    out_ref,
    energy_ref,
    spin_in,
    bond_in,
    heat_in,
    state,
    bond_x,
    bond_yo,
    bond_ys,
    bond_z,
    bond_halo,
    trial,
    load_sem,
    bond_send,
    bond_recv,
    send_sem,
    recv_sem,
):
    planes, rows, columns = spin_in.shape[2:]
    half = rows // 2
    chunk = min(16, half)
    me = lax.axis_index("gz")
    count = lax.axis_size("gz")
    upper = lax.rem(me + 1, count)
    lower = lax.rem(me + count - 1, count)
    main = pl.ds(PAD, half)

    loads = [
        pltpu.make_async_copy(spin_hbm, spin_in, load_sem.at[0]),
        pltpu.make_async_copy(bond_hbm, bond_in, load_sem.at[1]),
        pltpu.make_async_copy(level_hbm, heat_in.at[0], load_sem.at[2]),
        pltpu.make_async_copy(height_hbm, heat_in.at[1], load_sem.at[3]),
        pltpu.make_async_copy(angle_hbm, heat_in.at[2], load_sem.at[4]),
    ]
    for load in loads:
        load.start()

    barrier = pltpu.get_barrier_semaphore()
    for neighbour in (lower, upper):
        pl.semaphore_signal(
            barrier, inc=1, device_id={"gz": neighbour}, device_id_type=MESH
        )

    lane = lax.broadcasted_iota(jnp.int32, (half, columns), 1) % 2
    lane_chunk = lax.broadcasted_iota(jnp.int32, (chunk, columns), 1) % 2
    swapped = bits_ref[0] != 0

    def order_of(slot):
        other = 1 - slot
        return jnp.where(swapped, order_ref[other], order_ref[slot])

    def beta_of(slot):
        other = 1 - slot
        return jnp.where(swapped, beta_ref[other], beta_ref[slot])

    def parity(slot, plane):
        return lax.rem(me * planes + plane + order_of(slot), 2)

    def upward(step, slot):
        return pltpu.make_async_remote_copy(
            src_ref=state.at[step, slot, planes, :, main],
            dst_ref=state.at[step, slot, 0, :, main],
            send_sem=send_sem.at[step, slot, 0],
            recv_sem=recv_sem.at[step, slot, 0],
            device_id={"gz": upper},
            device_id_type=MESH,
        )

    def downward(step, slot):
        return pltpu.make_async_remote_copy(
            src_ref=state.at[step, slot, 1, :, main],
            dst_ref=state.at[step, slot, planes + 1, :, main],
            send_sem=send_sem.at[step, slot, 1],
            recv_sem=recv_sem.at[step, slot, 1],
            device_id={"gz": lower},
            device_id_type=MESH,
        )

    bond_up = pltpu.make_async_remote_copy(
        src_ref=bond_in.at[2, planes - 1],
        dst_ref=bond_halo,
        send_sem=bond_send,
        recv_sem=bond_recv,
        device_id={"gz": upper},
        device_id_type=MESH,
    )

    even_rows = pl.ds(0, half, stride=2)
    odd_rows = pl.ds(1, half, stride=2)

    def wrap_rows(step, slot, plane):
        for part in range(3):
            state[step, slot, plane, part, PAD - 1 : PAD] = state[
                step, slot, plane, part, PAD + half - 1 : PAD + half
            ]
            state[step, slot, plane, part, PAD + half : PAD + half + 1] = state[
                step, slot, plane, part, PAD : PAD + 1
            ]

    def pack_spins(plane, _):
        for part in range(3):
            pairs = [
                (spin_in[r, part, plane, even_rows, :], spin_in[r, part, plane, odd_rows, :])
                for r in (0, 1)
            ]
            for slot in (0, 1):
                even = jnp.where(swapped, pairs[1 - slot][0], pairs[slot][0])
                odd = jnp.where(swapped, pairs[1 - slot][1], pairs[slot][1])
                mask = lane == parity(slot, plane)
                state[0, slot, plane + 1, part, main] = jnp.where(mask, even, odd)
                state[1, slot, plane + 1, part, main] = jnp.where(mask, odd, even)
        for slot in (0, 1):
            wrap_rows(1, slot, plane + 1)
            wrap_rows(0, slot, plane + 1)
        return 0

    loads[0].wait()
    lax.fori_loop(0, planes, pack_spins, 0)
    loads[1].wait()

    pl.semaphore_wait(barrier, 2)
    for slot in (0, 1):
        upward(1, slot).start()
        downward(1, slot).start()
    bond_up.start()

    def pack_bonds(plane, _):
        even, odd = bond_in[0, plane, even_rows, :], bond_in[0, plane, odd_rows, :]
        first = jnp.where(lane == 0, even, odd)
        second = jnp.where(lane == 0, odd, even)
        bond_x[0, plane, 0] = first
        bond_x[1, plane, 0] = second
        bond_x[0, plane, 1] = pltpu.roll(second, 1, 1)
        bond_x[1, plane, 1] = pltpu.roll(first, 1, 1)
        even, odd = bond_in[1, plane, even_rows, :], bond_in[1, plane, odd_rows, :]
        before = pltpu.roll(odd, 1, 0)
        bond_ys[plane] = even
        bond_yo[0, plane] = jnp.where(lane == 0, before, odd)
        bond_yo[1, plane] = jnp.where(lane == 0, odd, before)
        even, odd = bond_in[2, plane, even_rows, :], bond_in[2, plane, odd_rows, :]
        bond_z[0, plane + 1] = jnp.where(lane == 0, even, odd)
        bond_z[1, plane + 1] = jnp.where(lane == 0, odd, even)
        return 0

    lax.fori_loop(0, planes, pack_bonds, 0)
    bond_up.wait_recv()
    even, odd = bond_halo[even_rows, :], bond_halo[odd_rows, :]
    bond_z[0, 0] = jnp.where(lane == 0, even, odd)
    bond_z[1, 0] = jnp.where(lane == 0, odd, even)

    for load in loads[2:]:
        load.wait()

    def pack_heat(slot, plane):
        side = 1 - slot
        mask = lane_chunk == parity(slot, plane)
        for start in range(0, half, chunk):
            here = pl.ds(start, chunk)
            even_here = pl.ds(2 * start, chunk, stride=2)
            odd_here = pl.ds(2 * start + 1, chunk, stride=2)
            draws = []
            for kind in range(3):
                even = jnp.where(
                    swapped,
                    heat_in[kind, side, plane, even_here, :],
                    heat_in[kind, slot, plane, even_here, :],
                )
                odd = jnp.where(
                    swapped,
                    heat_in[kind, side, plane, odd_here, :],
                    heat_in[kind, slot, plane, odd_here, :],
                )
                draws.append((jnp.where(mask, even, odd), jnp.where(mask, odd, even)))
            for colour in (0, 1):
                level, height, angle = (draw[colour] for draw in draws)
                across = jnp.sqrt(jnp.maximum(1.0 - height * height, 0.0))
                cosine, sine = cos_sin(angle)
                trial[slot, colour, plane, 0, here] = level
                trial[slot, colour, plane, 1, here] = across * cosine
                trial[slot, colour, plane, 2, here] = across * sine
                trial[slot, colour, plane, 3, here] = height

    def pulls(step, slot, plane, pattern, mask, start):
        here = pl.ds(start, chunk)
        east, west = bond_x[pattern, plane - 1, 0, here], bond_x[pattern, plane - 1, 1, here]
        near, far = bond_ys[plane - 1, here], bond_yo[pattern, plane - 1, here]
        above, below = bond_z[pattern, plane, here], bond_z[pattern, plane - 1, here]
        at = pl.ds(PAD + start, chunk)
        out = []
        for part in range(3):
            centre = state[step, slot, plane, part, at]
            other = jnp.where(
                mask,
                state[step, slot, plane, part, pl.ds(PAD + start - 1, chunk)],
                state[step, slot, plane, part, pl.ds(PAD + start + 1, chunk)],
            )
            pulled = east * pltpu.roll(centre, columns - 1, 1) + west * pltpu.roll(centre, 1, 1)
            pulled = pulled + near * centre + far * other
            pulled = pulled + above * state[step, slot, plane + 1, part, at]
            pulled = pulled + below * state[step, slot, plane - 1, part, at]
            out.append(pulled)
        return out

    def dot(first, second):
        return first[0] * second[0] + first[1] * second[1] + first[2] * second[2]

    def relax_plane(step, slot, plane):
        pattern = lax.rem(parity(slot, plane - 1) + step + 1, 2)
        mask = lane_chunk == pattern
        for start in range(0, half, chunk):
            at = pl.ds(PAD + start, chunk)
            pulled = pulls(step, slot, plane, pattern, mask, start)
            old = [state[step - 1, slot, plane, part, at] for part in range(3)]
            scale = 2.0 * dot(old, pulled) / jnp.maximum(dot(pulled, pulled), 0.01)
            for part in range(3):
                state[step + 1, slot, plane, part, at] = scale * pulled[part] - old[part]
        wrap_rows(step + 1, slot, plane)

    def heat_plane(step, slot, plane):
        colour = step - OR_HALVES - 1
        pattern = lax.rem(parity(slot, plane - 1) + step + 1, 2)
        mask = lane_chunk == pattern
        beta = beta_of(slot)
        gain = jnp.zeros((8, columns), jnp.float32)
        for start in range(0, half, chunk):
            at = pl.ds(PAD + start, chunk)
            here = pl.ds(start, chunk)
            pulled = pulls(step, slot, plane, pattern, mask, start)
            square = jnp.maximum(dot(pulled, pulled), 0.01)
            inverse = lax.rsqrt(square)
            reach = beta * (square * inverse)
            axis = [part * inverse for part in pulled]
            level = trial[slot, colour, plane - 1, 0, here]
            cosine = 1.0 + jnp.log((1.0 - level) + level * jnp.exp(-2.0 * reach)) / reach
            draw = [trial[slot, colour, plane - 1, part, here] for part in (1, 2, 3)]
            along = dot(draw, axis)
            tangent = [draw[part] - along * axis[part] for part in range(3)]
            norm = lax.rsqrt(jnp.maximum(dot(tangent, tangent), 0.0001))
            side = jnp.sqrt(jnp.maximum(1.0 - cosine * cosine, 0.0)) * norm
            fresh = [cosine * axis[part] + side * tangent[part] for part in range(3)]
            for part in range(3):
                state[step + 1, slot, plane, part, at] = fresh[part]
            gain = gain + jnp.sum(dot(fresh, pulled).reshape(-1, 8, columns), axis=0)
        wrap_rows(step + 1, slot, plane)
        return gain

    def boundary_first(index):
        return jnp.where(index == 0, 1, jnp.where(index == 1, planes, index))

    def halves(step, slot, body, send, initial):
        def visit(index, carry):
            plane = boundary_first(index)

            @pl.when(index == 0)
            def _():
                upward(step, slot).wait_recv()

            @pl.when(index == 1)
            def _():
                downward(step, slot).wait_recv()

            carry = body(step, slot, plane, carry)
            if send:

                @pl.when(index == 0)
                def _():
                    downward(step + 1, slot).start()

                @pl.when(index == 1)
                def _():
                    upward(step + 1, slot).start()

            return carry

        return lax.fori_loop(0, planes, visit, initial)

    def relax_body(step, slot, plane, carry):
        relax_plane(step, slot, plane)
        return carry

    def heat_body(step, slot, plane, carry):
        return carry + heat_plane(step, slot, plane)

    def relax_round(visit, _):
        step = visit // 2 + 1
        slot = lax.rem(visit, 2)
        halves(step, slot, relax_body, True, 0)
        share = planes // OR_HALVES

        def fill(index, _):
            pack_heat_dynamic(slot, (step - 1) * share + index)
            return 0

        lax.fori_loop(0, share, fill, 0)
        return 0

    def pack_heat_dynamic(slot, plane):
        pack_heat(slot, plane)

    lax.fori_loop(0, 2 * OR_HALVES, relax_round, 0)

    for step in (OR_HALVES + 1, OR_HALVES + 2):
        last = step == OR_HALVES + 2

        def heat_round(slot, _, step=step, last=last):
            zero = jnp.zeros((8, columns), jnp.float32)
            gain = halves(step, slot, heat_body, not last, zero)
            if last:
                energy_ref[slot] = gain
            return 0

        lax.fori_loop(0, 2, heat_round, 0)

    def unpack(plane, _):
        for slot in (0, 1):
            mask = lane == parity(slot, plane)
            for part in range(3):
                first = state[HALVES, slot, plane + 1, part, main]
                second = state[HALVES + 1, slot, plane + 1, part, main]
                out_ref[slot, part, plane, even_rows, :] = jnp.where(mask, first, second)
                out_ref[slot, part, plane, odd_rows, :] = jnp.where(mask, second, first)
        return 0

    lax.fori_loop(0, planes, unpack, 0)

    bond_up.wait_send()

    def drain(index, _):
        step = index // 2 + 1
        slot = lax.rem(index, 2)
        upward(step, slot).wait_send()
        downward(step, slot).wait_send()
        return 0

    lax.fori_loop(0, 2 * HALVES, drain, 0)


def sweep(spin_state, couplings, level, height, angle, beta, order, bits):
    slots, parts, planes, rows, columns = spin_state.shape
    half = rows // 2
    f32 = jnp.float32
    any_space = pl.BlockSpec(memory_space=pl.ANY)
    smem = pl.BlockSpec(memory_space=pltpu.SMEM)
    vmem = pl.BlockSpec(memory_space=pltpu.VMEM)
    return pl.pallas_call(
        sweep_kernel,
        out_shape=(
            jax.ShapeDtypeStruct(spin_state.shape, f32),
            jax.ShapeDtypeStruct((slots, 8, columns), f32),
        ),
        in_specs=[any_space] * 5 + [smem] * 3,
        out_specs=(vmem, vmem),
        scratch_shapes=[
            pltpu.VMEM(spin_state.shape, f32),
            pltpu.VMEM(couplings.shape, f32),
            pltpu.VMEM((3,) + level.shape, f32),
            pltpu.VMEM((HALVES + 2, slots, planes + 2, 3, half + 2 * PAD, columns), f32),
            pltpu.VMEM((2, planes, 2, half, columns), f32),
            pltpu.VMEM((2, planes, half, columns), f32),
            pltpu.VMEM((planes, half, columns), f32),
            pltpu.VMEM((2, planes + 1, half, columns), f32),
            pltpu.VMEM((rows, columns), f32),
            pltpu.VMEM((slots, 2, planes, 4, half, columns), f32),
            pltpu.SemaphoreType.DMA((5,)),
            pltpu.SemaphoreType.DMA,
            pltpu.SemaphoreType.DMA,
            pltpu.SemaphoreType.DMA((HALVES + 1, slots, 2)),
            pltpu.SemaphoreType.DMA((HALVES + 1, slots, 2)),
        ],
        compiler_params=pltpu.CompilerParams(
            collective_id=0, has_side_effects=True, vmem_limit_bytes=56 * 1024 * 1024
        ),
        name="sweep",
    )(spin_state, couplings, level, height, angle, beta, order, bits)


def copy_for_each(array, axis):
    copies = jnp.broadcast_to(array, (lax.axis_size(axis), *array.shape))
    return lax.all_to_all(copies, axis, split_axis=0, concat_axis=0, tiled=True)


def of_everyone(array, axis):
    return jnp.sum(copy_for_each(array, axis), axis=0)


def shifted(block, axis, distance):
    devices = range(lax.axis_size(axis))
    route = [(i - distance, i) for i in devices if i - distance in devices]
    return lax.ppermute(block, axis, route)


def on_device(
    spin_state,
    couplings,
    inverse_temps,
    colour_order,
    heat_level,
    heat_height,
    heat_angle,
    swap_bits,
):
    planes, rows, columns = spin_state.shape[2:]
    spin_now, gains = sweep(
        spin_state,
        couplings,
        heat_level,
        heat_height,
        heat_angle,
        inverse_temps,
        colour_order,
        swap_bits,
    )
    total_sites = float(columns * rows * planes * lax.axis_size("gz"))
    energy_now = of_everyone(-jnp.sum(gains, axis=(1, 2)), "gz") / total_sites
    below_spin, below_energy, below_bit = shifted(
        (spin_now[1:], energy_now[1:], swap_bits[1:].astype(jnp.float32)), "temp", 1
    )
    above_spin, above_energy = shifted((spin_now[:1], energy_now[:1]), "temp", -1)
    top_device = lax.axis_index("temp") == lax.axis_size("temp") - 1
    take_below = below_bit[0] > 0.5
    take_above = (swap_bits[1] != 0) & ~top_device
    spin_final = jnp.concatenate(
        [
            jnp.where(take_below, below_spin, spin_now[:1]),
            jnp.where(take_above, above_spin, spin_now[1:]),
        ]
    )
    energies = jnp.concatenate(
        [
            jnp.where(take_below, below_energy, energy_now[:1]),
            jnp.where(take_above, above_energy, energy_now[1:]),
        ]
    )
    return (spin_final, energies)


def solution(mesh):
    return jax.shard_map(
        on_device,
        mesh=mesh,
        in_specs=(
            P(("group", "temp"), None, "gz", None, None),
            P(None, ("group", "gz"), None, None),
            P(("group", "temp")),
            P(("group", "temp")),
            P(("group", "temp"), "gz", None, None),
            P(("group", "temp"), "gz", None, None),
            P(("group", "temp"), "gz", None, None),
            P(("group", "temp")),
        ),
        out_specs=(P(("group", "temp"), None, "gz", None, None), P(("group", "temp"))),
        check_vma=False,
    )
```

```python
import functools

import jax
import jax.numpy as jnp
from jax import lax
from jax.experimental import pallas as pl
from jax.experimental.pallas import tpu as pltpu
from jax.sharding import PartitionSpec as P

OR_SWEEPS = 2
OR_HALVES = 2 * OR_SWEEPS
HALVES = OR_HALVES + 2
PAD = 8
MESH = pl.DeviceIdType.MESH

SIN_TERMS = (
    1.0,
    -1.0 / 6,
    1.0 / 120,
    -1.0 / 5040,
    1.0 / 362880,
    -1.0 / 39916800,
    1.0 / 6227020800,
)
COS_TERMS = (
    1.0,
    -1.0 / 2,
    1.0 / 24,
    -1.0 / 720,
    1.0 / 40320,
    -1.0 / 3628800,
    1.0 / 479001600,
    -1.0 / 87178291200,
)


def series(terms, square):
    total = jnp.full_like(square, terms[-1])
    for term in terms[-2::-1]:
        total = total * square + term
    return total


def cos_sin(angle):
    half = 0.5 * angle
    square = half * half
    sine = half * series(SIN_TERMS, square)
    cosine = series(COS_TERMS, square)
    return 1.0 - 2.0 * sine * sine, 2.0 * sine * cosine


def far_distances(count):
    distances, known = [], 2
    while known < count // 2:
        distances.append(known)
        known *= 2
    return distances


def step_kernel(
    spin_hbm,
    bond_hbm,
    level_hbm,
    height_hbm,
    angle_hbm,
    beta_ref,
    order_ref,
    bits_ref,
    out_ref,
    energy_ref,
    spin_in,
    bond_in,
    heat_in,
    state,
    bond_x,
    bond_yo,
    bond_ys,
    bond_z,
    bond_halo,
    trial,
    meta,
    meta_got,
    draws,
    draws_got,
    trial_got,
    share_sum,
    share_got,
    total_sum,
    total_got,
    load_sem,
    bond_send,
    bond_recv,
    send_sem,
    recv_sem,
    meta_send,
    meta_recv,
    draw_send,
    draw_recv,
    swap_send,
    swap_recv,
    share_send,
    share_recv,
    total_send,
    total_recv,
    far_sem,
):
    planes, rows, columns = spin_in.shape[2:]
    half = rows // 2
    chunk = min(16, half)
    me = lax.axis_index("gz")
    count = lax.axis_size("gz")
    upper = lax.rem(me + 1, count)
    lower = lax.rem(me + count - 1, count)
    here_temp = lax.axis_index("temp")
    temps = lax.axis_size("temp")
    main = pl.ds(PAD, half)
    got = HALVES + 2
    distances = far_distances(count)

    loads = [
        pltpu.make_async_copy(spin_hbm, spin_in, load_sem.at[0]),
        pltpu.make_async_copy(bond_hbm, bond_in, load_sem.at[1]),
        pltpu.make_async_copy(level_hbm, heat_in.at[0], load_sem.at[2]),
        pltpu.make_async_copy(height_hbm, heat_in.at[1], load_sem.at[3]),
        pltpu.make_async_copy(angle_hbm, heat_in.at[2], load_sem.at[4]),
    ]
    for load in loads:
        load.start()

    def temp_towards(slot):
        return lax.rem(here_temp + 2 * slot - 1 + temps, temps)

    barrier = pltpu.get_barrier_semaphore()
    for neighbour in (lower, upper):
        pl.semaphore_signal(
            barrier, inc=1, device_id={"gz": neighbour}, device_id_type=MESH
        )
    for slot in (0, 1):
        pl.semaphore_signal(
            barrier, inc=1, device_id={"temp": temp_towards(slot)}, device_id_type=MESH
        )

    lane = lax.broadcasted_iota(jnp.int32, (half, columns), 1) % 2
    lane_chunk = lax.broadcasted_iota(jnp.int32, (chunk, columns), 1) % 2
    swapped = bits_ref[0] != 0

    def order_of(slot):
        other = 1 - slot
        return jnp.where(swapped, order_ref[other], order_ref[slot])

    def beta_of(slot):
        other = 1 - slot
        return jnp.where(swapped, beta_ref[other], beta_ref[slot])

    def parity(slot, plane):
        return lax.rem(me * planes + plane + order_of(slot), 2)

    for slot in (0, 1):
        meta[slot, 0:1] = jnp.full((1, columns), beta_of(slot), jnp.float32)
        meta[slot, 1:2] = jnp.full((1, columns), order_of(slot), jnp.int32).astype(jnp.float32)
        meta[slot, 2:3] = jnp.full((1, columns), bits_ref[1], jnp.int32).astype(jnp.float32)

    def upward(step, slot):
        return pltpu.make_async_remote_copy(
            src_ref=state.at[step, slot, planes, :, main],
            dst_ref=state.at[step, slot, 0, :, main],
            send_sem=send_sem.at[step, slot, 0],
            recv_sem=recv_sem.at[step, slot, 0],
            device_id={"gz": upper},
            device_id_type=MESH,
        )

    def downward(step, slot):
        return pltpu.make_async_remote_copy(
            src_ref=state.at[step, slot, 1, :, main],
            dst_ref=state.at[step, slot, planes + 1, :, main],
            send_sem=send_sem.at[step, slot, 1],
            recv_sem=recv_sem.at[step, slot, 1],
            device_id={"gz": lower},
            device_id_type=MESH,
        )

    bond_up = pltpu.make_async_remote_copy(
        src_ref=bond_in.at[2, planes - 1],
        dst_ref=bond_halo,
        send_sem=bond_send,
        recv_sem=bond_recv,
        device_id={"gz": upper},
        device_id_type=MESH,
    )

    def along_temp(source, target, send, recv, slot):
        return pltpu.make_async_remote_copy(
            src_ref=source,
            dst_ref=target,
            send_sem=send,
            recv_sem=recv,
            device_id={"temp": temp_towards(slot)},
            device_id_type=MESH,
        )

    def meta_copy(slot):
        return along_temp(
            meta.at[slot], meta_got.at[1 - slot], meta_send.at[slot], meta_recv.at[1 - slot], slot
        )

    def draw_copy(slot, plane):
        return along_temp(
            draws.at[slot, plane],
            draws_got.at[1 - slot, plane],
            draw_send.at[slot, plane],
            draw_recv.at[1 - slot, plane],
            slot,
        )

    def swap_copy(slot, plane):
        return along_temp(
            state.at[HALVES, slot, plane, :, main],
            state.at[got, 1 - slot, plane, :, main],
            swap_send.at[slot, plane],
            swap_recv.at[1 - slot, plane],
            slot,
        )

    def total_copy(slot):
        return along_temp(
            total_sum, total_got.at[1 - slot], total_send.at[slot], total_recv.at[1 - slot], slot
        )

    def share_copy(distance):
        return pltpu.make_async_remote_copy(
            src_ref=share_sum,
            dst_ref=share_got.at[distance - 1],
            send_sem=share_send.at[distance - 1],
            recv_sem=share_recv.at[distance - 1],
            device_id={"gz": lax.rem(me + distance, count)},
            device_id_type=MESH,
        )

    def far_signal(index):
        if index < len(distances):
            for move in (distances[index], count - distances[index]):
                pl.semaphore_signal(
                    far_sem.at[index],
                    inc=1,
                    device_id={"gz": lax.rem(me + move, count)},
                    device_id_type=MESH,
                )

    def far_wait(index):
        if index < len(distances):
            pl.semaphore_wait(far_sem.at[index], 2)

    even_rows = pl.ds(0, half, stride=2)
    odd_rows = pl.ds(1, half, stride=2)

    def wrap_rows(step, slot, plane):
        for part in range(3):
            state[step, slot, plane, part, PAD - 1 : PAD] = state[
                step, slot, plane, part, PAD + half - 1 : PAD + half
            ]
            state[step, slot, plane, part, PAD + half : PAD + half + 1] = state[
                step, slot, plane, part, PAD : PAD + 1
            ]

    def pack_spins(plane, _):
        for part in range(3):
            pairs = [
                (spin_in[r, part, plane, even_rows, :], spin_in[r, part, plane, odd_rows, :])
                for r in (0, 1)
            ]
            for slot in (0, 1):
                even = jnp.where(swapped, pairs[1 - slot][0], pairs[slot][0])
                odd = jnp.where(swapped, pairs[1 - slot][1], pairs[slot][1])
                mask = lane == parity(slot, plane)
                state[0, slot, plane + 1, part, main] = jnp.where(mask, even, odd)
                state[1, slot, plane + 1, part, main] = jnp.where(mask, odd, even)
        for slot in (0, 1):
            wrap_rows(1, slot, plane + 1)
            wrap_rows(0, slot, plane + 1)
        return 0

    loads[0].wait()
    lax.fori_loop(0, planes, pack_spins, 0)
    loads[1].wait()

    pl.semaphore_wait(barrier, 4)
    for slot in (0, 1):
        upward(1, slot).start()
        downward(1, slot).start()
    bond_up.start()
    for slot in (0, 1):
        meta_copy(slot).start()

    def pack_bonds(plane, _):
        even, odd = bond_in[0, plane, even_rows, :], bond_in[0, plane, odd_rows, :]
        first = jnp.where(lane == 0, even, odd)
        second = jnp.where(lane == 0, odd, even)
        bond_x[0, plane, 0] = first
        bond_x[1, plane, 0] = second
        bond_x[0, plane, 1] = pltpu.roll(second, 1, 1)
        bond_x[1, plane, 1] = pltpu.roll(first, 1, 1)
        even, odd = bond_in[1, plane, even_rows, :], bond_in[1, plane, odd_rows, :]
        before = pltpu.roll(odd, 1, 0)
        bond_ys[plane] = even
        bond_yo[0, plane] = jnp.where(lane == 0, before, odd)
        bond_yo[1, plane] = jnp.where(lane == 0, odd, before)
        even, odd = bond_in[2, plane, even_rows, :], bond_in[2, plane, odd_rows, :]
        bond_z[0, plane + 1] = jnp.where(lane == 0, even, odd)
        bond_z[1, plane + 1] = jnp.where(lane == 0, odd, even)
        return 0

    lax.fori_loop(0, planes, pack_bonds, 0)
    bond_up.wait_recv()
    even, odd = bond_halo[even_rows, :], bond_halo[odd_rows, :]
    bond_z[0, 0] = jnp.where(lane == 0, even, odd)
    bond_z[1, 0] = jnp.where(lane == 0, odd, even)

    for load in loads[2:]:
        load.wait()

    def pack_heat(slot, plane):
        side = 1 - slot
        mask = lane_chunk == parity(slot, plane)
        for start in range(0, half, chunk):
            here = pl.ds(start, chunk)
            even_here = pl.ds(2 * start, chunk, stride=2)
            odd_here = pl.ds(2 * start + 1, chunk, stride=2)
            packed = []
            for kind in range(3):
                even = jnp.where(
                    swapped,
                    heat_in[kind, side, plane, even_here, :],
                    heat_in[kind, slot, plane, even_here, :],
                )
                odd = jnp.where(
                    swapped,
                    heat_in[kind, side, plane, odd_here, :],
                    heat_in[kind, slot, plane, odd_here, :],
                )
                packed.append((jnp.where(mask, even, odd), jnp.where(mask, odd, even)))
                draws[slot, plane, kind, here] = packed[kind][1]
            for colour in (0, 1):
                level, height, angle = (draw[colour] for draw in packed)
                across = jnp.sqrt(jnp.maximum(1.0 - height * height, 0.0))
                cosine, sine = cos_sin(angle)
                trial[slot, colour, plane, 0, here] = level
                trial[slot, colour, plane, 1, here] = across * cosine
                trial[slot, colour, plane, 2, here] = across * sine
                trial[slot, colour, plane, 3, here] = height

    def bonds_of(pattern, plane, start):
        here = pl.ds(start, chunk)
        return (
            bond_x[pattern, plane - 1, 0, here],
            bond_x[pattern, plane - 1, 1, here],
            bond_ys[plane - 1, here],
            bond_yo[pattern, plane - 1, here],
            bond_z[pattern, plane, here],
            bond_z[pattern, plane - 1, here],
        )

    def pulls(step, slot, plane, bonds, mask, start):
        east, west, near, far, above, below = bonds
        at = pl.ds(PAD + start, chunk)
        out = []
        for part in range(3):
            centre = state[step, slot, plane, part, at]
            other = jnp.where(
                mask,
                state[step, slot, plane, part, pl.ds(PAD + start - 1, chunk)],
                state[step, slot, plane, part, pl.ds(PAD + start + 1, chunk)],
            )
            pulled = east * pltpu.roll(centre, columns - 1, 1) + west * pltpu.roll(centre, 1, 1)
            pulled = pulled + near * centre + far * other
            pulled = pulled + above * state[step, slot, plane + 1, part, at]
            pulled = pulled + below * state[step, slot, plane - 1, part, at]
            out.append(pulled)
        return out

    def dot(first, second):
        return first[0] * second[0] + first[1] * second[1] + first[2] * second[2]

    def relax_plane(step, slot, plane):
        pattern = lax.rem(parity(slot, plane - 1) + step + 1, 2)
        mask = lane_chunk == pattern
        for start in range(0, half, chunk):
            at = pl.ds(PAD + start, chunk)
            pulled = pulls(step, slot, plane, bonds_of(pattern, plane, start), mask, start)
            old = [state[step - 1, slot, plane, part, at] for part in range(3)]
            scale = 2.0 * dot(old, pulled) / jnp.maximum(dot(pulled, pulled), 0.01)
            for part in range(3):
                state[step + 1, slot, plane, part, at] = scale * pulled[part] - old[part]
        wrap_rows(step + 1, slot, plane)

    def heated(pulled, beta, level, draw):
        square = jnp.maximum(dot(pulled, pulled), 0.01)
        inverse = lax.rsqrt(square)
        reach = beta * (square * inverse)
        axis = [part * inverse for part in pulled]
        cosine = 1.0 + jnp.log((1.0 - level) + level * jnp.exp(-2.0 * reach)) / reach
        along = dot(draw, axis)
        tangent = [draw[part] - along * axis[part] for part in range(3)]
        norm = lax.rsqrt(jnp.maximum(dot(tangent, tangent), 0.0001))
        side = jnp.sqrt(jnp.maximum(1.0 - cosine * cosine, 0.0)) * norm
        return [cosine * axis[part] + side * tangent[part] for part in range(3)]

    def heat_plane(step, slot, plane):
        colour = step - OR_HALVES - 1
        pattern = lax.rem(parity(slot, plane - 1) + step + 1, 2)
        mask = lane_chunk == pattern
        beta = beta_of(slot)
        gain = jnp.zeros((8, columns), jnp.float32)
        for start in range(0, half, chunk):
            at = pl.ds(PAD + start, chunk)
            here = pl.ds(start, chunk)
            pulled = pulls(step, slot, plane, bonds_of(pattern, plane, start), mask, start)
            level = trial[slot, colour, plane - 1, 0, here]
            draw = [trial[slot, colour, plane - 1, part, here] for part in (1, 2, 3)]
            fresh = heated(pulled, beta, level, draw)
            for part in range(3):
                state[step + 1, slot, plane, part, at] = fresh[part]
            gain = gain + jnp.sum(dot(fresh, pulled).reshape(-1, 8, columns), axis=0)
        wrap_rows(step + 1, slot, plane)
        return gain

    def halves(step, slot, body, initial, send=True, swap=False):
        def visit(index, carry):
            outer = index < 2
            low = outer & (lax.rem(index + me, 2) == 0)
            high = outer & (lax.rem(index + me, 2) == 1)
            plane = jnp.where(low, 1, jnp.where(high, planes, index))

            @pl.when(low)
            def _():
                upward(step, slot).wait_recv()

            @pl.when(high)
            def _():
                downward(step, slot).wait_recv()

            carry = body(step, slot, plane, carry)
            if send:

                @pl.when(low)
                def _():
                    downward(step + 1, slot).start()

                @pl.when(high)
                def _():
                    upward(step + 1, slot).start()

            if swap:
                swap_copy(slot, plane).start()
            return carry

        return lax.fori_loop(0, planes, visit, initial)

    def relax_body(step, slot, plane, carry):
        relax_plane(step, slot, plane)
        return carry

    def heat_body(step, slot, plane, carry):
        return carry + heat_plane(step, slot, plane)

    share = planes // OR_HALVES

    def relax_round(visit, _):
        step = visit // 2 + 1
        slot = lax.rem(visit, 2)
        halves(step, slot, relax_body, 0)

        def fill(index, _):
            plane = (step - 1) * share + index
            pack_heat(slot, plane)
            draw_copy(slot, plane).start()
            return 0

        lax.fori_loop(0, share, fill, 0)

        @pl.when(visit == 1)
        def _():
            far_signal(0)

        return 0

    lax.fori_loop(0, 2 * OR_HALVES, relax_round, 0)
    far_wait(0)
    far_signal(1)

    zero = jnp.zeros((8, columns), jnp.float32)

    def first_heat(slot, _):
        halves(OR_HALVES + 1, slot, heat_body, zero, swap=True)
        return 0

    lax.fori_loop(0, 2, first_heat, 0)
    far_wait(1)
    far_signal(2)

    def second_heat(slot, _):
        gain = halves(OR_HALVES + 2, slot, heat_body, zero, send=False)
        share_sum[pl.ds(slot, 1), :] = jnp.sum(gain, axis=0, keepdims=True)
        return 0

    lax.fori_loop(0, 2, second_heat, 0)
    far_wait(2)

    def give_share(distance, _):
        share_copy(distance).start()
        return 0

    lax.fori_loop(1, count, give_share, 0)

    def pass_on(slot, _):
        swap_copy(1 - slot, 1).wait_recv()
        downward(got, slot).start()
        swap_copy(1 - slot, planes).wait_recv()
        upward(got, slot).start()
        return 0

    lax.fori_loop(0, 2, pass_on, 0)

    def prepare(visit, _):
        slot = visit // planes
        plane = lax.rem(visit, planes)
        draw_copy(1 - slot, plane).wait_recv()
        for start in range(0, half, chunk):
            here = pl.ds(start, chunk)
            level, height, angle = (draws_got[slot, plane, kind, here] for kind in range(3))
            across = jnp.sqrt(jnp.maximum(1.0 - height * height, 0.0))
            cosine, sine = cos_sin(angle)
            trial_got[slot, plane, 0, here] = level
            trial_got[slot, plane, 1, here] = across * cosine
            trial_got[slot, plane, 2, here] = across * sine
            trial_got[slot, plane, 3, here] = height
        return 0

    lax.fori_loop(0, 2 * planes, prepare, 0)

    def take_share(distance, sums):
        share_copy(distance).wait_recv()
        return sums + share_got[distance - 1]

    total_sum[...] = lax.fori_loop(1, count, take_share, share_sum[...])
    for slot in (0, 1):
        total_copy(slot).start()
        meta_copy(1 - slot).wait_recv()

    taking = [
        (meta_got[0, 2:3] > 0.5) & (here_temp > 0),
        jnp.full((1, columns), bits_ref[1], jnp.int32) * jnp.where(here_temp < temps - 1, 1, 0) > 0,
    ]

    def finish_plane(slot, plane):
        take = jnp.broadcast_to(taking[slot], (chunk, columns))
        flip = jnp.broadcast_to(meta_got[slot, 1:2] > 0.5, (chunk, columns))
        beta = meta_got[slot, 0:1]
        base = lax.rem(me * planes + plane - 1, 2)
        first_mask = (lane_chunk == base) ^ flip
        own_mask = lane_chunk == parity(slot, plane - 1)
        unpack_mask = jnp.where(take, first_mask.astype(jnp.int32), own_mask.astype(jnp.int32)) > 0
        for start in range(0, half, chunk):
            at = pl.ds(PAD + start, chunk)
            here = pl.ds(start, chunk)
            plain = bonds_of(1 - base, plane, start)
            other = bonds_of(base, plane, start)
            bonds = [jnp.where(flip, b, a) for a, b in zip(plain, other)]
            pulled = pulls(got, slot, plane, bonds, ~first_mask, start)
            level = trial_got[slot, plane - 1, 0, here]
            draw = [trial_got[slot, plane - 1, part, here] for part in (1, 2, 3)]
            fresh = heated(pulled, beta, level, draw)
            for part in range(3):
                first = jnp.where(
                    take, state[got, slot, plane, part, at], state[HALVES, slot, plane, part, at]
                )
                second = jnp.where(take, fresh[part], state[HALVES + 1, slot, plane, part, at])
                out_ref[slot, part, plane - 1, pl.ds(2 * start, chunk, stride=2), :] = jnp.where(
                    unpack_mask, first, second
                )
                out_ref[slot, part, plane - 1, pl.ds(2 * start + 1, chunk, stride=2), :] = jnp.where(
                    unpack_mask, second, first
                )

    for slot in (0, 1):

        def arrive(plane, _, slot=slot):
            @pl.when((plane > 1) & (plane < planes))
            def _():
                swap_copy(1 - slot, plane).wait_recv()

            wrap_rows(got, slot, plane)
            return 0

        def inner(plane, _, slot=slot):
            finish_plane(slot, plane)
            return 0

        lax.fori_loop(1, planes + 1, arrive, 0)
        upward(got, slot).wait_recv()
        downward(got, slot).wait_recv()
        lax.fori_loop(1, planes + 1, inner, 0)

    for slot in (0, 1):
        total_copy(1 - slot).wait_recv()
        own = total_sum[slot : slot + 1]
        other = total_got[slot, 1 - slot : 2 - slot]
        value = jnp.where(taking[slot], other, own)
        sites = float(columns * rows * planes * count)
        energy_ref[slot] = -jnp.sum(value) / sites

    bond_up.wait_send()
    for slot in (0, 1):
        meta_copy(slot).wait_send()
        total_copy(slot).wait_send()

    def drain_halo(index, _):
        step = index // 2 + 1
        slot = lax.rem(index, 2)
        upward(step, slot).wait_send()
        downward(step, slot).wait_send()
        return 0

    lax.fori_loop(0, 2 * HALVES, drain_halo, 0)
    for slot in (0, 1):
        upward(got, slot).wait_send()
        downward(got, slot).wait_send()

    def drain_temp(index, _):
        slot = index // planes
        plane = lax.rem(index, planes)
        draw_copy(slot, plane).wait_send()
        swap_copy(slot, plane + 1).wait_send()
        return 0

    lax.fori_loop(0, 2 * planes, drain_temp, 0)

    def drain_share(distance, _):
        share_copy(distance).wait_send()
        return 0

    lax.fori_loop(1, count, drain_share, 0)


def on_device(
    spin_state,
    couplings,
    inverse_temps,
    colour_order,
    heat_level,
    heat_height,
    heat_angle,
    swap_bits,
):
    slots, parts, planes, rows, columns = spin_state.shape
    half = rows // 2
    count = lax.axis_size("gz")
    f32 = jnp.float32
    dma = pltpu.SemaphoreType.DMA
    any_space = pl.BlockSpec(memory_space=pl.ANY)
    smem = pl.BlockSpec(memory_space=pltpu.SMEM)
    vmem = pl.BlockSpec(memory_space=pltpu.VMEM)
    steps = HALVES + 3
    return pl.pallas_call(
        step_kernel,
        out_shape=(
            jax.ShapeDtypeStruct(spin_state.shape, f32),
            jax.ShapeDtypeStruct((slots,), f32),
        ),
        in_specs=[any_space] * 5 + [smem] * 3,
        out_specs=(vmem, smem),
        scratch_shapes=[
            pltpu.VMEM(spin_state.shape, f32),
            pltpu.VMEM(couplings.shape, f32),
            pltpu.VMEM((3,) + heat_level.shape, f32),
            pltpu.VMEM((steps, slots, planes + 2, 3, half + 2 * PAD, columns), f32),
            pltpu.VMEM((2, planes, 2, half, columns), f32),
            pltpu.VMEM((2, planes, half, columns), f32),
            pltpu.VMEM((planes, half, columns), f32),
            pltpu.VMEM((2, planes + 1, half, columns), f32),
            pltpu.VMEM((rows, columns), f32),
            pltpu.VMEM((slots, 2, planes, 4, half, columns), f32),
            pltpu.VMEM((slots, 8, columns), f32),
            pltpu.VMEM((slots, 8, columns), f32),
            pltpu.VMEM((slots, planes, 3, half, columns), f32),
            pltpu.VMEM((slots, planes, 3, half, columns), f32),
            pltpu.VMEM((slots, planes, 4, half, columns), f32),
            pltpu.VMEM((2, columns), f32),
            pltpu.VMEM((count - 1, 2, columns), f32),
            pltpu.VMEM((2, columns), f32),
            pltpu.VMEM((slots, 2, columns), f32),
            dma((5,)),
            dma,
            dma,
            dma((steps, slots, 2)),
            dma((steps, slots, 2)),
            dma((slots,)),
            dma((slots,)),
            dma((slots, planes)),
            dma((slots, planes)),
            dma((slots, planes + 1)),
            dma((slots, planes + 1)),
            dma((count - 1,)),
            dma((count - 1,)),
            dma((slots,)),
            dma((slots,)),
            pltpu.SemaphoreType.REGULAR((max(1, len(far_distances(count))),)),
        ],
        compiler_params=pltpu.CompilerParams(
            collective_id=0, has_side_effects=True, vmem_limit_bytes=56 * 1024 * 1024
        ),
        name="replica_step",
    )(
        spin_state,
        couplings,
        heat_level,
        heat_height,
        heat_angle,
        inverse_temps,
        colour_order,
        swap_bits,
    )


def solution(mesh):
    return jax.shard_map(
        on_device,
        mesh=mesh,
        in_specs=(
            P(("group", "temp"), None, "gz", None, None),
            P(None, ("group", "gz"), None, None),
            P(("group", "temp")),
            P(("group", "temp")),
            P(("group", "temp"), "gz", None, None),
            P(("group", "temp"), "gz", None, None),
            P(("group", "temp"), "gz", None, None),
            P(("group", "temp")),
        ),
        out_specs=(P(("group", "temp"), None, "gz", None, None), P(("group", "temp"))),
        check_vma=False,
    )
```

```python
import functools

import jax
import jax.numpy as jnp
from jax import lax
from jax.experimental import pallas as pl
from jax.experimental.pallas import tpu as pltpu
from jax.sharding import PartitionSpec as P

OR_SWEEPS = 2
OR_HALVES = 2 * OR_SWEEPS
HALVES = OR_HALVES + 2
PAD = 8
CHUNKS = 4
MESH = pl.DeviceIdType.MESH

SIN_TERMS = (
    1.0,
    -1.0 / 6,
    1.0 / 120,
    -1.0 / 5040,
    1.0 / 362880,
    -1.0 / 39916800,
    1.0 / 6227020800,
)
COS_TERMS = (
    1.0,
    -1.0 / 2,
    1.0 / 24,
    -1.0 / 720,
    1.0 / 40320,
    -1.0 / 3628800,
    1.0 / 479001600,
    -1.0 / 87178291200,
)


def series(terms, square):
    total = jnp.full_like(square, terms[-1])
    for term in terms[-2::-1]:
        total = total * square + term
    return total


def cos_sin(angle):
    half = 0.5 * angle
    square = half * half
    sine = half * series(SIN_TERMS, square)
    cosine = series(COS_TERMS, square)
    return 1.0 - 2.0 * sine * sine, 2.0 * sine * cosine


def far_distances(count):
    distances, known = [], 2
    while known < count // 2:
        distances.append(known)
        known *= 2
    return distances


def step_kernel(
    spin_hbm,
    bond_hbm,
    level_hbm,
    height_hbm,
    angle_hbm,
    beta_hbm,
    order_hbm,
    bits_hbm,
    out_ref,
    energy_ref,
    beta_ref,
    order_ref,
    bits_ref,
    spin_in,
    bond_in,
    heat_in,
    state,
    bond_x,
    bond_yo,
    bond_ys,
    bond_z,
    bond_halo,
    trial,
    meta,
    meta_got,
    draws,
    draws_got,
    trial_got,
    share_sum,
    share_got,
    total_sum,
    total_got,
    gains,
    small_sem,
    spin_sem,
    load_sem,
    bond_send,
    bond_recv,
    send_sem,
    recv_sem,
    meta_send,
    meta_recv,
    draw_send,
    draw_recv,
    swap_send,
    swap_recv,
    share_send,
    share_recv,
    total_send,
    total_recv,
    far_sem,
):
    planes, rows, columns = spin_in.shape[2:]
    half = rows // 2
    piece = half // CHUNKS
    chunk = min(16, piece)
    me = lax.axis_index("gz")
    count = lax.axis_size("gz")
    upper = lax.rem(me + 1, count)
    lower = lax.rem(me + count - 1, count)
    here_temp = lax.axis_index("temp")
    temps = lax.axis_size("temp")
    main = pl.ds(PAD, half)
    got = HALVES + 2
    distances = far_distances(count)

    far_low = lax.rem(me, 2) == 0
    far_plane = jnp.where(far_low, 1, planes)
    near_plane = jnp.where(far_low, planes, 1)

    small = [
        pltpu.make_async_copy(source, target, small_sem.at[index])
        for index, (source, target) in enumerate(
            ((bits_hbm, bits_ref), (order_hbm, order_ref), (beta_hbm, beta_ref))
        )
    ]

    def spin_load(plane):
        return pltpu.make_async_copy(
            spin_hbm.at[:, :, plane - 1], spin_in.at[:, :, plane - 1], spin_sem.at[plane - 1]
        )

    loads = [
        pltpu.make_async_copy(bond_hbm, bond_in, load_sem.at[0]),
        pltpu.make_async_copy(level_hbm, heat_in.at[0], load_sem.at[1]),
        pltpu.make_async_copy(height_hbm, heat_in.at[1], load_sem.at[2]),
        pltpu.make_async_copy(angle_hbm, heat_in.at[2], load_sem.at[3]),
    ]
    for load in small:
        load.start()
    plane_order = [far_plane, near_plane] + list(range(2, planes))
    for plane in plane_order:
        spin_load(plane).start()
    for load in loads:
        load.start()

    def temp_towards(slot):
        return lax.rem(here_temp + 2 * slot - 1 + temps, temps)

    barrier = pltpu.get_barrier_semaphore()
    for neighbour in (lower, upper):
        pl.semaphore_signal(
            barrier, inc=1, device_id={"gz": neighbour}, device_id_type=MESH
        )
    for slot in (0, 1):
        pl.semaphore_signal(
            barrier, inc=1, device_id={"temp": temp_towards(slot)}, device_id_type=MESH
        )

    lane = lax.broadcasted_iota(jnp.int32, (half, columns), 1) % 2
    lane_chunk = lax.broadcasted_iota(jnp.int32, (chunk, columns), 1) % 2
    for load in small:
        load.wait()
    swapped = bits_ref[0] != 0

    def order_of(slot):
        other = 1 - slot
        return jnp.where(swapped, order_ref[other], order_ref[slot])

    def beta_of(slot):
        other = 1 - slot
        return jnp.where(swapped, beta_ref[other], beta_ref[slot])

    def parity(slot, plane):
        return lax.rem(me * planes + plane + order_of(slot), 2)

    for slot in (0, 1):
        meta[slot, 0:1] = jnp.full((1, columns), beta_of(slot), jnp.float32)
        meta[slot, 1:2] = jnp.full((1, columns), order_of(slot), jnp.int32).astype(jnp.float32)
        meta[slot, 2:3] = jnp.full((1, columns), bits_ref[1], jnp.int32).astype(jnp.float32)

    def halo(step, slot, down, rows_at, part):
        return pltpu.make_async_remote_copy(
            src_ref=state.at[step, slot, jnp.where(down, 1, planes), :, rows_at],
            dst_ref=state.at[step, slot, jnp.where(down, planes + 1, 0), :, rows_at],
            send_sem=send_sem.at[slot, part],
            recv_sem=recv_sem.at[1 if step is got else lax.rem(step, 2), slot, part],
            device_id={"gz": jnp.where(down, lower, upper)},
            device_id_type=MESH,
        )

    def far_out(step, slot, part):
        return halo(step, slot, far_low, pl.ds(PAD + part * piece, piece), part)

    def far_in(step, slot, part):
        return halo(step, slot, ~far_low, pl.ds(PAD + part * piece, piece), part)

    def near_out(step, slot):
        return halo(step, slot, ~far_low, main, CHUNKS)

    def near_in(step, slot):
        return halo(step, slot, far_low, main, CHUNKS)

    bond_up = pltpu.make_async_remote_copy(
        src_ref=bond_hbm.at[2, planes - 1],
        dst_ref=bond_halo,
        send_sem=bond_send,
        recv_sem=bond_recv,
        device_id={"gz": upper},
        device_id_type=MESH,
    )

    def along_temp(source, target, send, recv, slot):
        return pltpu.make_async_remote_copy(
            src_ref=source,
            dst_ref=target,
            send_sem=send,
            recv_sem=recv,
            device_id={"temp": temp_towards(slot)},
            device_id_type=MESH,
        )

    def meta_copy(slot):
        return along_temp(
            meta.at[slot], meta_got.at[1 - slot], meta_send.at[slot], meta_recv.at[1 - slot], slot
        )

    def draw_copy(slot, plane):
        return along_temp(
            draws.at[slot, plane],
            draws_got.at[1 - slot, plane],
            draw_send,
            draw_recv.at[1 - slot],
            slot,
        )

    def all_draws(slot):
        return along_temp(
            draws.at[slot], draws_got.at[1 - slot], draw_send, draw_recv.at[1 - slot], slot
        )

    def swap_copy(slot, plane):
        return along_temp(
            state.at[HALVES, slot, plane, :, main],
            state.at[got, 1 - slot, plane, :, main],
            swap_send.at[slot, plane - 1],
            swap_recv.at[1 - slot, plane - 1],
            slot,
        )

    def total_copy(slot):
        return along_temp(
            total_sum, total_got.at[1 - slot], total_send.at[slot], total_recv.at[1 - slot], slot
        )

    def share_copy(distance):
        return pltpu.make_async_remote_copy(
            src_ref=share_sum,
            dst_ref=share_got.at[distance - 1],
            send_sem=share_send,
            recv_sem=share_recv,
            device_id={"gz": lax.rem(me + distance, count)},
            device_id_type=MESH,
        )

    all_shares = pltpu.make_async_remote_copy(
        src_ref=share_got,
        dst_ref=share_got,
        send_sem=share_send,
        recv_sem=share_recv,
        device_id={"gz": upper},
        device_id_type=MESH,
    )

    def far_signal(index):
        if index < len(distances):
            for move in (distances[index], count - distances[index]):
                pl.semaphore_signal(
                    far_sem.at[index],
                    inc=1,
                    device_id={"gz": lax.rem(me + move, count)},
                    device_id_type=MESH,
                )

    def far_wait(index):
        if index < len(distances):
            pl.semaphore_wait(far_sem.at[index], 2)

    even_rows = pl.ds(0, half, stride=2)
    odd_rows = pl.ds(1, half, stride=2)

    def wrap_rows(step, slot, plane):
        for part in range(3):
            state[step, slot, plane, part, PAD - 1 : PAD] = state[
                step, slot, plane, part, PAD + half - 1 : PAD + half
            ]
            state[step, slot, plane, part, PAD + half : PAD + half + 1] = state[
                step, slot, plane, part, PAD : PAD + 1
            ]

    def pack_spins(plane):
        for part in range(3):
            pairs = [
                (
                    spin_in[r, part, plane - 1, even_rows, :],
                    spin_in[r, part, plane - 1, odd_rows, :],
                )
                for r in (0, 1)
            ]
            for slot in (0, 1):
                even = jnp.where(swapped, pairs[1 - slot][0], pairs[slot][0])
                odd = jnp.where(swapped, pairs[1 - slot][1], pairs[slot][1])
                mask = lane == parity(slot, plane - 1)
                state[0, slot, plane, part, main] = jnp.where(mask, even, odd)
                state[1, slot, plane, part, main] = jnp.where(mask, odd, even)
        for slot in (0, 1):
            wrap_rows(1, slot, plane)

    pl.semaphore_wait(barrier, 4)
    bond_up.start()
    spin_load(far_plane).wait()
    pack_spins(far_plane)
    for slot in (0, 1):
        for part in range(CHUNKS):
            far_out(1, slot, part).start()
    spin_load(near_plane).wait()
    pack_spins(near_plane)
    for slot in (0, 1):
        near_out(1, slot).start()
        meta_copy(slot).start()

    def pack_inner(plane, _):
        spin_load(plane).wait()
        pack_spins(plane)
        return 0

    lax.fori_loop(2, planes, pack_inner, 0)
    loads[0].wait()

    def pack_bonds(plane, _):
        even, odd = bond_in[0, plane, even_rows, :], bond_in[0, plane, odd_rows, :]
        first = jnp.where(lane == 0, even, odd)
        second = jnp.where(lane == 0, odd, even)
        bond_x[0, plane, 0] = first
        bond_x[1, plane, 0] = second
        bond_x[0, plane, 1] = pltpu.roll(second, 1, 1)
        bond_x[1, plane, 1] = pltpu.roll(first, 1, 1)
        even, odd = bond_in[1, plane, even_rows, :], bond_in[1, plane, odd_rows, :]
        before = pltpu.roll(odd, 1, 0)
        bond_ys[plane] = even
        bond_yo[0, plane] = jnp.where(lane == 0, before, odd)
        bond_yo[1, plane] = jnp.where(lane == 0, odd, before)
        even, odd = bond_in[2, plane, even_rows, :], bond_in[2, plane, odd_rows, :]
        bond_z[0, plane + 1] = jnp.where(lane == 0, even, odd)
        bond_z[1, plane + 1] = jnp.where(lane == 0, odd, even)
        return 0

    lax.fori_loop(0, planes, pack_bonds, 0)

    def pack_heat(slot, plane):
        side = 1 - slot
        mask = lane_chunk == parity(slot, plane)
        for start in range(0, half, chunk):
            here = pl.ds(start, chunk)
            even_here = pl.ds(2 * start, chunk, stride=2)
            odd_here = pl.ds(2 * start + 1, chunk, stride=2)
            packed = []
            for kind in range(3):
                even = jnp.where(
                    swapped,
                    heat_in[kind, side, plane, even_here, :],
                    heat_in[kind, slot, plane, even_here, :],
                )
                odd = jnp.where(
                    swapped,
                    heat_in[kind, side, plane, odd_here, :],
                    heat_in[kind, slot, plane, odd_here, :],
                )
                packed.append((jnp.where(mask, even, odd), jnp.where(mask, odd, even)))
                draws[slot, plane, kind, here] = packed[kind][1]
            for colour in (0, 1):
                level, height, angle = (draw[colour] for draw in packed)
                across = jnp.sqrt(jnp.maximum(1.0 - height * height, 0.0))
                cosine, sine = cos_sin(angle)
                trial[slot, colour, plane, 0, here] = level
                trial[slot, colour, plane, 1, here] = across * cosine
                trial[slot, colour, plane, 2, here] = across * sine
                trial[slot, colour, plane, 3, here] = height

    def bonds_of(pattern, plane, start):
        here = pl.ds(start, chunk)
        return (
            bond_x[pattern, plane - 1, 0, here],
            bond_x[pattern, plane - 1, 1, here],
            bond_ys[plane - 1, here],
            bond_yo[pattern, plane - 1, here],
            bond_z[pattern, plane, here],
            bond_z[pattern, plane - 1, here],
        )

    def pulls(step, slot, plane, bonds, mask, start):
        east, west, near, far, above, below = bonds
        at = pl.ds(PAD + start, chunk)
        out = []
        for part in range(3):
            centre = state[step, slot, plane, part, at]
            other = jnp.where(
                mask,
                state[step, slot, plane, part, pl.ds(PAD + start - 1, chunk)],
                state[step, slot, plane, part, pl.ds(PAD + start + 1, chunk)],
            )
            pulled = east * pltpu.roll(centre, columns - 1, 1) + west * pltpu.roll(centre, 1, 1)
            pulled = pulled + near * centre + far * other
            pulled = pulled + above * state[step, slot, plane + 1, part, at]
            pulled = pulled + below * state[step, slot, plane - 1, part, at]
            out.append(pulled)
        return out

    def dot(first, second):
        return first[0] * second[0] + first[1] * second[1] + first[2] * second[2]

    def colour_of(step, slot, plane):
        return lax.rem(parity(slot, plane - 1) + step + 1, 2)

    def relax_rows(step, slot, plane, start):
        pattern = colour_of(step, slot, plane)
        at = pl.ds(PAD + start, chunk)
        bonds = bonds_of(pattern, plane, start)
        pulled = pulls(step, slot, plane, bonds, lane_chunk == pattern, start)
        old = [state[step - 1, slot, plane, part, at] for part in range(3)]
        scale = 2.0 * dot(old, pulled) / jnp.maximum(dot(pulled, pulled), 0.01)
        for part in range(3):
            state[step + 1, slot, plane, part, at] = scale * pulled[part] - old[part]
        return 0

    def heated(pulled, beta, level, draw):
        square = jnp.maximum(dot(pulled, pulled), 0.01)
        inverse = lax.rsqrt(square)
        reach = beta * (square * inverse)
        axis = [part * inverse for part in pulled]
        cosine = 1.0 + jnp.log((1.0 - level) + level * jnp.exp(-2.0 * reach)) / reach
        along = dot(draw, axis)
        tangent = [draw[part] - along * axis[part] for part in range(3)]
        norm = lax.rsqrt(jnp.maximum(dot(tangent, tangent), 0.0001))
        side = jnp.sqrt(jnp.maximum(1.0 - cosine * cosine, 0.0)) * norm
        return [cosine * axis[part] + side * tangent[part] for part in range(3)]

    def heat_rows(step, slot, plane, start):
        colour = step - OR_HALVES - 1
        pattern = colour_of(step, slot, plane)
        at = pl.ds(PAD + start, chunk)
        here = pl.ds(start, chunk)
        bonds = bonds_of(pattern, plane, start)
        pulled = pulls(step, slot, plane, bonds, lane_chunk == pattern, start)
        level = trial[slot, colour, plane - 1, 0, here]
        draw = [trial[slot, colour, plane - 1, part, here] for part in (1, 2, 3)]
        fresh = heated(pulled, beta_of(slot), level, draw)
        for part in range(3):
            state[step + 1, slot, plane, part, at] = fresh[part]
        return jnp.sum(dot(fresh, pulled).reshape(-1, 8, columns), axis=0)

    def whole_plane(step, slot, plane, rows_of):
        total = 0
        for start in range(0, half, chunk):
            total = total + rows_of(step, slot, plane, start)
        wrap_rows(step + 1, slot, plane)
        return total

    def outer_planes(step, slot, rows_of, send, swap):
        total = 0
        for part in range(CHUNKS):
            far_in(step, slot, part).wait_recv()
            for start in range(part * piece, (part + 1) * piece, chunk):
                total = total + rows_of(step, slot, far_plane, start)
            if send:
                far_out(step, slot, part).wait_send()
                far_out(step + 1, slot, part).start()
        wrap_rows(step + 1, slot, far_plane)
        near_in(step, slot).wait_recv()
        total = total + whole_plane(step, slot, near_plane, rows_of)
        if send:
            near_out(step, slot).wait_send()
            near_out(step + 1, slot).start()
        if swap:
            swap_copy(slot, far_plane).start()
            swap_copy(slot, near_plane).start()
        return total

    def inner_planes(step, slot, rows_of, swap, initial):
        def visit(plane, total):
            total = total + whole_plane(step, slot, plane, rows_of)
            if swap:
                swap_copy(slot, plane).start()
            return total

        return lax.fori_loop(2, planes, visit, initial)

    zero = jnp.zeros((8, columns), jnp.float32)

    def first_inner(slot, _):
        inner_planes(1, slot, relax_rows, False, 0)
        return 0

    lax.fori_loop(0, 2, first_inner, 0)
    for load in loads[1:]:
        load.wait()

    def fill(visit, _):
        slot = visit // planes
        plane = lax.rem(visit, planes)
        pack_heat(slot, plane)
        draw_copy(slot, plane).start()
        return 0

    lax.fori_loop(0, 2 * planes, fill, 0)
    bond_up.wait_recv()
    even, odd = bond_halo[even_rows, :], bond_halo[odd_rows, :]
    bond_z[0, 0] = jnp.where(lane == 0, even, odd)
    bond_z[1, 0] = jnp.where(lane == 0, odd, even)

    def relax_round(visit, _):
        step = visit // 2 + 1
        slot = lax.rem(visit, 2)
        outer_planes(step, slot, relax_rows, True, False)
        inner_planes(step + 1, slot, relax_rows, False, 0)

        @pl.when(visit == 1)
        def _():
            far_signal(0)

        return 0

    lax.fori_loop(0, 2 * (OR_HALVES - 1), relax_round, 0)

    def last_relax(slot, _):
        outer_planes(OR_HALVES, slot, relax_rows, True, False)
        inner_planes(OR_HALVES + 1, slot, heat_rows, True, zero)
        return 0

    lax.fori_loop(0, 2, last_relax, 0)
    far_wait(0)
    far_signal(1)

    def first_heat(slot, _):
        outer_planes(OR_HALVES + 1, slot, heat_rows, True, True)
        gains[slot] = inner_planes(OR_HALVES + 2, slot, heat_rows, False, zero)
        return 0

    lax.fori_loop(0, 2, first_heat, 0)
    far_wait(1)
    far_signal(2)

    def second_heat(slot, _):
        gain = gains[slot] + outer_planes(OR_HALVES + 2, slot, heat_rows, False, False)
        share_sum[pl.ds(slot, 1), :] = jnp.sum(gain, axis=0, keepdims=True)
        return 0

    lax.fori_loop(0, 2, second_heat, 0)
    far_wait(2)

    share_copy(count // 2).start()

    def give_share(index, _):
        share_copy(count // 2 - index).start()
        share_copy(count // 2 + index).start()
        return 0

    lax.fori_loop(1, count // 2, give_share, 0)

    def pass_far(slot, _):
        swap_copy(1 - slot, far_plane).wait_recv()
        for part in range(CHUNKS):
            far_out(HALVES, slot, part).wait_send()
            far_out(got, slot, part).start()
        wrap_rows(got, slot, far_plane)
        return 0

    def pass_near(slot, _):
        swap_copy(1 - slot, near_plane).wait_recv()
        near_out(HALVES, slot).wait_send()
        near_out(got, slot).start()
        wrap_rows(got, slot, near_plane)
        return 0

    lax.fori_loop(0, 2, pass_far, 0)
    lax.fori_loop(0, 2, pass_near, 0)
    for slot in (0, 1):
        all_draws(1 - slot).wait_recv()
        meta_copy(1 - slot).wait_recv()

    def prepare(visit, _):
        slot = visit // planes
        plane = lax.rem(visit, planes)
        for start in range(0, half, chunk):
            here = pl.ds(start, chunk)
            level, height, angle = (draws_got[slot, plane, kind, here] for kind in range(3))
            across = jnp.sqrt(jnp.maximum(1.0 - height * height, 0.0))
            cosine, sine = cos_sin(angle)
            trial_got[slot, plane, 0, here] = level
            trial_got[slot, plane, 1, here] = across * cosine
            trial_got[slot, plane, 2, here] = across * sine
            trial_got[slot, plane, 3, here] = height
        return 0

    lax.fori_loop(0, 2 * planes, prepare, 0)

    taking = [
        (meta_got[0, 2:3] > 0.5) & (here_temp > 0),
        jnp.full((1, columns), bits_ref[1], jnp.int32) * jnp.where(here_temp < temps - 1, 1, 0) > 0,
    ]

    def finish_plane(slot, plane):
        take = jnp.broadcast_to(taking[slot], (chunk, columns))
        flip = jnp.broadcast_to(meta_got[slot, 1:2] > 0.5, (chunk, columns))
        beta = meta_got[slot, 0:1]
        base = lax.rem(me * planes + plane - 1, 2)
        first_mask = (lane_chunk == base) ^ flip
        own_mask = lane_chunk == parity(slot, plane - 1)
        unpack_mask = jnp.where(take, first_mask.astype(jnp.int32), own_mask.astype(jnp.int32)) > 0
        for start in range(0, half, chunk):
            at = pl.ds(PAD + start, chunk)
            here = pl.ds(start, chunk)
            plain = bonds_of(1 - base, plane, start)
            other = bonds_of(base, plane, start)
            bonds = [jnp.where(flip, b, a) for a, b in zip(plain, other)]
            pulled = pulls(got, slot, plane, bonds, ~first_mask, start)
            level = trial_got[slot, plane - 1, 0, here]
            draw = [trial_got[slot, plane - 1, part, here] for part in (1, 2, 3)]
            fresh = heated(pulled, beta, level, draw)
            for part in range(3):
                first = jnp.where(
                    take, state[got, slot, plane, part, at], state[HALVES, slot, plane, part, at]
                )
                second = jnp.where(take, fresh[part], state[HALVES + 1, slot, plane, part, at])
                out_ref[slot, part, plane - 1, pl.ds(2 * start, chunk, stride=2), :] = jnp.where(
                    unpack_mask, first, second
                )
                out_ref[slot, part, plane - 1, pl.ds(2 * start + 1, chunk, stride=2), :] = jnp.where(
                    unpack_mask, second, first
                )

    def arrive(visit, _):
        slot = visit // (planes - 2)
        plane = lax.rem(visit, planes - 2) + 2
        swap_copy(1 - slot, plane).wait_recv()
        wrap_rows(got, slot, plane)
        return 0

    lax.fori_loop(0, 2 * (planes - 2), arrive, 0)

    def finish_inner(plane, _):
        for slot in (0, 1):
            finish_plane(slot, plane)
        return 0

    lax.fori_loop(2, planes, finish_inner, 0)

    def finish_outer(index, _):
        @pl.when(index == 0)
        def _():
            for slot in (0, 1):
                near_in(got, slot).wait_recv()

        @pl.when(index == 1)
        def _():
            for slot in (0, 1):
                for part in range(CHUNKS):
                    far_in(got, slot, part).wait_recv()

        plane = jnp.where(index == 0, near_plane, far_plane)
        for slot in (0, 1):
            finish_plane(slot, plane)
        return 0

    lax.fori_loop(0, 2, finish_outer, 0)

    all_shares.wait_recv()
    total_sum[...] = share_sum[...] + jnp.sum(share_got[...], axis=0)
    for slot in (0, 1):
        total_copy(slot).start()

    bond_up.wait_send()
    all_shares.wait_send()
    for slot in (0, 1):
        meta_copy(slot).wait_send()
        all_draws(slot).wait_send()
        for part in range(CHUNKS):
            far_out(got, slot, part).wait_send()
        near_out(got, slot).wait_send()

    def drain_swap(index, _):
        swap_copy(index // planes, lax.rem(index, planes) + 1).wait_send()
        return 0

    lax.fori_loop(0, 2 * planes, drain_swap, 0)

    for slot in (0, 1):
        total_copy(1 - slot).wait_recv()
        own = total_sum[slot : slot + 1]
        other = total_got[slot, 1 - slot : 2 - slot]
        value = jnp.where(taking[slot], other, own)
        sites = float(columns * rows * planes * count)
        energy_ref[slot] = -jnp.sum(value) / sites

    for slot in (0, 1):
        total_copy(slot).wait_send()


def on_device(
    spin_state,
    couplings,
    inverse_temps,
    colour_order,
    heat_level,
    heat_height,
    heat_angle,
    swap_bits,
):
    slots, parts, planes, rows, columns = spin_state.shape
    half = rows // 2
    count = lax.axis_size("gz")
    f32 = jnp.float32
    dma = pltpu.SemaphoreType.DMA
    any_space = pl.BlockSpec(memory_space=pl.ANY)
    smem = pl.BlockSpec(memory_space=pltpu.SMEM)
    vmem = pl.BlockSpec(memory_space=pltpu.VMEM)
    steps = HALVES + 3
    return pl.pallas_call(
        step_kernel,
        out_shape=(
            pltpu.VMEM(spin_state.shape, f32),
            jax.ShapeDtypeStruct((slots,), f32),
        ),
        in_specs=[any_space] * 8,
        out_specs=(vmem, smem),
        scratch_shapes=[
            pltpu.SMEM((slots,), f32),
            pltpu.SMEM((slots,), jnp.int32),
            pltpu.SMEM((slots,), jnp.int32),
            pltpu.VMEM(spin_state.shape, f32),
            pltpu.VMEM(couplings.shape, f32),
            pltpu.VMEM((3,) + heat_level.shape, f32),
            pltpu.VMEM((steps, slots, planes + 2, 3, half + 2 * PAD, columns), f32),
            pltpu.VMEM((2, planes, 2, half, columns), f32),
            pltpu.VMEM((2, planes, half, columns), f32),
            pltpu.VMEM((planes, half, columns), f32),
            pltpu.VMEM((2, planes + 1, half, columns), f32),
            pltpu.VMEM((rows, columns), f32),
            pltpu.VMEM((slots, 2, planes, 4, half, columns), f32),
            pltpu.VMEM((slots, 8, columns), f32),
            pltpu.VMEM((slots, 8, columns), f32),
            pltpu.VMEM((slots, planes, 3, half, columns), f32),
            pltpu.VMEM((slots, planes, 3, half, columns), f32),
            pltpu.VMEM((slots, planes, 4, half, columns), f32),
            pltpu.VMEM((2, columns), f32),
            pltpu.VMEM((count - 1, 2, columns), f32),
            pltpu.VMEM((2, columns), f32),
            pltpu.VMEM((slots, 2, columns), f32),
            pltpu.VMEM((slots, 8, columns), f32),
            dma((3,)),
            dma((planes,)),
            dma((4,)),
            dma,
            dma,
            dma((slots, CHUNKS + 1)),
            dma((2, slots, CHUNKS + 1)),
            dma((slots,)),
            dma((slots,)),
            dma,
            dma((slots,)),
            dma((slots, planes)),
            dma((slots, planes)),
            dma,
            dma,
            dma((slots,)),
            dma((slots,)),
            pltpu.SemaphoreType.REGULAR((max(1, len(far_distances(count))),)),
        ],
        compiler_params=pltpu.CompilerParams(
            collective_id=0, has_side_effects=True, vmem_limit_bytes=56 * 1024 * 1024
        ),
        name="replica_step",
    )(
        spin_state,
        couplings,
        heat_level,
        heat_height,
        heat_angle,
        inverse_temps,
        colour_order,
        swap_bits,
    )


def solution(mesh):
    return jax.shard_map(
        on_device,
        mesh=mesh,
        in_specs=(
            P(("group", "temp"), None, "gz", None, None),
            P(None, ("group", "gz"), None, None),
            P(("group", "temp")),
            P(("group", "temp")),
            P(("group", "temp"), "gz", None, None),
            P(("group", "temp"), "gz", None, None),
            P(("group", "temp"), "gz", None, None),
            P(("group", "temp")),
        ),
        out_specs=(P(("group", "temp"), None, "gz", None, None), P(("group", "temp"))),
        check_vma=False,
    )
```

```python
import functools

import jax
import jax.numpy as jnp
from jax import lax
from jax.experimental import pallas as pl
from jax.experimental.pallas import tpu as pltpu
from jax.sharding import PartitionSpec as P

OR_SWEEPS = 2
OR_HALVES = 2 * OR_SWEEPS
HALVES = OR_HALVES + 2
PAD = 8
CHUNKS = 4
MESH = pl.DeviceIdType.MESH

SIN_TERMS = (
    1.0,
    -1.0 / 6,
    1.0 / 120,
    -1.0 / 5040,
    1.0 / 362880,
    -1.0 / 39916800,
    1.0 / 6227020800,
)
COS_TERMS = (
    1.0,
    -1.0 / 2,
    1.0 / 24,
    -1.0 / 720,
    1.0 / 40320,
    -1.0 / 3628800,
    1.0 / 479001600,
    -1.0 / 87178291200,
)


def series(terms, square):
    total = jnp.full_like(square, terms[-1])
    for term in terms[-2::-1]:
        total = total * square + term
    return total


def cos_sin(angle):
    half = 0.5 * angle
    square = half * half
    sine = half * series(SIN_TERMS, square)
    cosine = series(COS_TERMS, square)
    return 1.0 - 2.0 * sine * sine, 2.0 * sine * cosine


def far_distances(count):
    distances, known = [], 2
    while known < count // 2:
        distances.append(known)
        known *= 2
    return distances


def step_kernel(
    spin_hbm,
    bond_hbm,
    level_hbm,
    height_hbm,
    angle_hbm,
    beta_hbm,
    order_hbm,
    bits_hbm,
    out_ref,
    energy_ref,
    beta_ref,
    order_ref,
    bits_ref,
    spin_in,
    bond_in,
    heat_in,
    state,
    bond_x,
    bond_yo,
    bond_ys,
    bond_z,
    bond_halo,
    trial,
    meta,
    meta_got,
    draws,
    draws_got,
    trial_got,
    share_sum,
    share_got,
    total_sum,
    total_got,
    gains,
    small_sem,
    spin_sem,
    load_sem,
    bond_send,
    bond_recv,
    send_sem,
    recv_sem,
    meta_send,
    meta_recv,
    draw_send,
    draw_recv,
    swap_send,
    swap_recv,
    share_send,
    share_recv,
    total_send,
    total_recv,
    far_sem,
):
    planes, rows, columns = spin_in.shape[2:]
    half = rows // 2
    piece = half // CHUNKS
    chunk = min(32, half)
    me = lax.axis_index("gz")
    count = lax.axis_size("gz")
    upper = lax.rem(me + 1, count)
    lower = lax.rem(me + count - 1, count)
    here_temp = lax.axis_index("temp")
    temps = lax.axis_size("temp")
    main = pl.ds(PAD, half)
    got = HALVES + 2
    distances = far_distances(count)

    far_low = lax.rem(me, 2) == 0
    far_plane = jnp.where(far_low, 1, planes)
    near_plane = jnp.where(far_low, planes, 1)

    small = [
        pltpu.make_async_copy(source, target, small_sem.at[index])
        for index, (source, target) in enumerate(
            ((bits_hbm, bits_ref), (order_hbm, order_ref), (beta_hbm, beta_ref))
        )
    ]

    def spin_load(plane):
        return pltpu.make_async_copy(
            spin_hbm.at[:, :, plane - 1], spin_in.at[:, :, plane - 1], spin_sem.at[plane - 1]
        )

    loads = [
        pltpu.make_async_copy(bond_hbm, bond_in, load_sem.at[0]),
        pltpu.make_async_copy(level_hbm, heat_in.at[0], load_sem.at[1]),
        pltpu.make_async_copy(height_hbm, heat_in.at[1], load_sem.at[2]),
        pltpu.make_async_copy(angle_hbm, heat_in.at[2], load_sem.at[3]),
    ]
    for load in small:
        load.start()
    plane_order = [far_plane, near_plane] + list(range(2, planes))
    for plane in plane_order:
        spin_load(plane).start()
    for load in loads:
        load.start()

    def temp_towards(slot):
        return lax.rem(here_temp + 2 * slot - 1 + temps, temps)

    barrier = pltpu.get_barrier_semaphore()
    for neighbour in (lower, upper):
        pl.semaphore_signal(
            barrier, inc=1, device_id={"gz": neighbour}, device_id_type=MESH
        )
    for slot in (0, 1):
        pl.semaphore_signal(
            barrier, inc=1, device_id={"temp": temp_towards(slot)}, device_id_type=MESH
        )

    lane = lax.broadcasted_iota(jnp.int32, (half, columns), 1) % 2
    lane_chunk = lax.broadcasted_iota(jnp.int32, (chunk, columns), 1) % 2
    def lane_piece(size):
        return lax.broadcasted_iota(jnp.int32, (size, columns), 1) % 2

    for load in small:
        load.wait()
    swapped = bits_ref[0] != 0

    def order_of(slot):
        other = 1 - slot
        return jnp.where(swapped, order_ref[other], order_ref[slot])

    def beta_of(slot):
        other = 1 - slot
        return jnp.where(swapped, beta_ref[other], beta_ref[slot])

    def parity(slot, plane):
        return lax.rem(me * planes + plane + order_of(slot), 2)

    for slot in (0, 1):
        meta[slot, 0:1] = jnp.full((1, columns), beta_of(slot), jnp.float32)
        meta[slot, 1:2] = jnp.full((1, columns), order_of(slot), jnp.int32).astype(jnp.float32)
        meta[slot, 2:3] = jnp.full((1, columns), bits_ref[1], jnp.int32).astype(jnp.float32)

    def halo(step, slot, down, rows_at, part):
        return pltpu.make_async_remote_copy(
            src_ref=state.at[step, slot, jnp.where(down, 1, planes), :, rows_at],
            dst_ref=state.at[step, slot, jnp.where(down, planes + 1, 0), :, rows_at],
            send_sem=send_sem.at[slot, part],
            recv_sem=recv_sem.at[2 if isinstance(step, int) and step == got else lax.rem(step, 2), slot, part],
            device_id={"gz": jnp.where(down, lower, upper)},
            device_id_type=MESH,
        )

    def far_out(step, slot, part):
        return halo(step, slot, far_low, pl.ds(PAD + part * piece, piece), part)

    def far_in(step, slot, part):
        return halo(step, slot, ~far_low, pl.ds(PAD + part * piece, piece), part)

    def near_out(step, slot):
        return halo(step, slot, ~far_low, main, CHUNKS)

    def near_in(step, slot):
        return halo(step, slot, far_low, main, CHUNKS)

    bond_up = pltpu.make_async_remote_copy(
        src_ref=bond_hbm.at[2, planes - 1],
        dst_ref=bond_halo,
        send_sem=bond_send,
        recv_sem=bond_recv,
        device_id={"gz": upper},
        device_id_type=MESH,
    )

    def along_temp(source, target, send, recv, slot):
        return pltpu.make_async_remote_copy(
            src_ref=source,
            dst_ref=target,
            send_sem=send,
            recv_sem=recv,
            device_id={"temp": temp_towards(slot)},
            device_id_type=MESH,
        )

    def meta_copy(slot):
        return along_temp(
            meta.at[slot], meta_got.at[1 - slot], meta_send.at[slot], meta_recv.at[1 - slot], slot
        )

    def draw_copy(slot, plane):
        return along_temp(
            draws.at[slot, plane],
            draws_got.at[1 - slot, plane],
            draw_send,
            draw_recv.at[1 - slot],
            slot,
        )

    def all_draws(slot):
        return along_temp(
            draws.at[slot], draws_got.at[1 - slot], draw_send, draw_recv.at[1 - slot], slot
        )

    def swap_copy(slot, plane):
        return along_temp(
            state.at[HALVES, slot, plane, :, main],
            state.at[got, 1 - slot, plane, :, main],
            swap_send.at[slot, plane - 1],
            swap_recv.at[1 - slot, plane - 1],
            slot,
        )

    def total_copy(slot):
        return along_temp(
            total_sum, total_got.at[1 - slot], total_send.at[slot], total_recv.at[1 - slot], slot
        )

    def share_copy(distance):
        return pltpu.make_async_remote_copy(
            src_ref=share_sum,
            dst_ref=share_got.at[distance - 1],
            send_sem=share_send,
            recv_sem=share_recv,
            device_id={"gz": lax.rem(me + distance, count)},
            device_id_type=MESH,
        )

    all_shares = pltpu.make_async_remote_copy(
        src_ref=share_got,
        dst_ref=share_got,
        send_sem=share_send,
        recv_sem=share_recv,
        device_id={"gz": upper},
        device_id_type=MESH,
    )

    def far_signal(index):
        if index < len(distances):
            for move in (distances[index], count - distances[index]):
                pl.semaphore_signal(
                    far_sem.at[index],
                    inc=1,
                    device_id={"gz": lax.rem(me + move, count)},
                    device_id_type=MESH,
                )

    def far_wait(index):
        if index < len(distances):
            pl.semaphore_wait(far_sem.at[index], 2)

    even_rows = pl.ds(0, half, stride=2)
    odd_rows = pl.ds(1, half, stride=2)

    def wrap_rows(step, slot, plane):
        for part in range(3):
            state[step, slot, plane, part, PAD - 1 : PAD] = state[
                step, slot, plane, part, PAD + half - 1 : PAD + half
            ]
            state[step, slot, plane, part, PAD + half : PAD + half + 1] = state[
                step, slot, plane, part, PAD : PAD + 1
            ]

    def pack_spins(plane):
        for part in range(3):
            pairs = [
                (
                    spin_in[r, part, plane - 1, even_rows, :],
                    spin_in[r, part, plane - 1, odd_rows, :],
                )
                for r in (0, 1)
            ]
            for slot in (0, 1):
                even = jnp.where(swapped, pairs[1 - slot][0], pairs[slot][0])
                odd = jnp.where(swapped, pairs[1 - slot][1], pairs[slot][1])
                mask = lane == parity(slot, plane - 1)
                state[0, slot, plane, part, main] = jnp.where(mask, even, odd)
                state[1, slot, plane, part, main] = jnp.where(mask, odd, even)
        for slot in (0, 1):
            wrap_rows(1, slot, plane)

    pl.semaphore_wait(barrier, 4)
    bond_up.start()
    spin_load(far_plane).wait()
    pack_spins(far_plane)
    for slot in (0, 1):
        for part in range(CHUNKS):
            far_out(1, slot, part).start()
    spin_load(near_plane).wait()
    pack_spins(near_plane)
    for slot in (0, 1):
        near_out(1, slot).start()
        meta_copy(slot).start()

    def pack_inner(plane, _):
        spin_load(plane).wait()
        pack_spins(plane)
        return 0

    lax.fori_loop(2, planes, pack_inner, 0)
    loads[0].wait()

    def pack_bonds(plane, _):
        even, odd = bond_in[0, plane, even_rows, :], bond_in[0, plane, odd_rows, :]
        first = jnp.where(lane == 0, even, odd)
        second = jnp.where(lane == 0, odd, even)
        bond_x[0, plane, 0] = first
        bond_x[1, plane, 0] = second
        bond_x[0, plane, 1] = pltpu.roll(second, 1, 1)
        bond_x[1, plane, 1] = pltpu.roll(first, 1, 1)
        even, odd = bond_in[1, plane, even_rows, :], bond_in[1, plane, odd_rows, :]
        before = pltpu.roll(odd, 1, 0)
        bond_ys[plane] = even
        bond_yo[0, plane] = jnp.where(lane == 0, before, odd)
        bond_yo[1, plane] = jnp.where(lane == 0, odd, before)
        even, odd = bond_in[2, plane, even_rows, :], bond_in[2, plane, odd_rows, :]
        bond_z[0, plane + 1] = jnp.where(lane == 0, even, odd)
        bond_z[1, plane + 1] = jnp.where(lane == 0, odd, even)
        return 0

    lax.fori_loop(0, planes, pack_bonds, 0)

    def pack_heat(slot, plane):
        side = 1 - slot
        mask = lane_chunk == parity(slot, plane)
        for start in range(0, half, chunk):
            here = pl.ds(start, chunk)
            even_here = pl.ds(2 * start, chunk, stride=2)
            odd_here = pl.ds(2 * start + 1, chunk, stride=2)
            packed = []
            for kind in range(3):
                even = jnp.where(
                    swapped,
                    heat_in[kind, side, plane, even_here, :],
                    heat_in[kind, slot, plane, even_here, :],
                )
                odd = jnp.where(
                    swapped,
                    heat_in[kind, side, plane, odd_here, :],
                    heat_in[kind, slot, plane, odd_here, :],
                )
                packed.append((jnp.where(mask, even, odd), jnp.where(mask, odd, even)))
                draws[slot, plane, kind, here] = packed[kind][1]
            for colour in (0, 1):
                level, height, angle = (draw[colour] for draw in packed)
                across = jnp.sqrt(jnp.maximum(1.0 - height * height, 0.0))
                cosine, sine = cos_sin(angle)
                trial[slot, colour, plane, 0, here] = level
                trial[slot, colour, plane, 1, here] = across * cosine
                trial[slot, colour, plane, 2, here] = across * sine
                trial[slot, colour, plane, 3, here] = height

    def bonds_of(pattern, plane, start, size=chunk):
        here = pl.ds(start, size)
        return (
            bond_x[pattern, plane - 1, 0, here],
            bond_x[pattern, plane - 1, 1, here],
            bond_ys[plane - 1, here],
            bond_yo[pattern, plane - 1, here],
            bond_z[pattern, plane, here],
            bond_z[pattern, plane - 1, here],
        )

    def pulls(step, slot, plane, bonds, mask, start, size=chunk):
        east, west, near, far, above, below = bonds
        at = pl.ds(PAD + start, size)
        out = []
        for part in range(3):
            centre = state[step, slot, plane, part, at]
            other = jnp.where(
                mask,
                state[step, slot, plane, part, pl.ds(PAD + start - 1, size)],
                state[step, slot, plane, part, pl.ds(PAD + start + 1, size)],
            )
            pulled = east * pltpu.roll(centre, columns - 1, 1) + west * pltpu.roll(centre, 1, 1)
            pulled = pulled + near * centre + far * other
            pulled = pulled + above * state[step, slot, plane + 1, part, at]
            pulled = pulled + below * state[step, slot, plane - 1, part, at]
            out.append(pulled)
        return out

    def dot(first, second):
        return first[0] * second[0] + first[1] * second[1] + first[2] * second[2]

    def colour_of(step, slot, plane):
        return lax.rem(parity(slot, plane - 1) + step + 1, 2)

    def relax_rows(step, slot, plane, start, size):
        pattern = colour_of(step, slot, plane)
        at = pl.ds(PAD + start, size)
        bonds = bonds_of(pattern, plane, start, size)
        pulled = pulls(step, slot, plane, bonds, lane_piece(size) == pattern, start, size)
        old = [state[step - 1, slot, plane, part, at] for part in range(3)]
        scale = 2.0 * dot(old, pulled) / jnp.maximum(dot(pulled, pulled), 0.01)
        for part in range(3):
            state[step + 1, slot, plane, part, at] = scale * pulled[part] - old[part]
        return 0

    def heated(pulled, beta, level, draw):
        square = jnp.maximum(dot(pulled, pulled), 0.01)
        inverse = lax.rsqrt(square)
        reach = beta * (square * inverse)
        axis = [part * inverse for part in pulled]
        cosine = 1.0 + jnp.log((1.0 - level) + level * jnp.exp(-2.0 * reach)) / reach
        along = dot(draw, axis)
        tangent = [draw[part] - along * axis[part] for part in range(3)]
        norm = lax.rsqrt(jnp.maximum(dot(tangent, tangent), 0.0001))
        side = jnp.sqrt(jnp.maximum(1.0 - cosine * cosine, 0.0)) * norm
        return [cosine * axis[part] + side * tangent[part] for part in range(3)]

    def heat_rows(step, slot, plane, start, size):
        colour = step - OR_HALVES - 1
        pattern = colour_of(step, slot, plane)
        at = pl.ds(PAD + start, size)
        here = pl.ds(start, size)
        bonds = bonds_of(pattern, plane, start, size)
        pulled = pulls(step, slot, plane, bonds, lane_piece(size) == pattern, start, size)
        level = trial[slot, colour, plane - 1, 0, here]
        draw = [trial[slot, colour, plane - 1, part, here] for part in (1, 2, 3)]
        fresh = heated(pulled, beta_of(slot), level, draw)
        for part in range(3):
            state[step + 1, slot, plane, part, at] = fresh[part]
        return jnp.sum(dot(fresh, pulled).reshape(-1, 8, columns), axis=0)

    def whole_plane(step, slot, plane, rows_of):
        total = 0
        for start in range(0, half, chunk):
            total = total + rows_of(step, slot, plane, start, chunk)
        wrap_rows(step + 1, slot, plane)
        return total

    def outer_planes(step, slot, rows_of, send, swap):
        total = 0
        for part in range(CHUNKS):
            far_in(step, slot, part).wait_recv()
            total = total + rows_of(step, slot, far_plane, part * piece, piece)
            if send:
                far_out(step, slot, part).wait_send()
                far_out(step + 1, slot, part).start()
        wrap_rows(step + 1, slot, far_plane)
        near_in(step, slot).wait_recv()
        total = total + whole_plane(step, slot, near_plane, rows_of)
        if send:
            near_out(step, slot).wait_send()
            near_out(step + 1, slot).start()
        if swap:
            swap_copy(slot, far_plane).start()
            swap_copy(slot, near_plane).start()
        return total

    def inner_planes(step, slot, rows_of, swap, initial):
        def visit(plane, total):
            total = total + whole_plane(step, slot, plane, rows_of)
            if swap:
                swap_copy(slot, plane).start()
            return total

        return lax.fori_loop(2, planes, visit, initial)

    zero = jnp.zeros((8, columns), jnp.float32)

    def first_inner(slot, _):
        inner_planes(1, slot, relax_rows, False, 0)
        return 0

    lax.fori_loop(0, 2, first_inner, 0)
    for load in loads[1:]:
        load.wait()

    def fill(visit, _):
        slot = visit // planes
        plane = lax.rem(visit, planes)
        pack_heat(slot, plane)
        draw_copy(slot, plane).start()
        return 0

    lax.fori_loop(0, 2 * planes, fill, 0)
    bond_up.wait_recv()
    even, odd = bond_halo[even_rows, :], bond_halo[odd_rows, :]
    bond_z[0, 0] = jnp.where(lane == 0, even, odd)
    bond_z[1, 0] = jnp.where(lane == 0, odd, even)

    def relax_round(visit, _):
        step = visit // 2 + 1
        slot = lax.rem(visit, 2)
        outer_planes(step, slot, relax_rows, True, False)
        inner_planes(step + 1, slot, relax_rows, False, 0)

        @pl.when(visit == 1)
        def _():
            far_signal(0)

        return 0

    lax.fori_loop(0, 2 * (OR_HALVES - 1), relax_round, 0)

    def last_relax(slot, _):
        outer_planes(OR_HALVES, slot, relax_rows, True, False)
        inner_planes(OR_HALVES + 1, slot, heat_rows, True, zero)
        return 0

    lax.fori_loop(0, 2, last_relax, 0)
    far_wait(0)
    far_signal(1)

    def first_heat(slot, _):
        outer_planes(OR_HALVES + 1, slot, heat_rows, True, True)
        gains[slot] = inner_planes(OR_HALVES + 2, slot, heat_rows, False, zero)
        return 0

    lax.fori_loop(0, 2, first_heat, 0)
    far_wait(1)
    far_signal(2)

    def second_heat(slot):
        gain = gains[slot] + outer_planes(OR_HALVES + 2, slot, heat_rows, False, False)
        share_sum[slot : slot + 1, :] = jnp.sum(gain, axis=0, keepdims=True)

    def pass_far(slot):
        swap_copy(1 - slot, far_plane).wait_recv()
        for part in range(CHUNKS):
            far_out(HALVES, slot, part).wait_send()
            far_out(got, slot, part).start()
        wrap_rows(got, slot, far_plane)

    second_heat(0)
    second_heat(1)
    far_wait(2)
    share_copy(count // 2).start()

    def give_share(index, _):
        share_copy(count // 2 - index).start()
        share_copy(count // 2 + index).start()
        return 0

    lax.fori_loop(1, count // 2, give_share, 0)

    def pass_near(slot, _):
        swap_copy(1 - slot, near_plane).wait_recv()
        near_out(HALVES, slot).wait_send()
        near_out(got, slot).start()
        wrap_rows(got, slot, near_plane)
        return 0

    pass_far(1)
    pass_far(0)
    lax.fori_loop(0, 2, pass_near, 0)
    for slot in (0, 1):
        all_draws(1 - slot).wait_recv()
        meta_copy(1 - slot).wait_recv()

    def prepare(visit, _):
        slot = visit // planes
        plane = lax.rem(visit, planes)
        for start in range(0, half, chunk):
            here = pl.ds(start, chunk)
            level, height, angle = (draws_got[slot, plane, kind, here] for kind in range(3))
            across = jnp.sqrt(jnp.maximum(1.0 - height * height, 0.0))
            cosine, sine = cos_sin(angle)
            trial_got[slot, plane, 0, here] = level
            trial_got[slot, plane, 1, here] = across * cosine
            trial_got[slot, plane, 2, here] = across * sine
            trial_got[slot, plane, 3, here] = height
        return 0

    lax.fori_loop(0, 2 * planes, prepare, 0)

    taking = [
        (meta_got[0, 2:3] > 0.5) & (here_temp > 0),
        jnp.full((1, columns), bits_ref[1], jnp.int32) * jnp.where(here_temp < temps - 1, 1, 0) > 0,
    ]

    def finish_plane(slot, plane):
        take = jnp.broadcast_to(taking[slot], (chunk, columns))
        flip = jnp.broadcast_to(meta_got[slot, 1:2] > 0.5, (chunk, columns))
        beta = meta_got[slot, 0:1]
        base = lax.rem(me * planes + plane - 1, 2)
        first_mask = (lane_chunk == base) ^ flip
        own_mask = lane_chunk == parity(slot, plane - 1)
        unpack_mask = jnp.where(take, first_mask.astype(jnp.int32), own_mask.astype(jnp.int32)) > 0
        for start in range(0, half, chunk):
            at = pl.ds(PAD + start, chunk)
            here = pl.ds(start, chunk)
            plain = bonds_of(1 - base, plane, start)
            other = bonds_of(base, plane, start)
            bonds = [jnp.where(flip, b, a) for a, b in zip(plain, other)]
            pulled = pulls(got, slot, plane, bonds, ~first_mask, start)
            level = trial_got[slot, plane - 1, 0, here]
            draw = [trial_got[slot, plane - 1, part, here] for part in (1, 2, 3)]
            fresh = heated(pulled, beta, level, draw)
            for part in range(3):
                first = jnp.where(
                    take, state[got, slot, plane, part, at], state[HALVES, slot, plane, part, at]
                )
                second = jnp.where(take, fresh[part], state[HALVES + 1, slot, plane, part, at])
                out_ref[slot, part, plane - 1, pl.ds(2 * start, chunk, stride=2), :] = jnp.where(
                    unpack_mask, first, second
                )
                out_ref[slot, part, plane - 1, pl.ds(2 * start + 1, chunk, stride=2), :] = jnp.where(
                    unpack_mask, second, first
                )

    def arrive(visit, _):
        slot = visit // (planes - 2)
        plane = lax.rem(visit, planes - 2) + 2
        swap_copy(1 - slot, plane).wait_recv()
        wrap_rows(got, slot, plane)
        return 0

    lax.fori_loop(0, 2 * (planes - 2), arrive, 0)

    def finish_inner(plane, _):
        for slot in (0, 1):
            finish_plane(slot, plane)
        return 0

    lax.fori_loop(2, planes, finish_inner, 0)

    all_shares.wait_recv()
    total_sum[...] = share_sum[...] + jnp.sum(share_got[...], axis=0)
    for slot in (0, 1):
        total_copy(slot).start()

    def finish_outer(index, _):
        @pl.when(index == 0)
        def _():
            for slot in (0, 1):
                near_in(got, slot).wait_recv()

        @pl.when(index == 1)
        def _():
            for slot in (0, 1):
                for part in range(CHUNKS):
                    far_in(got, slot, part).wait_recv()

        plane = jnp.where(index == 0, near_plane, far_plane)
        for slot in (0, 1):
            finish_plane(slot, plane)
        return 0

    lax.fori_loop(0, 2, finish_outer, 0)

    bond_up.wait_send()
    all_shares.wait_send()
    for slot in (0, 1):
        meta_copy(slot).wait_send()
        all_draws(slot).wait_send()
        for part in range(CHUNKS):
            far_out(got, slot, part).wait_send()
        near_out(got, slot).wait_send()

    def drain_swap(index, _):
        swap_copy(index // planes, lax.rem(index, planes) + 1).wait_send()
        return 0

    lax.fori_loop(0, 2 * planes, drain_swap, 0)

    for slot in (0, 1):
        total_copy(1 - slot).wait_recv()
        own = total_sum[slot : slot + 1]
        other = total_got[slot, 1 - slot : 2 - slot]
        value = jnp.where(taking[slot], other, own)
        sites = float(columns * rows * planes * count)
        energy_ref[slot] = -jnp.sum(value) / sites

    for slot in (0, 1):
        total_copy(slot).wait_send()


def on_device(
    spin_state,
    couplings,
    inverse_temps,
    colour_order,
    heat_level,
    heat_height,
    heat_angle,
    swap_bits,
):
    slots, parts, planes, rows, columns = spin_state.shape
    half = rows // 2
    count = lax.axis_size("gz")
    f32 = jnp.float32
    dma = pltpu.SemaphoreType.DMA
    any_space = pl.BlockSpec(memory_space=pl.ANY)
    smem = pl.BlockSpec(memory_space=pltpu.SMEM)
    vmem = pl.BlockSpec(memory_space=pltpu.VMEM)
    steps = HALVES + 3
    return pl.pallas_call(
        step_kernel,
        out_shape=(
            pltpu.VMEM(spin_state.shape, f32),
            jax.ShapeDtypeStruct((slots,), f32),
        ),
        in_specs=[any_space] * 8,
        out_specs=(vmem, smem),
        scratch_shapes=[
            pltpu.SMEM((slots,), f32),
            pltpu.SMEM((slots,), jnp.int32),
            pltpu.SMEM((slots,), jnp.int32),
            pltpu.VMEM(spin_state.shape, f32),
            pltpu.VMEM(couplings.shape, f32),
            pltpu.VMEM((3,) + heat_level.shape, f32),
            pltpu.VMEM((steps, slots, planes + 2, 3, half + 2 * PAD, columns), f32),
            pltpu.VMEM((2, planes, 2, half, columns), f32),
            pltpu.VMEM((2, planes, half, columns), f32),
            pltpu.VMEM((planes, half, columns), f32),
            pltpu.VMEM((2, planes + 1, half, columns), f32),
            pltpu.VMEM((rows, columns), f32),
            pltpu.VMEM((slots, 2, planes, 4, half, columns), f32),
            pltpu.VMEM((slots, 8, columns), f32),
            pltpu.VMEM((slots, 8, columns), f32),
            pltpu.VMEM((slots, planes, 3, half, columns), f32),
            pltpu.VMEM((slots, planes, 3, half, columns), f32),
            pltpu.VMEM((slots, planes, 4, half, columns), f32),
            pltpu.VMEM((2, columns), f32),
            pltpu.VMEM((count - 1, 2, columns), f32),
            pltpu.VMEM((2, columns), f32),
            pltpu.VMEM((slots, 2, columns), f32),
            pltpu.VMEM((slots, 8, columns), f32),
            dma((3,)),
            dma((planes,)),
            dma((4,)),
            dma,
            dma,
            dma((slots, CHUNKS + 1)),
            dma((3, slots, CHUNKS + 1)),
            dma((slots,)),
            dma((slots,)),
            dma,
            dma((slots,)),
            dma((slots, planes)),
            dma((slots, planes)),
            dma,
            dma,
            dma((slots,)),
            dma((slots,)),
            pltpu.SemaphoreType.REGULAR((max(1, len(far_distances(count))),)),
        ],
        compiler_params=pltpu.CompilerParams(
            collective_id=0, has_side_effects=True, vmem_limit_bytes=56 * 1024 * 1024
        ),
        name="replica_step",
    )(
        spin_state,
        couplings,
        heat_level,
        heat_height,
        heat_angle,
        inverse_temps,
        colour_order,
        swap_bits,
    )


def solution(mesh):
    return jax.shard_map(
        on_device,
        mesh=mesh,
        in_specs=(
            P(("group", "temp"), None, "gz", None, None),
            P(None, ("group", "gz"), None, None),
            P(("group", "temp")),
            P(("group", "temp")),
            P(("group", "temp"), "gz", None, None),
            P(("group", "temp"), "gz", None, None),
            P(("group", "temp"), "gz", None, None),
            P(("group", "temp")),
        ),
        out_specs=(P(("group", "temp"), None, "gz", None, None), P(("group", "temp"))),
        check_vma=False,
    )
```

```python
import functools

import jax
import jax.numpy as jnp
from jax import lax
from jax.experimental import pallas as pl
from jax.experimental.pallas import tpu as pltpu
from jax.sharding import PartitionSpec as P

OR_SWEEPS = 2
OR_HALVES = 2 * OR_SWEEPS
HALVES = OR_HALVES + 2
PAD = 8
CHUNKS = 4
MESH = pl.DeviceIdType.MESH

SIN_TERMS = (
    1.0,
    -1.0 / 6,
    1.0 / 120,
    -1.0 / 5040,
    1.0 / 362880,
    -1.0 / 39916800,
    1.0 / 6227020800,
)
COS_TERMS = (
    1.0,
    -1.0 / 2,
    1.0 / 24,
    -1.0 / 720,
    1.0 / 40320,
    -1.0 / 3628800,
    1.0 / 479001600,
    -1.0 / 87178291200,
)


def series(terms, square):
    total = jnp.full_like(square, terms[-1])
    for term in terms[-2::-1]:
        total = total * square + term
    return total


def cos_sin(angle):
    half = 0.5 * angle
    square = half * half
    sine = half * series(SIN_TERMS, square)
    cosine = series(COS_TERMS, square)
    return 1.0 - 2.0 * sine * sine, 2.0 * sine * cosine


def far_distances(count):
    distances, known = [], 2
    while known < count // 2:
        distances.append(known)
        known *= 2
    return distances


def step_kernel(
    spin_hbm,
    bond_hbm,
    level_hbm,
    height_hbm,
    angle_hbm,
    beta_hbm,
    order_hbm,
    bits_hbm,
    out_ref,
    energy_ref,
    beta_ref,
    order_ref,
    bits_ref,
    spin_in,
    bond_in,
    heat_in,
    state,
    bond_x,
    bond_yo,
    bond_ys,
    bond_z,
    bond_halo,
    bond_top,
    trial,
    meta,
    meta_got,
    draws,
    draws_got,
    trial_got,
    share_sum,
    share_got,
    total_sum,
    total_got,
    gains,
    small_sem,
    spin_sem,
    load_sem,
    bond_send,
    bond_recv,
    send_sem,
    recv_sem,
    meta_send,
    meta_recv,
    draw_send,
    draw_recv,
    swap_send,
    swap_recv,
    share_send,
    share_recv,
    total_send,
    total_recv,
    far_sem,
):
    planes, rows, columns = spin_in.shape[2:]
    half = rows // 2
    piece = half // CHUNKS
    chunk = min(32, half)
    me = lax.axis_index("gz")
    count = lax.axis_size("gz")
    upper = lax.rem(me + 1, count)
    lower = lax.rem(me + count - 1, count)
    here_temp = lax.axis_index("temp")
    temps = lax.axis_size("temp")
    main = pl.ds(PAD, half)
    got = HALVES + 2
    distances = far_distances(count)

    far_low = lax.rem(me, 2) == 0
    far_plane = jnp.where(far_low, 1, planes)
    near_plane = jnp.where(far_low, planes, 1)

    small = [
        pltpu.make_async_copy(source, target, small_sem.at[index])
        for index, (source, target) in enumerate(
            ((bits_hbm, bits_ref), (order_hbm, order_ref), (beta_hbm, beta_ref))
        )
    ]

    def spin_load(plane):
        return pltpu.make_async_copy(
            spin_hbm.at[:, :, plane - 1], spin_in.at[:, :, plane - 1], spin_sem.at[plane - 1]
        )

    loads = [
        pltpu.make_async_copy(bond_hbm, bond_in, load_sem.at[0]),
        pltpu.make_async_copy(level_hbm, heat_in.at[0], load_sem.at[1]),
        pltpu.make_async_copy(height_hbm, heat_in.at[1], load_sem.at[2]),
        pltpu.make_async_copy(angle_hbm, heat_in.at[2], load_sem.at[3]),
    ]
    for load in small:
        load.start()
    top_load = pltpu.make_async_copy(bond_hbm.at[2, planes - 1], bond_top, load_sem.at[4])
    top_load.start()
    plane_order = [far_plane, near_plane] + list(range(2, planes))
    for plane in plane_order:
        spin_load(plane).start()
    for load in loads:
        load.start()

    def temp_towards(slot):
        return lax.rem(here_temp + 2 * slot - 1 + temps, temps)

    barrier = pltpu.get_barrier_semaphore()
    for neighbour in (lower, upper):
        pl.semaphore_signal(
            barrier, inc=1, device_id={"gz": neighbour}, device_id_type=MESH
        )
    for slot in (0, 1):
        pl.semaphore_signal(
            barrier, inc=1, device_id={"temp": temp_towards(slot)}, device_id_type=MESH
        )

    lane = lax.broadcasted_iota(jnp.int32, (half, columns), 1) % 2
    lane_chunk = lax.broadcasted_iota(jnp.int32, (chunk, columns), 1) % 2
    def lane_piece(size):
        return lax.broadcasted_iota(jnp.int32, (size, columns), 1) % 2

    for load in small:
        load.wait()
    swapped = bits_ref[0] != 0

    def order_of(slot):
        other = 1 - slot
        return jnp.where(swapped, order_ref[other], order_ref[slot])

    def beta_of(slot):
        other = 1 - slot
        return jnp.where(swapped, beta_ref[other], beta_ref[slot])

    def parity(slot, plane):
        return lax.rem(me * planes + plane + order_of(slot), 2)

    for slot in (0, 1):
        meta[slot, 0:1] = jnp.full((1, columns), beta_of(slot), jnp.float32)
        meta[slot, 1:2] = jnp.full((1, columns), order_of(slot), jnp.int32).astype(jnp.float32)
        meta[slot, 2:3] = jnp.full((1, columns), bits_ref[1], jnp.int32).astype(jnp.float32)

    def halo(step, slot, down, rows_at, part):
        return pltpu.make_async_remote_copy(
            src_ref=state.at[step, slot, jnp.where(down, 1, planes), :, rows_at],
            dst_ref=state.at[step, slot, jnp.where(down, planes + 1, 0), :, rows_at],
            send_sem=send_sem.at[slot, part],
            recv_sem=recv_sem.at[2 if isinstance(step, int) and step == got else lax.rem(step, 2), slot, part],
            device_id={"gz": jnp.where(down, lower, upper)},
            device_id_type=MESH,
        )

    def far_out(step, slot, part):
        return halo(step, slot, far_low, pl.ds(PAD + part * piece, piece), part)

    def far_in(step, slot, part):
        return halo(step, slot, ~far_low, pl.ds(PAD + part * piece, piece), part)

    def near_out(step, slot):
        return halo(step, slot, ~far_low, main, CHUNKS)

    def near_in(step, slot):
        return halo(step, slot, far_low, main, CHUNKS)

    bond_up = pltpu.make_async_remote_copy(
        src_ref=bond_top,
        dst_ref=bond_halo,
        send_sem=bond_send,
        recv_sem=bond_recv,
        device_id={"gz": upper},
        device_id_type=MESH,
    )

    def along_temp(source, target, send, recv, slot):
        return pltpu.make_async_remote_copy(
            src_ref=source,
            dst_ref=target,
            send_sem=send,
            recv_sem=recv,
            device_id={"temp": temp_towards(slot)},
            device_id_type=MESH,
        )

    def meta_copy(slot):
        return along_temp(
            meta.at[slot], meta_got.at[1 - slot], meta_send.at[slot], meta_recv.at[1 - slot], slot
        )

    def draw_copy(slot, plane):
        return along_temp(
            draws.at[slot, plane],
            draws_got.at[1 - slot, plane],
            draw_send,
            draw_recv.at[1 - slot],
            slot,
        )

    def all_draws(slot):
        return along_temp(
            draws.at[slot], draws_got.at[1 - slot], draw_send, draw_recv.at[1 - slot], slot
        )

    def swap_copy(slot, plane):
        return along_temp(
            state.at[HALVES, slot, plane, :, main],
            state.at[got, 1 - slot, plane, :, main],
            swap_send,
            swap_recv.at[1 - slot, plane - 1],
            slot,
        )

    all_swaps = along_temp(
        state.at[HALVES, :, pl.ds(1, planes), :, main],
        state.at[got, :, pl.ds(1, planes), :, main],
        swap_send,
        swap_recv.at[0, 0],
        0,
    )

    def total_copy(slot):
        return along_temp(
            total_sum, total_got.at[1 - slot], total_send.at[slot], total_recv.at[1 - slot], slot
        )

    def share_copy(distance):
        return pltpu.make_async_remote_copy(
            src_ref=share_sum,
            dst_ref=share_got.at[distance - 1],
            send_sem=share_send,
            recv_sem=share_recv,
            device_id={"gz": lax.rem(me + distance, count)},
            device_id_type=MESH,
        )

    all_shares = pltpu.make_async_remote_copy(
        src_ref=share_got,
        dst_ref=share_got,
        send_sem=share_send,
        recv_sem=share_recv,
        device_id={"gz": upper},
        device_id_type=MESH,
    )

    def far_signal(index):
        if index < len(distances):
            for move in (distances[index], count - distances[index]):
                pl.semaphore_signal(
                    far_sem.at[index],
                    inc=1,
                    device_id={"gz": lax.rem(me + move, count)},
                    device_id_type=MESH,
                )

    def far_wait(index):
        if index < len(distances):
            pl.semaphore_wait(far_sem.at[index], 2)

    even_rows = pl.ds(0, half, stride=2)
    odd_rows = pl.ds(1, half, stride=2)

    def wrap_rows(step, slot, plane):
        for part in range(3):
            state[step, slot, plane, part, PAD - 1 : PAD] = state[
                step, slot, plane, part, PAD + half - 1 : PAD + half
            ]
            state[step, slot, plane, part, PAD + half : PAD + half + 1] = state[
                step, slot, plane, part, PAD : PAD + 1
            ]

    def pack_spins(plane):
        for part in range(3):
            pairs = [
                (
                    spin_in[r, part, plane - 1, even_rows, :],
                    spin_in[r, part, plane - 1, odd_rows, :],
                )
                for r in (0, 1)
            ]
            for slot in (0, 1):
                even = jnp.where(swapped, pairs[1 - slot][0], pairs[slot][0])
                odd = jnp.where(swapped, pairs[1 - slot][1], pairs[slot][1])
                mask = lane == parity(slot, plane - 1)
                state[0, slot, plane, part, main] = jnp.where(mask, even, odd)
                state[1, slot, plane, part, main] = jnp.where(mask, odd, even)
        for slot in (0, 1):
            wrap_rows(1, slot, plane)

    def first_copy(slot, down, rows_at, part):
        return pltpu.make_async_remote_copy(
            src_ref=state.at[jnp.where(down, 1, 0), slot, jnp.where(down, 1, 0), :, rows_at],
            dst_ref=state.at[1, slot, jnp.where(down, planes + 1, 0), :, rows_at],
            send_sem=send_sem.at[slot, part],
            recv_sem=recv_sem.at[1, slot, part],
            device_id={"gz": jnp.where(down, lower, upper)},
            device_id_type=MESH,
        )

    def stage_products():
        even, odd = bond_top[even_rows, :], bond_top[odd_rows, :]
        for slot in (0, 1):
            bond = jnp.where(lane == parity(slot, planes - 1), odd, even)
            for part in range(3):
                state[0, slot, 0, part, main] = bond * state[1, slot, planes, part, main]

    pl.semaphore_wait(barrier, 4)
    top_load.wait()
    spin_load(far_plane).wait()
    pack_spins(far_plane)

    @pl.when(~far_low)
    def _():
        stage_products()

    for slot in (0, 1):
        for part in range(CHUNKS):
            first_copy(slot, far_low, pl.ds(PAD + part * piece, piece), part).start()
    spin_load(near_plane).wait()
    pack_spins(near_plane)

    @pl.when(far_low)
    def _():
        stage_products()

    for slot in (0, 1):
        first_copy(slot, ~far_low, main, CHUNKS).start()
        meta_copy(slot).start()
    bond_up.start()

    def pack_inner(plane, _):
        spin_load(plane).wait()
        pack_spins(plane)
        return 0

    lax.fori_loop(2, planes, pack_inner, 0)
    loads[0].wait()

    def pack_bonds(plane, _):
        even, odd = bond_in[0, plane, even_rows, :], bond_in[0, plane, odd_rows, :]
        first = jnp.where(lane == 0, even, odd)
        second = jnp.where(lane == 0, odd, even)
        bond_x[0, plane, 0] = first
        bond_x[1, plane, 0] = second
        bond_x[0, plane, 1] = pltpu.roll(second, 1, 1)
        bond_x[1, plane, 1] = pltpu.roll(first, 1, 1)
        even, odd = bond_in[1, plane, even_rows, :], bond_in[1, plane, odd_rows, :]
        before = pltpu.roll(odd, 1, 0)
        bond_ys[plane] = even
        bond_yo[0, plane] = jnp.where(lane == 0, before, odd)
        bond_yo[1, plane] = jnp.where(lane == 0, odd, before)
        even, odd = bond_in[2, plane, even_rows, :], bond_in[2, plane, odd_rows, :]
        bond_z[0, plane + 1] = jnp.where(lane == 0, even, odd)
        bond_z[1, plane + 1] = jnp.where(lane == 0, odd, even)
        return 0

    lax.fori_loop(0, planes, pack_bonds, 0)

    def pack_heat(slot, plane):
        side = 1 - slot
        mask = lane_chunk == parity(slot, plane)
        for start in range(0, half, chunk):
            here = pl.ds(start, chunk)
            even_here = pl.ds(2 * start, chunk, stride=2)
            odd_here = pl.ds(2 * start + 1, chunk, stride=2)
            packed = []
            for kind in range(3):
                even = jnp.where(
                    swapped,
                    heat_in[kind, side, plane, even_here, :],
                    heat_in[kind, slot, plane, even_here, :],
                )
                odd = jnp.where(
                    swapped,
                    heat_in[kind, side, plane, odd_here, :],
                    heat_in[kind, slot, plane, odd_here, :],
                )
                packed.append((jnp.where(mask, even, odd), jnp.where(mask, odd, even)))
                draws[slot, plane, kind, here] = packed[kind][1]
            for colour in (0, 1):
                level, height, angle = (draw[colour] for draw in packed)
                across = jnp.sqrt(jnp.maximum(1.0 - height * height, 0.0))
                cosine, sine = cos_sin(angle)
                trial[slot, colour, plane, 0, here] = level
                trial[slot, colour, plane, 1, here] = across * cosine
                trial[slot, colour, plane, 2, here] = across * sine
                trial[slot, colour, plane, 3, here] = height

    def bonds_of(pattern, plane, start, size=chunk):
        here = pl.ds(start, size)
        return (
            bond_x[pattern, plane - 1, 0, here],
            bond_x[pattern, plane - 1, 1, here],
            bond_ys[plane - 1, here],
            bond_yo[pattern, plane - 1, here],
            bond_z[pattern, plane, here],
            bond_z[pattern, plane - 1, here],
        )

    def pulls(step, slot, plane, bonds, mask, start, size=chunk):
        east, west, near, far, above, below = bonds
        at = pl.ds(PAD + start, size)
        out = []
        for part in range(3):
            centre = state[step, slot, plane, part, at]
            other = jnp.where(
                mask,
                state[step, slot, plane, part, pl.ds(PAD + start - 1, size)],
                state[step, slot, plane, part, pl.ds(PAD + start + 1, size)],
            )
            pulled = east * pltpu.roll(centre, columns - 1, 1) + west * pltpu.roll(centre, 1, 1)
            pulled = pulled + near * centre + far * other
            pulled = pulled + above * state[step, slot, plane + 1, part, at]
            pulled = pulled + below * state[step, slot, plane - 1, part, at]
            out.append(pulled)
        return out

    def dot(first, second):
        return first[0] * second[0] + first[1] * second[1] + first[2] * second[2]

    def colour_of(step, slot, plane):
        return lax.rem(parity(slot, plane - 1) + step + 1, 2)

    def relax_rows(step, slot, plane, start, size):
        pattern = colour_of(step, slot, plane)
        at = pl.ds(PAD + start, size)
        bonds = bonds_of(pattern, plane, start, size)
        pulled = pulls(step, slot, plane, bonds, lane_piece(size) == pattern, start, size)
        old = [state[step - 1, slot, plane, part, at] for part in range(3)]
        scale = 2.0 * dot(old, pulled) / jnp.maximum(dot(pulled, pulled), 0.01)
        for part in range(3):
            state[step + 1, slot, plane, part, at] = scale * pulled[part] - old[part]
        return 0

    def heated(pulled, beta, level, draw):
        square = jnp.maximum(dot(pulled, pulled), 0.01)
        inverse = lax.rsqrt(square)
        reach = beta * (square * inverse)
        axis = [part * inverse for part in pulled]
        cosine = 1.0 + jnp.log((1.0 - level) + level * jnp.exp(-2.0 * reach)) / reach
        along = dot(draw, axis)
        tangent = [draw[part] - along * axis[part] for part in range(3)]
        norm = lax.rsqrt(jnp.maximum(dot(tangent, tangent), 0.0001))
        side = jnp.sqrt(jnp.maximum(1.0 - cosine * cosine, 0.0)) * norm
        return [cosine * axis[part] + side * tangent[part] for part in range(3)]

    def heat_rows(step, slot, plane, start, size):
        colour = step - OR_HALVES - 1
        pattern = colour_of(step, slot, plane)
        at = pl.ds(PAD + start, size)
        here = pl.ds(start, size)
        bonds = bonds_of(pattern, plane, start, size)
        pulled = pulls(step, slot, plane, bonds, lane_piece(size) == pattern, start, size)
        level = trial[slot, colour, plane - 1, 0, here]
        draw = [trial[slot, colour, plane - 1, part, here] for part in (1, 2, 3)]
        fresh = heated(pulled, beta_of(slot), level, draw)
        for part in range(3):
            state[step + 1, slot, plane, part, at] = fresh[part]
        return jnp.sum(dot(fresh, pulled).reshape(-1, 8, columns), axis=0)

    def whole_plane(step, slot, plane, rows_of):
        total = 0
        for start in range(0, half, chunk):
            total = total + rows_of(step, slot, plane, start, chunk)
        wrap_rows(step + 1, slot, plane)
        return total

    def far_rows(step, slot, rows_of, send, swap):
        total = 0
        for part in range(CHUNKS):
            far_in(step, slot, part).wait_recv()
            total = total + rows_of(step, slot, far_plane, part * piece, piece)
            if send:
                far_out(step, slot, part).wait_send()
                far_out(step + 1, slot, part).start()
        wrap_rows(step + 1, slot, far_plane)
        if swap:
            swap_copy(slot, far_plane).start()
        return total

    def near_rows(step, slot, rows_of, send, swap):
        near_in(step, slot).wait_recv()
        total = whole_plane(step, slot, near_plane, rows_of)
        if send:
            near_out(step, slot).wait_send()
            near_out(step + 1, slot).start()
        if swap:
            swap_copy(slot, near_plane).start()
        return total

    def both(body):
        def visit(slot, _):
            body(slot)
            return 0

        lax.fori_loop(0, 2, visit, 0)

    def inner_planes(step, slot, rows_of, swap, initial):
        def visit(plane, total):
            total = total + whole_plane(step, slot, plane, rows_of)
            if swap:
                swap_copy(slot, plane).start()
            return total

        return lax.fori_loop(2, planes, visit, initial)

    zero = jnp.zeros((8, columns), jnp.float32)

    def first_inner(slot, _):
        inner_planes(1, slot, relax_rows, False, 0)
        return 0

    lax.fori_loop(0, 2, first_inner, 0)
    for load in loads[1:]:
        load.wait()

    def fill(visit, _):
        slot = visit // planes
        plane = lax.rem(visit, planes)
        pack_heat(slot, plane)
        draw_copy(slot, plane).start()
        return 0

    lax.fori_loop(0, 2 * planes, fill, 0)
    bond_z[0, 0] = jnp.ones((half, columns), jnp.float32)
    bond_z[1, 0] = jnp.ones((half, columns), jnp.float32)

    def relax_round(step, _):
        both(lambda slot: far_rows(step, slot, relax_rows, True, False))
        both(lambda slot: near_rows(step, slot, relax_rows, True, False))

        @pl.when(step == 1)
        def _():
            far_signal(0)
            bond_up.wait_recv()
            even, odd = bond_halo[even_rows, :], bond_halo[odd_rows, :]
            bond_z[0, 0] = jnp.where(lane == 0, even, odd)
            bond_z[1, 0] = jnp.where(lane == 0, odd, even)

        both(lambda slot: inner_planes(step + 1, slot, relax_rows, False, 0))
        return 0

    lax.fori_loop(1, OR_HALVES, relax_round, 0)
    both(lambda slot: far_rows(OR_HALVES, slot, relax_rows, True, False))
    both(lambda slot: near_rows(OR_HALVES, slot, relax_rows, True, False))
    both(lambda slot: inner_planes(OR_HALVES + 1, slot, heat_rows, True, zero))
    far_wait(0)
    far_signal(1)

    both(lambda slot: far_rows(OR_HALVES + 1, slot, heat_rows, True, True))
    both(lambda slot: near_rows(OR_HALVES + 1, slot, heat_rows, True, True))

    def inner_gain(slot):
        gains[slot] = inner_planes(OR_HALVES + 2, slot, heat_rows, False, zero)

    def far_gain(slot):
        gains[slot] = gains[slot] + far_rows(OR_HALVES + 2, slot, heat_rows, False, False)

    def near_gain(slot):
        gain = gains[slot] + near_rows(OR_HALVES + 2, slot, heat_rows, False, False)
        share_sum[pl.ds(slot, 1), :] = jnp.sum(gain, axis=0, keepdims=True)

    both(inner_gain)
    far_wait(1)
    far_signal(2)
    both(far_gain)
    both(near_gain)
    far_wait(2)

    def pass_far(slot):
        swap_copy(1 - slot, far_plane).wait_recv()
        for part in range(CHUNKS):
            far_out(HALVES, slot, part).wait_send()
            far_out(got, slot, part).start()
        wrap_rows(got, slot, far_plane)

    share_copy(count // 2).start()

    def give_share(index, _):
        share_copy(count // 2 - index).start()
        share_copy(count // 2 + index).start()
        return 0

    lax.fori_loop(1, count // 2, give_share, 0, unroll=True)

    def pass_near(slot, _):
        swap_copy(1 - slot, near_plane).wait_recv()
        near_out(HALVES, slot).wait_send()
        near_out(got, slot).start()
        wrap_rows(got, slot, near_plane)
        return 0

    pass_far(1)
    pass_far(0)
    lax.fori_loop(0, 2, pass_near, 0)
    for slot in (0, 1):
        all_draws(1 - slot).wait_recv()
        meta_copy(1 - slot).wait_recv()

    def prepare(visit, _):
        slot = visit // planes
        plane = lax.rem(visit, planes)
        for start in range(0, half, chunk):
            here = pl.ds(start, chunk)
            level, height, angle = (draws_got[slot, plane, kind, here] for kind in range(3))
            across = jnp.sqrt(jnp.maximum(1.0 - height * height, 0.0))
            cosine, sine = cos_sin(angle)
            trial_got[slot, plane, 0, here] = level
            trial_got[slot, plane, 1, here] = across * cosine
            trial_got[slot, plane, 2, here] = across * sine
            trial_got[slot, plane, 3, here] = height
        return 0

    lax.fori_loop(0, 2 * planes, prepare, 0)

    taking = [
        (meta_got[0, 2:3] > 0.5) & (here_temp > 0),
        jnp.full((1, columns), bits_ref[1], jnp.int32) * jnp.where(here_temp < temps - 1, 1, 0) > 0,
    ]

    def finish_plane(slot, plane):
        take = jnp.broadcast_to(taking[slot], (chunk, columns))
        flip = jnp.broadcast_to(meta_got[slot, 1:2] > 0.5, (chunk, columns))
        beta = meta_got[slot, 0:1]
        base = lax.rem(me * planes + plane - 1, 2)
        first_mask = (lane_chunk == base) ^ flip
        own_mask = lane_chunk == parity(slot, plane - 1)
        unpack_mask = jnp.where(take, first_mask.astype(jnp.int32), own_mask.astype(jnp.int32)) > 0
        for start in range(0, half, chunk):
            at = pl.ds(PAD + start, chunk)
            here = pl.ds(start, chunk)
            plain = bonds_of(1 - base, plane, start)
            other = bonds_of(base, plane, start)
            bonds = [jnp.where(flip, b, a) for a, b in zip(plain, other)]
            pulled = pulls(got, slot, plane, bonds, ~first_mask, start)
            level = trial_got[slot, plane - 1, 0, here]
            draw = [trial_got[slot, plane - 1, part, here] for part in (1, 2, 3)]
            fresh = heated(pulled, beta, level, draw)
            for part in range(3):
                first = jnp.where(
                    take, state[got, slot, plane, part, at], state[HALVES, slot, plane, part, at]
                )
                second = jnp.where(take, fresh[part], state[HALVES + 1, slot, plane, part, at])
                out_ref[slot, part, plane - 1, pl.ds(2 * start, chunk, stride=2), :] = jnp.where(
                    unpack_mask, first, second
                )
                out_ref[slot, part, plane - 1, pl.ds(2 * start + 1, chunk, stride=2), :] = jnp.where(
                    unpack_mask, second, first
                )

    def arrive(visit, _):
        slot = visit // (planes - 2)
        plane = lax.rem(visit, planes - 2) + 2
        swap_copy(1 - slot, plane).wait_recv()
        wrap_rows(got, slot, plane)
        return 0

    lax.fori_loop(0, 2 * (planes - 2), arrive, 0)

    def finish_inner(plane, _):
        for slot in (0, 1):
            finish_plane(slot, plane)
        return 0

    lax.fori_loop(2, planes, finish_inner, 0)

    all_shares.wait_recv()
    total_sum[...] = share_sum[...] + jnp.sum(share_got[...], axis=0)
    for slot in (0, 1):
        total_copy(slot).start()

    def finish_outer(index, _):
        @pl.when(index == 0)
        def _():
            for slot in (0, 1):
                near_in(got, slot).wait_recv()

        @pl.when(index == 1)
        def _():
            for slot in (0, 1):
                for part in range(CHUNKS):
                    far_in(got, slot, part).wait_recv()

        plane = jnp.where(index == 0, near_plane, far_plane)
        for slot in (0, 1):
            finish_plane(slot, plane)
        return 0

    lax.fori_loop(0, 2, finish_outer, 0)

    bond_up.wait_send()
    all_shares.wait_send()
    for slot in (0, 1):
        meta_copy(slot).wait_send()
        all_draws(slot).wait_send()
        for part in range(CHUNKS):
            far_out(got, slot, part).wait_send()
        near_out(got, slot).wait_send()

    all_swaps.wait_send()

    for slot in (0, 1):
        total_copy(1 - slot).wait_recv()
    sites = float(columns * rows * planes * count)
    values = [
        jnp.where(taking[slot], total_got[slot, 1 - slot : 2 - slot], total_sum[slot : slot + 1])
        for slot in (0, 1)
    ]
    sums = [-jnp.sum(value, axis=1, keepdims=True) / sites for value in values]
    spot = lax.broadcasted_iota(jnp.int32, (1, columns), 1)
    energy_ref[...] = jnp.where(spot == 0, sums[0], sums[1])

    for slot in (0, 1):
        total_copy(slot).wait_send()


def on_device(
    spin_state,
    couplings,
    inverse_temps,
    colour_order,
    heat_level,
    heat_height,
    heat_angle,
    swap_bits,
):
    slots, parts, planes, rows, columns = spin_state.shape
    half = rows // 2
    count = lax.axis_size("gz")
    f32 = jnp.float32
    dma = pltpu.SemaphoreType.DMA
    any_space = pl.BlockSpec(memory_space=pl.ANY)
    vmem = pl.BlockSpec(memory_space=pltpu.VMEM)
    steps = HALVES + 3
    spins, energies = pl.pallas_call(
        step_kernel,
        out_shape=(
            pltpu.VMEM(spin_state.shape, f32),
            pltpu.VMEM((1, columns), f32),
        ),
        in_specs=[any_space] * 8,
        out_specs=(vmem, vmem),
        scratch_shapes=[
            pltpu.SMEM((slots,), f32),
            pltpu.SMEM((slots,), jnp.int32),
            pltpu.SMEM((slots,), jnp.int32),
            pltpu.VMEM(spin_state.shape, f32),
            pltpu.VMEM(couplings.shape, f32),
            pltpu.VMEM((3,) + heat_level.shape, f32),
            pltpu.VMEM((steps, slots, planes + 2, 3, half + 2 * PAD, columns), f32),
            pltpu.VMEM((2, planes, 2, half, columns), f32),
            pltpu.VMEM((2, planes, half, columns), f32),
            pltpu.VMEM((planes, half, columns), f32),
            pltpu.VMEM((2, planes + 1, half, columns), f32),
            pltpu.VMEM((rows, columns), f32),
            pltpu.VMEM((rows, columns), f32),
            pltpu.VMEM((slots, 2, planes, 4, half, columns), f32),
            pltpu.VMEM((slots, 8, columns), f32),
            pltpu.VMEM((slots, 8, columns), f32),
            pltpu.VMEM((slots, planes, 3, half, columns), f32),
            pltpu.VMEM((slots, planes, 3, half, columns), f32),
            pltpu.VMEM((slots, planes, 4, half, columns), f32),
            pltpu.VMEM((2, columns), f32),
            pltpu.VMEM((count - 1, 2, columns), f32),
            pltpu.VMEM((2, columns), f32),
            pltpu.VMEM((slots, 2, columns), f32),
            pltpu.VMEM((slots, 8, columns), f32),
            dma((3,)),
            dma((planes,)),
            dma((5,)),
            dma,
            dma,
            dma((slots, CHUNKS + 1)),
            dma((3, slots, CHUNKS + 1)),
            dma((slots,)),
            dma((slots,)),
            dma,
            dma((slots,)),
            dma,
            dma((slots, planes)),
            dma,
            dma,
            dma((slots,)),
            dma((slots,)),
            pltpu.SemaphoreType.REGULAR((max(1, len(far_distances(count))),)),
        ],
        compiler_params=pltpu.CompilerParams(
            collective_id=0, has_side_effects=True, vmem_limit_bytes=56 * 1024 * 1024
        ),
        name="replica_step",
    )(
        spin_state,
        couplings,
        heat_level,
        heat_height,
        heat_angle,
        inverse_temps,
        colour_order,
        swap_bits,
    )
    return (spins, energies[0, :slots])


def solution(mesh):
    return jax.shard_map(
        on_device,
        mesh=mesh,
        in_specs=(
            P(("group", "temp"), None, "gz", None, None),
            P(None, ("group", "gz"), None, None),
            P(("group", "temp")),
            P(("group", "temp")),
            P(("group", "temp"), "gz", None, None),
            P(("group", "temp"), "gz", None, None),
            P(("group", "temp"), "gz", None, None),
            P(("group", "temp")),
        ),
        out_specs=(P(("group", "temp"), None, "gz", None, None), P(("group", "temp"))),
        check_vma=False,
    )
```

```python
import functools

import jax
import jax.numpy as jnp
from jax import lax
from jax.experimental import pallas as pl
from jax.experimental.pallas import tpu as pltpu
from jax.sharding import PartitionSpec as P

OR_SWEEPS = 2
OR_HALVES = 2 * OR_SWEEPS
HALVES = OR_HALVES + 2
PAD = 8
CHUNKS = 4
MESH = pl.DeviceIdType.MESH

SIN_TERMS = (
    1.0,
    -1.0 / 6,
    1.0 / 120,
    -1.0 / 5040,
    1.0 / 362880,
    -1.0 / 39916800,
    1.0 / 6227020800,
)
COS_TERMS = (
    1.0,
    -1.0 / 2,
    1.0 / 24,
    -1.0 / 720,
    1.0 / 40320,
    -1.0 / 3628800,
    1.0 / 479001600,
    -1.0 / 87178291200,
)


def series(terms, square):
    total = jnp.full_like(square, terms[-1])
    for term in terms[-2::-1]:
        total = total * square + term
    return total


def cos_sin(angle):
    half = 0.5 * angle
    square = half * half
    sine = half * series(SIN_TERMS, square)
    cosine = series(COS_TERMS, square)
    return 1.0 - 2.0 * sine * sine, 2.0 * sine * cosine


def far_distances(count):
    distances, known = [], 2
    while known < count // 2:
        distances.append(known)
        known *= 2
    return distances


def step_kernel(
    spin_hbm,
    bond_hbm,
    level_hbm,
    height_hbm,
    angle_hbm,
    beta_hbm,
    order_hbm,
    bits_hbm,
    out_ref,
    energy_ref,
    beta_ref,
    order_ref,
    bits_ref,
    spin_in,
    bond_in,
    heat_in,
    state,
    bond_x,
    bond_yo,
    bond_ys,
    bond_z,
    bond_halo,
    bond_top,
    trial,
    meta,
    meta_got,
    draws,
    draws_got,
    trial_got,
    share_sum,
    share_got,
    total_sum,
    total_got,
    gains,
    small_sem,
    spin_sem,
    load_sem,
    bond_send,
    bond_recv,
    send_sem,
    recv_sem,
    meta_send,
    meta_recv,
    draw_send,
    draw_recv,
    swap_send,
    swap_recv,
    share_send,
    share_recv,
    total_send,
    total_recv,
    far_sem,
):
    planes, rows, columns = spin_in.shape[2:]
    half = rows // 2
    piece = half // CHUNKS
    chunk = min(32, half)
    me = lax.axis_index("gz")
    count = lax.axis_size("gz")
    upper = lax.rem(me + 1, count)
    lower = lax.rem(me + count - 1, count)
    here_temp = lax.axis_index("temp")
    temps = lax.axis_size("temp")
    main = pl.ds(PAD, half)
    got = HALVES + 2
    distances = far_distances(count)

    def temp_towards(slot):
        return lax.rem(here_temp + 2 * slot - 1 + temps, temps)

    def has(slot):
        return (here_temp + slot > 0) & (here_temp + slot < temps)

    barrier = pltpu.get_barrier_semaphore()
    for neighbour in (lower, upper):
        pl.semaphore_signal(
            barrier, inc=1, device_id={"gz": neighbour}, device_id_type=MESH
        )
    for slot in (0, 1):

        @pl.when(has(slot))
        def _(slot=slot):
            pl.semaphore_signal(
                barrier, inc=1, device_id={"temp": temp_towards(slot)}, device_id_type=MESH
            )

    far_low = lax.rem(me, 2) == 0
    far_plane = jnp.where(far_low, 1, planes)
    near_plane = jnp.where(far_low, planes, 1)

    small = [
        pltpu.make_async_copy(source, target, small_sem.at[index])
        for index, (source, target) in enumerate(
            ((bits_hbm, bits_ref), (order_hbm, order_ref), (beta_hbm, beta_ref))
        )
    ]

    def spin_load(plane):
        return pltpu.make_async_copy(
            spin_hbm.at[:, :, plane - 1], spin_in.at[:, :, plane - 1], spin_sem.at[plane - 1]
        )

    loads = [
        pltpu.make_async_copy(bond_hbm, bond_in, load_sem.at[0]),
        pltpu.make_async_copy(level_hbm, heat_in.at[0], load_sem.at[1]),
        pltpu.make_async_copy(height_hbm, heat_in.at[1], load_sem.at[2]),
        pltpu.make_async_copy(angle_hbm, heat_in.at[2], load_sem.at[3]),
    ]
    for load in small:
        load.start()
    top_load = pltpu.make_async_copy(bond_hbm.at[2, planes - 1], bond_top, load_sem.at[4])
    top_load.start()
    plane_order = [far_plane, near_plane] + list(range(2, planes))
    for plane in plane_order:
        spin_load(plane).start()
    for load in loads:
        load.start()

    lane = lax.broadcasted_iota(jnp.int32, (half, columns), 1) % 2
    lane_chunk = lax.broadcasted_iota(jnp.int32, (chunk, columns), 1) % 2
    def lane_piece(size):
        return lax.broadcasted_iota(jnp.int32, (size, columns), 1) % 2

    for load in small:
        load.wait()
    swapped = bits_ref[0] != 0

    def order_of(slot):
        other = 1 - slot
        return jnp.where(swapped, order_ref[other], order_ref[slot])

    def beta_of(slot):
        other = 1 - slot
        return jnp.where(swapped, beta_ref[other], beta_ref[slot])

    def parity(slot, plane):
        return lax.rem(me * planes + plane + order_of(slot), 2)

    for slot in (0, 1):
        meta[slot, 0:1] = jnp.full((1, columns), beta_of(slot), jnp.float32)
        meta[slot, 1:2] = jnp.full((1, columns), order_of(slot), jnp.int32).astype(jnp.float32)
        meta[slot, 2:3] = jnp.full((1, columns), bits_ref[1], jnp.int32).astype(jnp.float32)

    def halo(step, slot, down, rows_at, part):
        return pltpu.make_async_remote_copy(
            src_ref=state.at[step, slot, jnp.where(down, 1, planes), :, rows_at],
            dst_ref=state.at[step, slot, jnp.where(down, planes + 1, 0), :, rows_at],
            send_sem=send_sem.at[slot, part],
            recv_sem=recv_sem.at[2 if isinstance(step, int) and step == got else lax.rem(step, 2), slot, part],
            device_id={"gz": jnp.where(down, lower, upper)},
            device_id_type=MESH,
        )

    def far_out(step, slot, part):
        return halo(step, slot, far_low, pl.ds(PAD + part * piece, piece), part)

    def far_in(step, slot, part):
        return halo(step, slot, ~far_low, pl.ds(PAD + part * piece, piece), part)

    def near_out(step, slot):
        return halo(step, slot, ~far_low, main, CHUNKS)

    def near_in(step, slot):
        return halo(step, slot, far_low, main, CHUNKS)

    bond_up = pltpu.make_async_remote_copy(
        src_ref=bond_top,
        dst_ref=bond_halo,
        send_sem=bond_send,
        recv_sem=bond_recv,
        device_id={"gz": upper},
        device_id_type=MESH,
    )

    def along_temp(source, target, send, recv, slot):
        return pltpu.make_async_remote_copy(
            src_ref=source,
            dst_ref=target,
            send_sem=send,
            recv_sem=recv,
            device_id={"temp": temp_towards(slot)},
            device_id_type=MESH,
        )

    def meta_copy(slot):
        return along_temp(
            meta.at[slot], meta_got.at[1 - slot], meta_send.at[slot], meta_recv.at[1 - slot], slot
        )

    def draw_copy(slot, plane):
        return along_temp(
            draws.at[slot, plane],
            draws_got.at[1 - slot, plane],
            draw_send.at[slot],
            draw_recv.at[1 - slot],
            slot,
        )

    def all_draws(slot):
        return along_temp(
            draws.at[slot], draws_got.at[1 - slot], draw_send.at[slot], draw_recv.at[1 - slot], slot
        )

    def swap_copy(slot, plane):
        return along_temp(
            state.at[HALVES, slot, plane, :, main],
            state.at[got, 1 - slot, plane, :, main],
            swap_send.at[slot],
            swap_recv.at[1 - slot, plane - 1],
            slot,
        )

    def all_swaps(slot):
        return along_temp(
            state.at[HALVES, slot, pl.ds(1, planes), :, main],
            state.at[got, 1 - slot, pl.ds(1, planes), :, main],
            swap_send.at[slot],
            swap_recv.at[0, 0],
            slot,
        )

    def total_copy(slot):
        return along_temp(
            total_sum, total_got.at[1 - slot], total_send.at[slot], total_recv.at[1 - slot], slot
        )

    def share_copy(distance):
        return pltpu.make_async_remote_copy(
            src_ref=share_sum,
            dst_ref=share_got.at[distance - 1],
            send_sem=share_send,
            recv_sem=share_recv,
            device_id={"gz": lax.rem(me + distance, count)},
            device_id_type=MESH,
        )

    all_shares = pltpu.make_async_remote_copy(
        src_ref=share_got,
        dst_ref=share_got,
        send_sem=share_send,
        recv_sem=share_recv,
        device_id={"gz": upper},
        device_id_type=MESH,
    )

    def far_signal(index):
        if index < len(distances):
            for move in (distances[index], count - distances[index]):
                pl.semaphore_signal(
                    far_sem.at[index],
                    inc=1,
                    device_id={"gz": lax.rem(me + move, count)},
                    device_id_type=MESH,
                )

    def far_wait(index):
        if index < len(distances):
            pl.semaphore_wait(far_sem.at[index], 2)

    even_rows = pl.ds(0, half, stride=2)
    odd_rows = pl.ds(1, half, stride=2)

    def wrap_rows(step, slot, plane):
        for part in range(3):
            state[step, slot, plane, part, PAD - 1 : PAD] = state[
                step, slot, plane, part, PAD + half - 1 : PAD + half
            ]
            state[step, slot, plane, part, PAD + half : PAD + half + 1] = state[
                step, slot, plane, part, PAD : PAD + 1
            ]

    def pack_spins(plane):
        for part in range(3):
            pairs = [
                (
                    spin_in[r, part, plane - 1, even_rows, :],
                    spin_in[r, part, plane - 1, odd_rows, :],
                )
                for r in (0, 1)
            ]
            for slot in (0, 1):
                even = jnp.where(swapped, pairs[1 - slot][0], pairs[slot][0])
                odd = jnp.where(swapped, pairs[1 - slot][1], pairs[slot][1])
                mask = lane == parity(slot, plane - 1)
                state[0, slot, plane, part, main] = jnp.where(mask, even, odd)
                state[1, slot, plane, part, main] = jnp.where(mask, odd, even)
        for slot in (0, 1):
            wrap_rows(1, slot, plane)

    def first_copy(slot, down, rows_at, part):
        return pltpu.make_async_remote_copy(
            src_ref=state.at[jnp.where(down, 1, 0), slot, jnp.where(down, 1, 0), :, rows_at],
            dst_ref=state.at[1, slot, jnp.where(down, planes + 1, 0), :, rows_at],
            send_sem=send_sem.at[slot, part],
            recv_sem=recv_sem.at[1, slot, part],
            device_id={"gz": jnp.where(down, lower, upper)},
            device_id_type=MESH,
        )

    def stage_products():
        even, odd = bond_top[even_rows, :], bond_top[odd_rows, :]
        for slot in (0, 1):
            bond = jnp.where(lane == parity(slot, planes - 1), odd, even)
            for part in range(3):
                state[0, slot, 0, part, main] = bond * state[1, slot, planes, part, main]

    pl.semaphore_wait(barrier, 2 + has(0).astype(jnp.int32) + has(1).astype(jnp.int32))
    top_load.wait()
    spin_load(far_plane).wait()
    pack_spins(far_plane)

    @pl.when(~far_low)
    def _():
        stage_products()

    for slot in (0, 1):
        for part in range(CHUNKS):
            first_copy(slot, far_low, pl.ds(PAD + part * piece, piece), part).start()
    spin_load(near_plane).wait()
    pack_spins(near_plane)

    @pl.when(far_low)
    def _():
        stage_products()

    for slot in (0, 1):
        first_copy(slot, ~far_low, main, CHUNKS).start()

        @pl.when(has(slot))
        def _(slot=slot):
            meta_copy(slot).start()

        @pl.when(~has(slot))
        def _(slot=slot):
            meta_got[slot] = jnp.zeros((8, columns), jnp.float32)

    bond_up.start()

    def pack_inner(plane, _):
        spin_load(plane).wait()
        pack_spins(plane)
        return 0

    lax.fori_loop(2, planes, pack_inner, 0)
    loads[0].wait()

    def pack_bonds(plane, _):
        even, odd = bond_in[0, plane, even_rows, :], bond_in[0, plane, odd_rows, :]
        first = jnp.where(lane == 0, even, odd)
        second = jnp.where(lane == 0, odd, even)
        bond_x[0, plane, 0] = first
        bond_x[1, plane, 0] = second
        bond_x[0, plane, 1] = pltpu.roll(second, 1, 1)
        bond_x[1, plane, 1] = pltpu.roll(first, 1, 1)
        even, odd = bond_in[1, plane, even_rows, :], bond_in[1, plane, odd_rows, :]
        before = pltpu.roll(odd, 1, 0)
        bond_ys[plane] = even
        bond_yo[0, plane] = jnp.where(lane == 0, before, odd)
        bond_yo[1, plane] = jnp.where(lane == 0, odd, before)
        even, odd = bond_in[2, plane, even_rows, :], bond_in[2, plane, odd_rows, :]
        bond_z[0, plane + 1] = jnp.where(lane == 0, even, odd)
        bond_z[1, plane + 1] = jnp.where(lane == 0, odd, even)
        return 0

    lax.fori_loop(0, planes, pack_bonds, 0)

    def pack_heat(slot, plane):
        side = 1 - slot
        mask = lane_chunk == parity(slot, plane)
        for start in range(0, half, chunk):
            here = pl.ds(start, chunk)
            even_here = pl.ds(2 * start, chunk, stride=2)
            odd_here = pl.ds(2 * start + 1, chunk, stride=2)
            packed = []
            for kind in range(3):
                even = jnp.where(
                    swapped,
                    heat_in[kind, side, plane, even_here, :],
                    heat_in[kind, slot, plane, even_here, :],
                )
                odd = jnp.where(
                    swapped,
                    heat_in[kind, side, plane, odd_here, :],
                    heat_in[kind, slot, plane, odd_here, :],
                )
                packed.append((jnp.where(mask, even, odd), jnp.where(mask, odd, even)))
                draws[slot, plane, kind, here] = packed[kind][1]
            for colour in (0, 1):
                level, height, angle = (draw[colour] for draw in packed)
                across = jnp.sqrt(jnp.maximum(1.0 - height * height, 0.0))
                cosine, sine = cos_sin(angle)
                trial[slot, colour, plane, 0, here] = level
                trial[slot, colour, plane, 1, here] = across * cosine
                trial[slot, colour, plane, 2, here] = across * sine
                trial[slot, colour, plane, 3, here] = height

    def bonds_of(pattern, plane, start, size=chunk):
        here = pl.ds(start, size)
        return (
            bond_x[pattern, plane - 1, 0, here],
            bond_x[pattern, plane - 1, 1, here],
            bond_ys[plane - 1, here],
            bond_yo[pattern, plane - 1, here],
            bond_z[pattern, plane, here],
            bond_z[pattern, plane - 1, here],
        )

    def pulls(step, slot, plane, bonds, mask, start, size=chunk):
        east, west, near, far, above, below = bonds
        at = pl.ds(PAD + start, size)
        out = []
        for part in range(3):
            centre = state[step, slot, plane, part, at]
            other = jnp.where(
                mask,
                state[step, slot, plane, part, pl.ds(PAD + start - 1, size)],
                state[step, slot, plane, part, pl.ds(PAD + start + 1, size)],
            )
            pulled = east * pltpu.roll(centre, columns - 1, 1) + west * pltpu.roll(centre, 1, 1)
            pulled = pulled + near * centre + far * other
            pulled = pulled + above * state[step, slot, plane + 1, part, at]
            pulled = pulled + below * state[step, slot, plane - 1, part, at]
            out.append(pulled)
        return out

    def dot(first, second):
        return first[0] * second[0] + first[1] * second[1] + first[2] * second[2]

    def colour_of(step, slot, plane):
        return lax.rem(parity(slot, plane - 1) + step + 1, 2)

    def relax_rows(step, slot, plane, start, size):
        pattern = colour_of(step, slot, plane)
        at = pl.ds(PAD + start, size)
        bonds = bonds_of(pattern, plane, start, size)
        pulled = pulls(step, slot, plane, bonds, lane_piece(size) == pattern, start, size)
        old = [state[step - 1, slot, plane, part, at] for part in range(3)]
        scale = 2.0 * dot(old, pulled) / jnp.maximum(dot(pulled, pulled), 0.01)
        for part in range(3):
            state[step + 1, slot, plane, part, at] = scale * pulled[part] - old[part]
        return 0

    def heated(pulled, beta, level, draw):
        square = jnp.maximum(dot(pulled, pulled), 0.01)
        inverse = lax.rsqrt(square)
        reach = beta * (square * inverse)
        axis = [part * inverse for part in pulled]
        cosine = 1.0 + jnp.log((1.0 - level) + level * jnp.exp(-2.0 * reach)) / reach
        along = dot(draw, axis)
        tangent = [draw[part] - along * axis[part] for part in range(3)]
        norm = lax.rsqrt(jnp.maximum(dot(tangent, tangent), 0.0001))
        side = jnp.sqrt(jnp.maximum(1.0 - cosine * cosine, 0.0)) * norm
        return [cosine * axis[part] + side * tangent[part] for part in range(3)]

    def heat_rows(step, slot, plane, start, size):
        colour = step - OR_HALVES - 1
        pattern = colour_of(step, slot, plane)
        at = pl.ds(PAD + start, size)
        here = pl.ds(start, size)
        bonds = bonds_of(pattern, plane, start, size)
        pulled = pulls(step, slot, plane, bonds, lane_piece(size) == pattern, start, size)
        level = trial[slot, colour, plane - 1, 0, here]
        draw = [trial[slot, colour, plane - 1, part, here] for part in (1, 2, 3)]
        fresh = heated(pulled, beta_of(slot), level, draw)
        for part in range(3):
            state[step + 1, slot, plane, part, at] = fresh[part]
        return jnp.sum(dot(fresh, pulled).reshape(-1, 8, columns), axis=0)

    def whole_plane(step, slot, plane, rows_of):
        total = 0
        for start in range(0, half, chunk):
            total = total + rows_of(step, slot, plane, start, chunk)
        wrap_rows(step + 1, slot, plane)
        return total

    def swap_start(slot, plane):
        @pl.when(has(slot))
        def _():
            swap_copy(slot, plane).start()

    def far_rows(step, slot, rows_of, send, swap):
        total = 0
        for part in range(CHUNKS):
            far_in(step, slot, part).wait_recv()
            total = total + rows_of(step, slot, far_plane, part * piece, piece)
            if send:
                far_out(step, slot, part).wait_send()
                far_out(step + 1, slot, part).start()
        wrap_rows(step + 1, slot, far_plane)
        if swap:
            swap_start(slot, far_plane)
        return total

    def near_rows(step, slot, rows_of, send, swap):
        near_in(step, slot).wait_recv()
        total = whole_plane(step, slot, near_plane, rows_of)
        if send:
            near_out(step, slot).wait_send()
            near_out(step + 1, slot).start()
        if swap:
            swap_start(slot, near_plane)
        return total

    def both(body):
        def visit(slot, _):
            body(slot)
            return 0

        lax.fori_loop(0, 2, visit, 0)

    def inner_planes(step, slot, rows_of, swap, initial):
        def visit(plane, total):
            total = total + whole_plane(step, slot, plane, rows_of)
            if swap:
                swap_start(slot, plane)
            return total

        return lax.fori_loop(2, planes, visit, initial)

    zero = jnp.zeros((8, columns), jnp.float32)

    def first_inner(slot, _):
        inner_planes(1, slot, relax_rows, False, 0)
        return 0

    lax.fori_loop(0, 2, first_inner, 0)
    for load in loads[1:]:
        load.wait()

    def fill(visit, _):
        slot = visit // planes
        plane = lax.rem(visit, planes)
        pack_heat(slot, plane)

        @pl.when(has(slot))
        def _():
            draw_copy(slot, plane).start()

        return 0

    lax.fori_loop(0, 2 * planes, fill, 0)
    bond_z[0, 0] = jnp.ones((half, columns), jnp.float32)
    bond_z[1, 0] = jnp.ones((half, columns), jnp.float32)

    def relax_round(step, _):
        both(lambda slot: far_rows(step, slot, relax_rows, True, False))
        both(lambda slot: near_rows(step, slot, relax_rows, True, False))

        @pl.when(step == 1)
        def _():
            far_signal(0)
            bond_up.wait_recv()
            even, odd = bond_halo[even_rows, :], bond_halo[odd_rows, :]
            bond_z[0, 0] = jnp.where(lane == 0, even, odd)
            bond_z[1, 0] = jnp.where(lane == 0, odd, even)

        @pl.when(step == 2)
        def _():
            far_wait(0)
            far_signal(1)

        both(lambda slot: inner_planes(step + 1, slot, relax_rows, False, 0))
        return 0

    lax.fori_loop(1, OR_HALVES, relax_round, 0)
    both(lambda slot: far_rows(OR_HALVES, slot, relax_rows, True, False))
    both(lambda slot: near_rows(OR_HALVES, slot, relax_rows, True, False))
    far_wait(1)
    far_signal(2)
    both(lambda slot: inner_planes(OR_HALVES + 1, slot, heat_rows, True, zero))

    both(lambda slot: far_rows(OR_HALVES + 1, slot, heat_rows, True, True))
    both(lambda slot: near_rows(OR_HALVES + 1, slot, heat_rows, True, True))

    def inner_gain(slot):
        gains[slot] = inner_planes(OR_HALVES + 2, slot, heat_rows, False, zero)

    def far_gain(slot):
        gains[slot] = gains[slot] + far_rows(OR_HALVES + 2, slot, heat_rows, False, False)

    def near_gain(slot):
        gain = gains[slot] + near_rows(OR_HALVES + 2, slot, heat_rows, False, False)
        share_sum[pl.ds(slot, 1), :] = jnp.sum(gain, axis=0, keepdims=True)

    both(inner_gain)
    both(far_gain)
    both(near_gain)
    far_wait(2)

    def pass_far(slot):
        for part in range(CHUNKS):
            far_out(HALVES, slot, part).wait_send()

        @pl.when(has(slot))
        def _():
            swap_copy(1 - slot, far_plane).wait_recv()
            for part in range(CHUNKS):
                far_out(got, slot, part).start()
            wrap_rows(got, slot, far_plane)

    share_copy(count // 2).start()

    def give_share(index, _):
        share_copy(count // 2 - index).start()
        share_copy(count // 2 + index).start()
        return 0

    lax.fori_loop(1, count // 2, give_share, 0, unroll=True)

    def pass_near(slot, _):
        near_out(HALVES, slot).wait_send()

        @pl.when(has(slot))
        def _():
            swap_copy(1 - slot, near_plane).wait_recv()
            near_out(got, slot).start()
            wrap_rows(got, slot, near_plane)

        return 0

    pass_far(1)
    pass_far(0)
    lax.fori_loop(0, 2, pass_near, 0)
    for slot in (0, 1):

        @pl.when(has(slot))
        def _(slot=slot):
            all_draws(1 - slot).wait_recv()
            meta_copy(1 - slot).wait_recv()

    def prepare(visit, _):
        slot = visit // planes
        plane = lax.rem(visit, planes)
        for start in range(0, half, chunk):
            here = pl.ds(start, chunk)
            level, height, angle = (draws_got[slot, plane, kind, here] for kind in range(3))
            across = jnp.sqrt(jnp.maximum(1.0 - height * height, 0.0))
            cosine, sine = cos_sin(angle)
            trial_got[slot, plane, 0, here] = level
            trial_got[slot, plane, 1, here] = across * cosine
            trial_got[slot, plane, 2, here] = across * sine
            trial_got[slot, plane, 3, here] = height
        return 0

    lax.fori_loop(0, 2 * planes, prepare, 0)

    taking = [
        (meta_got[0, 2:3] > 0.5) & (here_temp > 0),
        jnp.full((1, columns), bits_ref[1], jnp.int32) * jnp.where(here_temp < temps - 1, 1, 0) > 0,
    ]

    def finish_plane(slot, plane):
        take = jnp.broadcast_to(taking[slot], (chunk, columns))
        flip = jnp.broadcast_to(meta_got[slot, 1:2] > 0.5, (chunk, columns))
        beta = meta_got[slot, 0:1]
        base = lax.rem(me * planes + plane - 1, 2)
        first_mask = (lane_chunk == base) ^ flip
        own_mask = lane_chunk == parity(slot, plane - 1)
        unpack_mask = jnp.where(take, first_mask.astype(jnp.int32), own_mask.astype(jnp.int32)) > 0
        for start in range(0, half, chunk):
            at = pl.ds(PAD + start, chunk)
            here = pl.ds(start, chunk)
            plain = bonds_of(1 - base, plane, start)
            other = bonds_of(base, plane, start)
            bonds = [jnp.where(flip, b, a) for a, b in zip(plain, other)]
            pulled = pulls(got, slot, plane, bonds, ~first_mask, start)
            level = trial_got[slot, plane - 1, 0, here]
            draw = [trial_got[slot, plane - 1, part, here] for part in (1, 2, 3)]
            fresh = heated(pulled, beta, level, draw)
            for part in range(3):
                first = jnp.where(
                    take, state[got, slot, plane, part, at], state[HALVES, slot, plane, part, at]
                )
                second = jnp.where(take, fresh[part], state[HALVES + 1, slot, plane, part, at])
                out_ref[slot, part, plane - 1, pl.ds(2 * start, chunk, stride=2), :] = jnp.where(
                    unpack_mask, first, second
                )
                out_ref[slot, part, plane - 1, pl.ds(2 * start + 1, chunk, stride=2), :] = jnp.where(
                    unpack_mask, second, first
                )

    def arrive(visit, _):
        slot = visit // (planes - 2)
        plane = lax.rem(visit, planes - 2) + 2

        @pl.when(has(slot))
        def _():
            swap_copy(1 - slot, plane).wait_recv()
            wrap_rows(got, slot, plane)

        return 0

    lax.fori_loop(0, 2 * (planes - 2), arrive, 0)

    def finish_inner(plane, _):
        for slot in (0, 1):
            finish_plane(slot, plane)
        return 0

    lax.fori_loop(2, planes, finish_inner, 0)

    all_shares.wait_recv()
    total_sum[...] = share_sum[...] + jnp.sum(share_got[...], axis=0)
    for slot in (0, 1):

        @pl.when(has(slot))
        def _(slot=slot):
            total_copy(slot).start()

    def finish_outer(index, _):
        for slot in (0, 1):

            @pl.when((index == 0) & has(slot))
            def _(slot=slot):
                near_in(got, slot).wait_recv()

            @pl.when((index == 1) & has(slot))
            def _(slot=slot):
                for part in range(CHUNKS):
                    far_in(got, slot, part).wait_recv()

        plane = jnp.where(index == 0, near_plane, far_plane)
        for slot in (0, 1):
            finish_plane(slot, plane)
        return 0

    lax.fori_loop(0, 2, finish_outer, 0)

    bond_up.wait_send()
    all_shares.wait_send()
    for slot in (0, 1):

        @pl.when(has(slot))
        def _(slot=slot):
            meta_copy(slot).wait_send()
            all_draws(slot).wait_send()
            all_swaps(slot).wait_send()
            for part in range(CHUNKS):
                far_out(got, slot, part).wait_send()
            near_out(got, slot).wait_send()

    for slot in (0, 1):

        @pl.when(has(slot))
        def _(slot=slot):
            total_copy(1 - slot).wait_recv()

    sites = float(columns * rows * planes * count)
    values = [
        jnp.where(taking[slot], total_got[slot, 1 - slot : 2 - slot], total_sum[slot : slot + 1])
        for slot in (0, 1)
    ]
    sums = [-jnp.sum(value, axis=1, keepdims=True) / sites for value in values]
    spot = lax.broadcasted_iota(jnp.int32, (1, columns), 1)
    energy_ref[...] = jnp.where(spot == 0, sums[0], sums[1])

    for slot in (0, 1):

        @pl.when(has(slot))
        def _(slot=slot):
            total_copy(slot).wait_send()


def on_device(
    spin_state,
    couplings,
    inverse_temps,
    colour_order,
    heat_level,
    heat_height,
    heat_angle,
    swap_bits,
):
    slots, parts, planes, rows, columns = spin_state.shape
    half = rows // 2
    count = lax.axis_size("gz")
    f32 = jnp.float32
    dma = pltpu.SemaphoreType.DMA
    any_space = pl.BlockSpec(memory_space=pl.ANY)
    vmem = pl.BlockSpec(memory_space=pltpu.VMEM)
    steps = HALVES + 3
    spins, energies = pl.pallas_call(
        step_kernel,
        out_shape=(
            pltpu.VMEM(spin_state.shape, f32),
            pltpu.VMEM((1, columns), f32),
        ),
        in_specs=[any_space] * 8,
        out_specs=(vmem, vmem),
        scratch_shapes=[
            pltpu.SMEM((slots,), f32),
            pltpu.SMEM((slots,), jnp.int32),
            pltpu.SMEM((slots,), jnp.int32),
            pltpu.VMEM(spin_state.shape, f32),
            pltpu.VMEM(couplings.shape, f32),
            pltpu.VMEM((3,) + heat_level.shape, f32),
            pltpu.VMEM((steps, slots, planes + 2, 3, half + 2 * PAD, columns), f32),
            pltpu.VMEM((2, planes, 2, half, columns), f32),
            pltpu.VMEM((2, planes, half, columns), f32),
            pltpu.VMEM((planes, half, columns), f32),
            pltpu.VMEM((2, planes + 1, half, columns), f32),
            pltpu.VMEM((rows, columns), f32),
            pltpu.VMEM((rows, columns), f32),
            pltpu.VMEM((slots, 2, planes, 4, half, columns), f32),
            pltpu.VMEM((slots, 8, columns), f32),
            pltpu.VMEM((slots, 8, columns), f32),
            pltpu.VMEM((slots, planes, 3, half, columns), f32),
            pltpu.VMEM((slots, planes, 3, half, columns), f32),
            pltpu.VMEM((slots, planes, 4, half, columns), f32),
            pltpu.VMEM((2, columns), f32),
            pltpu.VMEM((count - 1, 2, columns), f32),
            pltpu.VMEM((2, columns), f32),
            pltpu.VMEM((slots, 2, columns), f32),
            pltpu.VMEM((slots, 8, columns), f32),
            dma((3,)),
            dma((planes,)),
            dma((5,)),
            dma,
            dma,
            dma((slots, CHUNKS + 1)),
            dma((3, slots, CHUNKS + 1)),
            dma((slots,)),
            dma((slots,)),
            dma((slots,)),
            dma((slots,)),
            dma((slots,)),
            dma((slots, planes)),
            dma,
            dma,
            dma((slots,)),
            dma((slots,)),
            pltpu.SemaphoreType.REGULAR((max(1, len(far_distances(count))),)),
        ],
        compiler_params=pltpu.CompilerParams(
            collective_id=0, has_side_effects=True, vmem_limit_bytes=56 * 1024 * 1024
        ),
        name="replica_step",
    )(
        spin_state,
        couplings,
        heat_level,
        heat_height,
        heat_angle,
        inverse_temps,
        colour_order,
        swap_bits,
    )
    return (spins, energies[0, :slots])


def solution(mesh):
    return jax.shard_map(
        on_device,
        mesh=mesh,
        in_specs=(
            P(("group", "temp"), None, "gz", None, None),
            P(None, ("group", "gz"), None, None),
            P(("group", "temp")),
            P(("group", "temp")),
            P(("group", "temp"), "gz", None, None),
            P(("group", "temp"), "gz", None, None),
            P(("group", "temp"), "gz", None, None),
            P(("group", "temp")),
        ),
        out_specs=(P(("group", "temp"), None, "gz", None, None), P(("group", "temp"))),
        check_vma=False,
    )
```

```python
import functools

import jax
import jax.numpy as jnp
from jax import lax
from jax.experimental import pallas as pl
from jax.experimental.pallas import tpu as pltpu
from jax.sharding import PartitionSpec as P

OR_SWEEPS = 2
OR_HALVES = 2 * OR_SWEEPS
HALVES = OR_HALVES + 2
PAD = 8
CHUNKS = 4
MESH = pl.DeviceIdType.MESH

SIN_TERMS = (
    1.0,
    -1.0 / 6,
    1.0 / 120,
    -1.0 / 5040,
    1.0 / 362880,
    -1.0 / 39916800,
    1.0 / 6227020800,
)
COS_TERMS = (
    1.0,
    -1.0 / 2,
    1.0 / 24,
    -1.0 / 720,
    1.0 / 40320,
    -1.0 / 3628800,
    1.0 / 479001600,
    -1.0 / 87178291200,
)


def series(terms, square):
    total = jnp.full_like(square, terms[-1])
    for term in terms[-2::-1]:
        total = total * square + term
    return total


def cos_sin(angle):
    half = 0.5 * angle
    square = half * half
    sine = half * series(SIN_TERMS, square)
    cosine = series(COS_TERMS, square)
    return 1.0 - 2.0 * sine * sine, 2.0 * sine * cosine


def far_distances(count):
    distances, known = [], 2
    while known < count // 2:
        distances.append(known)
        known *= 2
    return distances


def step_kernel(
    spin_hbm,
    bond_hbm,
    level_hbm,
    height_hbm,
    angle_hbm,
    beta_hbm,
    order_hbm,
    bits_hbm,
    out_ref,
    energy_ref,
    beta_ref,
    order_ref,
    bits_ref,
    spin_in,
    bond_in,
    heat_in,
    state,
    bond_x,
    bond_yo,
    bond_ys,
    bond_z,
    bond_halo,
    bond_top,
    trial,
    meta,
    meta_got,
    draws,
    draws_got,
    trial_got,
    share_sum,
    share_got,
    total_sum,
    total_got,
    gains,
    small_sem,
    spin_sem,
    load_sem,
    bond_send,
    bond_recv,
    send_sem,
    recv_sem,
    meta_send,
    meta_recv,
    draw_send,
    draw_recv,
    swap_send,
    swap_recv,
    share_send,
    share_recv,
    total_send,
    total_recv,
    far_sem,
):
    planes, rows, columns = spin_in.shape[2:]
    half = rows // 2
    piece = half // CHUNKS
    chunk = min(32, half)
    me = lax.axis_index("gz")
    count = lax.axis_size("gz")
    upper = lax.rem(me + 1, count)
    lower = lax.rem(me + count - 1, count)
    here_temp = lax.axis_index("temp")
    temps = lax.axis_size("temp")
    main = pl.ds(PAD, half)
    got = HALVES + 2
    distances = far_distances(count)

    def temp_towards(slot):
        return lax.rem(here_temp + 2 * slot - 1 + temps, temps)

    def has(slot):
        return (here_temp + slot > 0) & (here_temp + slot < temps)

    barrier = pltpu.get_barrier_semaphore()
    for neighbour in (lower, upper):
        pl.semaphore_signal(
            barrier, inc=1, device_id={"gz": neighbour}, device_id_type=MESH
        )
    for slot in (0, 1):

        @pl.when(has(slot))
        def _(slot=slot):
            pl.semaphore_signal(
                barrier, inc=1, device_id={"temp": temp_towards(slot)}, device_id_type=MESH
            )

    far_low = lax.rem(me, 2) == 0
    far_plane = jnp.where(far_low, 1, planes)
    near_plane = jnp.where(far_low, planes, 1)

    small = [
        pltpu.make_async_copy(source, target, small_sem.at[index])
        for index, (source, target) in enumerate(
            ((bits_hbm, bits_ref), (order_hbm, order_ref), (beta_hbm, beta_ref))
        )
    ]

    def spin_load(plane):
        return pltpu.make_async_copy(
            spin_hbm.at[:, :, plane - 1], spin_in.at[:, :, plane - 1], spin_sem.at[plane - 1]
        )

    loads = [
        pltpu.make_async_copy(bond_hbm, bond_in, load_sem.at[0]),
        pltpu.make_async_copy(level_hbm, heat_in.at[0], load_sem.at[1]),
        pltpu.make_async_copy(height_hbm, heat_in.at[1], load_sem.at[2]),
        pltpu.make_async_copy(angle_hbm, heat_in.at[2], load_sem.at[3]),
    ]
    for load in small:
        load.start()
    top_load = pltpu.make_async_copy(bond_hbm.at[2, planes - 1], bond_top, load_sem.at[4])
    top_load.start()
    plane_order = [far_plane, near_plane] + list(range(2, planes))
    for plane in plane_order:
        spin_load(plane).start()
    for load in loads:
        load.start()

    lane = lax.broadcasted_iota(jnp.int32, (half, columns), 1) % 2
    lane_chunk = lax.broadcasted_iota(jnp.int32, (chunk, columns), 1) % 2
    def lane_piece(size):
        return lax.broadcasted_iota(jnp.int32, (size, columns), 1) % 2

    for load in small:
        load.wait()
    swapped = bits_ref[0] != 0

    def order_of(slot):
        other = 1 - slot
        return jnp.where(swapped, order_ref[other], order_ref[slot])

    def beta_of(slot):
        other = 1 - slot
        return jnp.where(swapped, beta_ref[other], beta_ref[slot])

    def parity(slot, plane):
        return lax.rem(me * planes + plane + order_of(slot), 2)

    for slot in (0, 1):
        meta[slot, 0:1] = jnp.full((1, columns), beta_of(slot), jnp.float32)
        meta[slot, 1:2] = jnp.full((1, columns), order_of(slot), jnp.int32).astype(jnp.float32)
        meta[slot, 2:3] = jnp.full((1, columns), bits_ref[1], jnp.int32).astype(jnp.float32)

    def halo(step, slot, down, rows_at, part):
        return pltpu.make_async_remote_copy(
            src_ref=state.at[step, slot, jnp.where(down, 1, planes), :, rows_at],
            dst_ref=state.at[step, slot, jnp.where(down, planes + 1, 0), :, rows_at],
            send_sem=send_sem.at[slot, part],
            recv_sem=recv_sem.at[1 if isinstance(step, int) and step == got else lax.rem(step, 2), slot, part],
            device_id={"gz": jnp.where(down, lower, upper)},
            device_id_type=MESH,
        )

    def far_out(step, slot, part):
        return halo(step, slot, far_low, pl.ds(PAD + part * piece, piece), part)

    def far_in(step, slot, part):
        return halo(step, slot, ~far_low, pl.ds(PAD + part * piece, piece), part)

    def near_out(step, slot):
        return halo(step, slot, ~far_low, main, CHUNKS)

    def near_in(step, slot):
        return halo(step, slot, far_low, main, CHUNKS)

    bond_up = pltpu.make_async_remote_copy(
        src_ref=bond_top,
        dst_ref=bond_halo,
        send_sem=bond_send,
        recv_sem=bond_recv,
        device_id={"gz": upper},
        device_id_type=MESH,
    )

    def along_temp(source, target, send, recv, slot):
        return pltpu.make_async_remote_copy(
            src_ref=source,
            dst_ref=target,
            send_sem=send,
            recv_sem=recv,
            device_id={"temp": temp_towards(slot)},
            device_id_type=MESH,
        )

    def meta_copy(slot):
        return along_temp(
            meta.at[slot], meta_got.at[1 - slot], meta_send.at[slot], meta_recv.at[1 - slot], slot
        )

    def draw_copy(slot, plane):
        return along_temp(
            draws.at[slot, plane],
            draws_got.at[1 - slot, plane],
            draw_send.at[slot],
            draw_recv.at[1 - slot],
            slot,
        )

    def all_draws(slot):
        return along_temp(
            draws.at[slot], draws_got.at[1 - slot], draw_send.at[slot], draw_recv.at[1 - slot], slot
        )

    def swap_copy(slot, plane):
        return along_temp(
            state.at[HALVES, slot, plane, :, main],
            state.at[got, 1 - slot, plane, :, main],
            swap_send.at[slot],
            swap_recv.at[1 - slot, plane - 1],
            slot,
        )

    def all_swaps(slot):
        return along_temp(
            state.at[HALVES, slot, pl.ds(1, planes), :, main],
            state.at[got, 1 - slot, pl.ds(1, planes), :, main],
            swap_send.at[slot],
            swap_recv.at[0, 0],
            slot,
        )

    def total_copy(slot):
        return along_temp(
            total_sum, total_got.at[1 - slot], total_send.at[slot], total_recv.at[1 - slot], slot
        )

    def share_copy(distance):
        return pltpu.make_async_remote_copy(
            src_ref=share_sum,
            dst_ref=share_got.at[distance - 1],
            send_sem=share_send,
            recv_sem=share_recv,
            device_id={"gz": lax.rem(me + distance, count)},
            device_id_type=MESH,
        )

    all_shares = pltpu.make_async_remote_copy(
        src_ref=share_got,
        dst_ref=share_got,
        send_sem=share_send,
        recv_sem=share_recv,
        device_id={"gz": upper},
        device_id_type=MESH,
    )

    def far_signal(index):
        if index < len(distances):
            for move in (distances[index], count - distances[index]):
                pl.semaphore_signal(
                    far_sem.at[index],
                    inc=1,
                    device_id={"gz": lax.rem(me + move, count)},
                    device_id_type=MESH,
                )

    def far_wait(index):
        if index < len(distances):
            pl.semaphore_wait(far_sem.at[index], 2)

    even_rows = pl.ds(0, half, stride=2)
    odd_rows = pl.ds(1, half, stride=2)

    def wrap_rows(step, slot, plane):
        for part in range(3):
            state[step, slot, plane, part, PAD - 1 : PAD] = state[
                step, slot, plane, part, PAD + half - 1 : PAD + half
            ]
            state[step, slot, plane, part, PAD + half : PAD + half + 1] = state[
                step, slot, plane, part, PAD : PAD + 1
            ]

    def pack_spins(plane):
        for part in range(3):
            pairs = [
                (
                    spin_in[r, part, plane - 1, even_rows, :],
                    spin_in[r, part, plane - 1, odd_rows, :],
                )
                for r in (0, 1)
            ]
            for slot in (0, 1):
                even = jnp.where(swapped, pairs[1 - slot][0], pairs[slot][0])
                odd = jnp.where(swapped, pairs[1 - slot][1], pairs[slot][1])
                mask = lane == parity(slot, plane - 1)
                state[0, slot, plane, part, main] = jnp.where(mask, even, odd)
                state[1, slot, plane, part, main] = jnp.where(mask, odd, even)
        for slot in (0, 1):
            wrap_rows(1, slot, plane)

    def first_copy(slot, down, rows_at, part):
        return pltpu.make_async_remote_copy(
            src_ref=state.at[jnp.where(down, 1, 0), slot, jnp.where(down, 1, 0), :, rows_at],
            dst_ref=state.at[1, slot, jnp.where(down, planes + 1, 0), :, rows_at],
            send_sem=send_sem.at[slot, part],
            recv_sem=recv_sem.at[1, slot, part],
            device_id={"gz": jnp.where(down, lower, upper)},
            device_id_type=MESH,
        )

    def stage_products():
        even, odd = bond_top[even_rows, :], bond_top[odd_rows, :]
        for slot in (0, 1):
            bond = jnp.where(lane == parity(slot, planes - 1), odd, even)
            for part in range(3):
                state[0, slot, 0, part, main] = bond * state[1, slot, planes, part, main]

    pl.semaphore_wait(barrier, 2 + has(0).astype(jnp.int32) + has(1).astype(jnp.int32))
    top_load.wait()
    spin_load(far_plane).wait()
    pack_spins(far_plane)

    @pl.when(~far_low)
    def _():
        stage_products()

    for slot in (0, 1):
        for part in range(CHUNKS):
            first_copy(slot, far_low, pl.ds(PAD + part * piece, piece), part).start()
    spin_load(near_plane).wait()
    pack_spins(near_plane)

    @pl.when(far_low)
    def _():
        stage_products()

    for slot in (0, 1):
        first_copy(slot, ~far_low, main, CHUNKS).start()

        @pl.when(has(slot))
        def _(slot=slot):
            meta_copy(slot).start()

        @pl.when(~has(slot))
        def _(slot=slot):
            meta_got[slot] = jnp.zeros((8, columns), jnp.float32)

    bond_up.start()

    def pack_inner(plane, _):
        spin_load(plane).wait()
        pack_spins(plane)
        return 0

    lax.fori_loop(2, planes, pack_inner, 0)
    loads[0].wait()

    def pack_bonds(plane, _):
        even, odd = bond_in[0, plane, even_rows, :], bond_in[0, plane, odd_rows, :]
        first = jnp.where(lane == 0, even, odd)
        second = jnp.where(lane == 0, odd, even)
        bond_x[0, plane, 0] = first
        bond_x[1, plane, 0] = second
        bond_x[0, plane, 1] = pltpu.roll(second, 1, 1)
        bond_x[1, plane, 1] = pltpu.roll(first, 1, 1)
        even, odd = bond_in[1, plane, even_rows, :], bond_in[1, plane, odd_rows, :]
        before = pltpu.roll(odd, 1, 0)
        bond_ys[plane] = even
        bond_yo[0, plane] = jnp.where(lane == 0, before, odd)
        bond_yo[1, plane] = jnp.where(lane == 0, odd, before)
        even, odd = bond_in[2, plane, even_rows, :], bond_in[2, plane, odd_rows, :]
        bond_z[0, plane + 1] = jnp.where(lane == 0, even, odd)
        bond_z[1, plane + 1] = jnp.where(lane == 0, odd, even)
        return 0

    lax.fori_loop(0, planes, pack_bonds, 0)

    def pack_heat(slot, plane):
        side = 1 - slot
        mask = lane_chunk == parity(slot, plane)
        for start in range(0, half, chunk):
            here = pl.ds(start, chunk)
            even_here = pl.ds(2 * start, chunk, stride=2)
            odd_here = pl.ds(2 * start + 1, chunk, stride=2)
            packed = []
            for kind in range(3):
                even = jnp.where(
                    swapped,
                    heat_in[kind, side, plane, even_here, :],
                    heat_in[kind, slot, plane, even_here, :],
                )
                odd = jnp.where(
                    swapped,
                    heat_in[kind, side, plane, odd_here, :],
                    heat_in[kind, slot, plane, odd_here, :],
                )
                packed.append((jnp.where(mask, even, odd), jnp.where(mask, odd, even)))
                draws[slot, plane, kind, here] = packed[kind][1]
            for colour in (0, 1):
                level, height, angle = (draw[colour] for draw in packed)
                across = jnp.sqrt(jnp.maximum(1.0 - height * height, 0.0))
                cosine, sine = cos_sin(angle)
                trial[slot, colour, plane, 0, here] = level
                trial[slot, colour, plane, 1, here] = across * cosine
                trial[slot, colour, plane, 2, here] = across * sine
                trial[slot, colour, plane, 3, here] = height

    def bonds_of(pattern, plane, start, size=chunk):
        here = pl.ds(start, size)
        return (
            bond_x[pattern, plane - 1, 0, here],
            bond_x[pattern, plane - 1, 1, here],
            bond_ys[plane - 1, here],
            bond_yo[pattern, plane - 1, here],
            bond_z[pattern, plane, here],
            bond_z[pattern, plane - 1, here],
        )

    def pulls(step, slot, plane, bonds, mask, start, size=chunk):
        east, west, near, far, above, below = bonds
        at = pl.ds(PAD + start, size)
        out = []
        for part in range(3):
            centre = state[step, slot, plane, part, at]
            other = jnp.where(
                mask,
                state[step, slot, plane, part, pl.ds(PAD + start - 1, size)],
                state[step, slot, plane, part, pl.ds(PAD + start + 1, size)],
            )
            pulled = east * pltpu.roll(centre, columns - 1, 1) + west * pltpu.roll(centre, 1, 1)
            pulled = pulled + near * centre + far * other
            pulled = pulled + above * state[step, slot, plane + 1, part, at]
            pulled = pulled + below * state[step, slot, plane - 1, part, at]
            out.append(pulled)
        return out

    def dot(first, second):
        return first[0] * second[0] + first[1] * second[1] + first[2] * second[2]

    def colour_of(step, slot, plane):
        return lax.rem(parity(slot, plane - 1) + step + 1, 2)

    def relax_rows(step, slot, plane, start, size):
        pattern = colour_of(step, slot, plane)
        at = pl.ds(PAD + start, size)
        bonds = bonds_of(pattern, plane, start, size)
        pulled = pulls(step, slot, plane, bonds, lane_piece(size) == pattern, start, size)
        old = [state[step - 1, slot, plane, part, at] for part in range(3)]
        scale = 2.0 * dot(old, pulled) / jnp.maximum(dot(pulled, pulled), 0.01)
        for part in range(3):
            state[step + 1, slot, plane, part, at] = scale * pulled[part] - old[part]
        return 0

    def heated(pulled, beta, level, draw):
        square = jnp.maximum(dot(pulled, pulled), 0.01)
        inverse = lax.rsqrt(square)
        reach = beta * (square * inverse)
        axis = [part * inverse for part in pulled]
        cosine = 1.0 + jnp.log((1.0 - level) + level * jnp.exp(-2.0 * reach)) / reach
        along = dot(draw, axis)
        tangent = [draw[part] - along * axis[part] for part in range(3)]
        norm = lax.rsqrt(jnp.maximum(dot(tangent, tangent), 0.0001))
        side = jnp.sqrt(jnp.maximum(1.0 - cosine * cosine, 0.0)) * norm
        return [cosine * axis[part] + side * tangent[part] for part in range(3)]

    def heat_rows(step, slot, plane, start, size):
        colour = step - OR_HALVES - 1
        pattern = colour_of(step, slot, plane)
        at = pl.ds(PAD + start, size)
        here = pl.ds(start, size)
        bonds = bonds_of(pattern, plane, start, size)
        pulled = pulls(step, slot, plane, bonds, lane_piece(size) == pattern, start, size)
        level = trial[slot, colour, plane - 1, 0, here]
        draw = [trial[slot, colour, plane - 1, part, here] for part in (1, 2, 3)]
        fresh = heated(pulled, beta_of(slot), level, draw)
        for part in range(3):
            state[step + 1, slot, plane, part, at] = fresh[part]
        return jnp.sum(dot(fresh, pulled).reshape(-1, 8, columns), axis=0)

    def whole_plane(step, slot, plane, rows_of):
        total = 0
        for start in range(0, half, chunk):
            total = total + rows_of(step, slot, plane, start, chunk)
        wrap_rows(step + 1, slot, plane)
        return total

    def swap_start(slot, plane):
        @pl.when(has(slot))
        def _():
            swap_copy(slot, plane).start()

    def far_rows(step, slot, rows_of, send, swap):
        total = 0
        for part in range(CHUNKS):
            far_in(step, slot, part).wait_recv()
            total = total + rows_of(step, slot, far_plane, part * piece, piece)
            if send:
                far_out(step, slot, part).wait_send()
                far_out(step + 1, slot, part).start()
        wrap_rows(step + 1, slot, far_plane)
        if swap:
            swap_start(slot, far_plane)
        return total

    def near_rows(step, slot, rows_of, send, swap):
        near_in(step, slot).wait_recv()
        total = whole_plane(step, slot, near_plane, rows_of)
        if send:
            near_out(step, slot).wait_send()
            near_out(step + 1, slot).start()
        if swap:
            swap_start(slot, near_plane)
        return total

    def both(body):
        def visit(slot, _):
            body(slot)
            return 0

        lax.fori_loop(0, 2, visit, 0)

    def inner_planes(step, slot, rows_of, swap, initial):
        def visit(plane, total):
            total = total + whole_plane(step, slot, plane, rows_of)
            if swap:

                @pl.when(plane == 2)
                def _():
                    swap_start(slot, plane)

            return total

        return lax.fori_loop(2, planes, visit, initial)

    zero = jnp.zeros((8, columns), jnp.float32)

    def first_inner(slot, _):
        inner_planes(1, slot, relax_rows, False, 0)
        return 0

    lax.fori_loop(0, 2, first_inner, 0)
    for load in loads[1:]:
        load.wait()

    def fill(visit, _):
        slot = visit // planes
        plane = lax.rem(visit, planes)
        pack_heat(slot, plane)

        @pl.when(has(slot))
        def _():
            draw_copy(slot, plane).start()

        return 0

    lax.fori_loop(0, 2 * planes, fill, 0)
    bond_z[0, 0] = jnp.ones((half, columns), jnp.float32)
    bond_z[1, 0] = jnp.ones((half, columns), jnp.float32)

    def relax_round(step, _):
        both(lambda slot: far_rows(step, slot, relax_rows, True, False))
        both(lambda slot: near_rows(step, slot, relax_rows, True, False))

        @pl.when(step == 1)
        def _():
            far_signal(0)
            bond_up.wait_recv()
            even, odd = bond_halo[even_rows, :], bond_halo[odd_rows, :]
            bond_z[0, 0] = jnp.where(lane == 0, even, odd)
            bond_z[1, 0] = jnp.where(lane == 0, odd, even)

        @pl.when(step == 2)
        def _():
            far_wait(0)
            far_signal(1)

        both(lambda slot: inner_planes(step + 1, slot, relax_rows, False, 0))
        return 0

    lax.fori_loop(1, OR_HALVES, relax_round, 0)
    both(lambda slot: far_rows(OR_HALVES, slot, relax_rows, True, False))
    both(lambda slot: near_rows(OR_HALVES, slot, relax_rows, True, False))
    far_wait(1)
    far_signal(2)
    both(lambda slot: inner_planes(OR_HALVES + 1, slot, heat_rows, True, zero))

    both(lambda slot: far_rows(OR_HALVES + 1, slot, heat_rows, True, False))
    both(lambda slot: swap_start(slot, far_plane))
    both(lambda slot: near_rows(OR_HALVES + 1, slot, heat_rows, True, True))

    def rest_of_swap(visit, _):
        swap_start(lax.rem(visit, 2), visit // 2 + 3)
        return 0

    lax.fori_loop(0, 2 * (planes - 3), rest_of_swap, 0)

    def inner_gain(slot):
        gains[slot] = inner_planes(OR_HALVES + 2, slot, heat_rows, False, zero)

    def far_gain(slot):
        gains[slot] = gains[slot] + far_rows(OR_HALVES + 2, slot, heat_rows, False, False)

    def near_gain(slot):
        gain = gains[slot] + near_rows(OR_HALVES + 2, slot, heat_rows, False, False)
        share_sum[pl.ds(slot, 1), :] = jnp.sum(gain, axis=0, keepdims=True)

    both(inner_gain)
    both(far_gain)
    both(near_gain)
    far_wait(2)

    def pass_far(slot):
        for part in range(CHUNKS):
            far_out(HALVES, slot, part).wait_send()

        @pl.when(has(slot))
        def _():
            swap_copy(1 - slot, far_plane).wait_recv()
            for part in range(CHUNKS):
                far_out(got, slot, part).start()
            wrap_rows(got, slot, far_plane)

    close = min(3, count // 2 - 1)
    sides = [side for step in range(1, close + 1) for side in (step, count - step)]
    sides.append(count // 2)
    for step in range(count // 2 - 1, close, -1):
        sides += [step, count - step]
    for distance in sides:
        share_copy(distance).start()

    def pass_near(slot, _):
        near_out(HALVES, slot).wait_send()

        @pl.when(has(slot))
        def _():
            swap_copy(1 - slot, near_plane).wait_recv()
            near_out(got, slot).start()
            wrap_rows(got, slot, near_plane)

        return 0

    pass_far(1)
    pass_far(0)
    lax.fori_loop(0, 2, pass_near, 0)
    for slot in (0, 1):

        @pl.when(has(slot))
        def _(slot=slot):
            all_draws(1 - slot).wait_recv()
            meta_copy(1 - slot).wait_recv()

    def prepare(visit, _):
        slot = visit // planes
        plane = lax.rem(visit, planes)
        for start in range(0, half, chunk):
            here = pl.ds(start, chunk)
            level, height, angle = (draws_got[slot, plane, kind, here] for kind in range(3))
            across = jnp.sqrt(jnp.maximum(1.0 - height * height, 0.0))
            cosine, sine = cos_sin(angle)
            trial_got[slot, plane, 0, here] = level
            trial_got[slot, plane, 1, here] = across * cosine
            trial_got[slot, plane, 2, here] = across * sine
            trial_got[slot, plane, 3, here] = height
        return 0

    lax.fori_loop(0, 2 * planes, prepare, 0)

    taking = [
        (meta_got[0, 2:3] > 0.5) & (here_temp > 0),
        jnp.full((1, columns), bits_ref[1], jnp.int32) * jnp.where(here_temp < temps - 1, 1, 0) > 0,
    ]

    def finish_plane(slot, plane):
        take = jnp.broadcast_to(taking[slot], (chunk, columns))
        flip = jnp.broadcast_to(meta_got[slot, 1:2] > 0.5, (chunk, columns))
        beta = meta_got[slot, 0:1]
        base = lax.rem(me * planes + plane - 1, 2)
        first_mask = (lane_chunk == base) ^ flip
        own_mask = lane_chunk == parity(slot, plane - 1)
        unpack_mask = jnp.where(take, first_mask.astype(jnp.int32), own_mask.astype(jnp.int32)) > 0
        for start in range(0, half, chunk):
            at = pl.ds(PAD + start, chunk)
            here = pl.ds(start, chunk)
            plain = bonds_of(1 - base, plane, start)
            other = bonds_of(base, plane, start)
            bonds = [jnp.where(flip, b, a) for a, b in zip(plain, other)]
            pulled = pulls(got, slot, plane, bonds, ~first_mask, start)
            level = trial_got[slot, plane - 1, 0, here]
            draw = [trial_got[slot, plane - 1, part, here] for part in (1, 2, 3)]
            fresh = heated(pulled, beta, level, draw)
            for part in range(3):
                first = jnp.where(
                    take, state[got, slot, plane, part, at], state[HALVES, slot, plane, part, at]
                )
                second = jnp.where(take, fresh[part], state[HALVES + 1, slot, plane, part, at])
                out_ref[slot, part, plane - 1, pl.ds(2 * start, chunk, stride=2), :] = jnp.where(
                    unpack_mask, first, second
                )
                out_ref[slot, part, plane - 1, pl.ds(2 * start + 1, chunk, stride=2), :] = jnp.where(
                    unpack_mask, second, first
                )

    all_shares.wait_recv()
    total_sum[...] = share_sum[...] + jnp.sum(share_got[...], axis=0)
    for slot in (0, 1):

        @pl.when(has(slot))
        def _(slot=slot):
            total_copy(slot).start()

    def arrive(visit, _):
        slot = visit // (planes - 2)
        plane = lax.rem(visit, planes - 2) + 2

        @pl.when(has(slot))
        def _():
            swap_copy(1 - slot, plane).wait_recv()
            wrap_rows(got, slot, plane)

        return 0

    lax.fori_loop(0, 2 * (planes - 2), arrive, 0)

    def finish_inner(plane, _):
        for slot in (0, 1):
            finish_plane(slot, plane)
        return 0

    lax.fori_loop(2, planes, finish_inner, 0)

    def finish_outer(index, _):
        for slot in (0, 1):

            @pl.when((index == 0) & has(slot))
            def _(slot=slot):
                near_in(got, slot).wait_recv()

            @pl.when((index == 1) & has(slot))
            def _(slot=slot):
                for part in range(CHUNKS):
                    far_in(got, slot, part).wait_recv()

        plane = jnp.where(index == 0, near_plane, far_plane)
        for slot in (0, 1):
            finish_plane(slot, plane)
        return 0

    lax.fori_loop(0, 2, finish_outer, 0)

    bond_up.wait_send()
    all_shares.wait_send()
    for slot in (0, 1):

        @pl.when(has(slot))
        def _(slot=slot):
            meta_copy(slot).wait_send()
            all_draws(slot).wait_send()
            all_swaps(slot).wait_send()
            for part in range(CHUNKS):
                far_out(got, slot, part).wait_send()
            near_out(got, slot).wait_send()

    for slot in (0, 1):

        @pl.when(has(slot))
        def _(slot=slot):
            total_copy(1 - slot).wait_recv()

    sites = float(columns * rows * planes * count)
    values = [
        jnp.where(taking[slot], total_got[slot, 1 - slot : 2 - slot], total_sum[slot : slot + 1])
        for slot in (0, 1)
    ]
    sums = [-jnp.sum(value, axis=1, keepdims=True) / sites for value in values]
    spot = lax.broadcasted_iota(jnp.int32, (1, columns), 1)
    energy_ref[...] = jnp.where(spot == 0, sums[0], sums[1])

    for slot in (0, 1):

        @pl.when(has(slot))
        def _(slot=slot):
            total_copy(slot).wait_send()


def on_device(
    spin_state,
    couplings,
    inverse_temps,
    colour_order,
    heat_level,
    heat_height,
    heat_angle,
    swap_bits,
):
    slots, parts, planes, rows, columns = spin_state.shape
    half = rows // 2
    count = lax.axis_size("gz")
    f32 = jnp.float32
    dma = pltpu.SemaphoreType.DMA
    any_space = pl.BlockSpec(memory_space=pl.ANY)
    vmem = pl.BlockSpec(memory_space=pltpu.VMEM)
    steps = HALVES + 3
    spins, energies = pl.pallas_call(
        step_kernel,
        out_shape=(
            pltpu.VMEM(spin_state.shape, f32),
            pltpu.VMEM((1, columns), f32),
        ),
        in_specs=[any_space] * 8,
        out_specs=(vmem, vmem),
        scratch_shapes=[
            pltpu.SMEM((slots,), f32),
            pltpu.SMEM((slots,), jnp.int32),
            pltpu.SMEM((slots,), jnp.int32),
            pltpu.VMEM(spin_state.shape, f32),
            pltpu.VMEM(couplings.shape, f32),
            pltpu.VMEM((3,) + heat_level.shape, f32),
            pltpu.VMEM((steps, slots, planes + 2, 3, half + 2 * PAD, columns), f32),
            pltpu.VMEM((2, planes, 2, half, columns), f32),
            pltpu.VMEM((2, planes, half, columns), f32),
            pltpu.VMEM((planes, half, columns), f32),
            pltpu.VMEM((2, planes + 1, half, columns), f32),
            pltpu.VMEM((rows, columns), f32),
            pltpu.VMEM((rows, columns), f32),
            pltpu.VMEM((slots, 2, planes, 4, half, columns), f32),
            pltpu.VMEM((slots, 8, columns), f32),
            pltpu.VMEM((slots, 8, columns), f32),
            pltpu.VMEM((slots, planes, 3, half, columns), f32),
            pltpu.VMEM((slots, planes, 3, half, columns), f32),
            pltpu.VMEM((slots, planes, 4, half, columns), f32),
            pltpu.VMEM((2, columns), f32),
            pltpu.VMEM((count - 1, 2, columns), f32),
            pltpu.VMEM((2, columns), f32),
            pltpu.VMEM((slots, 2, columns), f32),
            pltpu.VMEM((slots, 8, columns), f32),
            dma((3,)),
            dma((planes,)),
            dma((5,)),
            dma,
            dma,
            dma((slots, CHUNKS + 1)),
            dma((2, slots, CHUNKS + 1)),
            dma((slots,)),
            dma((slots,)),
            dma((slots,)),
            dma((slots,)),
            dma((slots,)),
            dma((slots, planes)),
            dma,
            dma,
            dma((slots,)),
            dma((slots,)),
            pltpu.SemaphoreType.REGULAR((max(1, len(far_distances(count))),)),
        ],
        compiler_params=pltpu.CompilerParams(
            collective_id=0, has_side_effects=True, vmem_limit_bytes=56 * 1024 * 1024
        ),
        name="replica_step",
    )(
        spin_state,
        couplings,
        heat_level,
        heat_height,
        heat_angle,
        inverse_temps,
        colour_order,
        swap_bits,
    )
    return (spins, energies[0, :slots])


def solution(mesh):
    return jax.shard_map(
        on_device,
        mesh=mesh,
        in_specs=(
            P(("group", "temp"), None, "gz", None, None),
            P(None, ("group", "gz"), None, None),
            P(("group", "temp")),
            P(("group", "temp")),
            P(("group", "temp"), "gz", None, None),
            P(("group", "temp"), "gz", None, None),
            P(("group", "temp"), "gz", None, None),
            P(("group", "temp")),
        ),
        out_specs=(P(("group", "temp"), None, "gz", None, None), P(("group", "temp"))),
        check_vma=False,
    )
```

```python
import functools

import jax
import jax.numpy as jnp
from jax import lax
from jax.experimental import pallas as pl
from jax.experimental.pallas import tpu as pltpu
from jax.sharding import PartitionSpec as P

OR_SWEEPS = 2
OR_HALVES = 2 * OR_SWEEPS
HALVES = OR_HALVES + 2
PAD = 8
CHUNKS = 4
MESH = pl.DeviceIdType.MESH

SIN_TERMS = (
    1.0,
    -1.0 / 6,
    1.0 / 120,
    -1.0 / 5040,
    1.0 / 362880,
    -1.0 / 39916800,
    1.0 / 6227020800,
)
COS_TERMS = (
    1.0,
    -1.0 / 2,
    1.0 / 24,
    -1.0 / 720,
    1.0 / 40320,
    -1.0 / 3628800,
    1.0 / 479001600,
    -1.0 / 87178291200,
)


def series(terms, square):
    total = jnp.full_like(square, terms[-1])
    for term in terms[-2::-1]:
        total = total * square + term
    return total


def cos_sin(angle):
    half = 0.5 * angle
    square = half * half
    sine = half * series(SIN_TERMS, square)
    cosine = series(COS_TERMS, square)
    return 1.0 - 2.0 * sine * sine, 2.0 * sine * cosine


def far_distances(count):
    distances, known = [], 2
    while known < count // 2:
        distances.append(known)
        known *= 2
    return distances


def step_kernel(
    spin_hbm,
    bond_hbm,
    level_hbm,
    height_hbm,
    angle_hbm,
    beta_hbm,
    order_hbm,
    bits_hbm,
    out_ref,
    energy_ref,
    beta_ref,
    order_ref,
    bits_ref,
    spin_in,
    bond_in,
    heat_in,
    state,
    bond_x,
    bond_yo,
    bond_ys,
    bond_z,
    bond_halo,
    bond_top,
    trial,
    meta,
    meta_got,
    draws,
    draws_got,
    trial_got,
    share_sum,
    share_got,
    total_sum,
    total_got,
    gains,
    small_sem,
    spin_sem,
    load_sem,
    bond_send,
    bond_recv,
    send_sem,
    recv_sem,
    meta_send,
    meta_recv,
    draw_send,
    draw_recv,
    swap_send,
    swap_recv,
    share_send,
    share_recv,
    total_send,
    total_recv,
    far_sem,
):
    planes, rows, columns = spin_in.shape[2:]
    half = rows // 2
    piece = half // CHUNKS
    chunk = min(32, half)
    me = lax.axis_index("gz")
    count = lax.axis_size("gz")
    upper = lax.rem(me + 1, count)
    lower = lax.rem(me + count - 1, count)
    here_temp = lax.axis_index("temp")
    temps = lax.axis_size("temp")
    main = pl.ds(PAD, half)
    got = HALVES + 2
    distances = far_distances(count)

    def temp_towards(slot):
        return lax.rem(here_temp + 2 * slot - 1 + temps, temps)

    def has(slot):
        return (here_temp + slot > 0) & (here_temp + slot < temps)

    barrier = pltpu.get_barrier_semaphore()
    for neighbour in (lower, upper):
        pl.semaphore_signal(
            barrier, inc=1, device_id={"gz": neighbour}, device_id_type=MESH
        )
    for slot in (0, 1):

        @pl.when(has(slot))
        def _(slot=slot):
            pl.semaphore_signal(
                barrier, inc=1, device_id={"temp": temp_towards(slot)}, device_id_type=MESH
            )

    far_low = lax.rem(me, 2) == 0
    far_plane = jnp.where(far_low, 1, planes)
    near_plane = jnp.where(far_low, planes, 1)

    small = [
        pltpu.make_async_copy(source, target, small_sem.at[index])
        for index, (source, target) in enumerate(
            ((bits_hbm, bits_ref), (order_hbm, order_ref), (beta_hbm, beta_ref))
        )
    ]

    def spin_load(plane):
        return pltpu.make_async_copy(
            spin_hbm.at[:, :, plane - 1], spin_in.at[:, :, plane - 1], spin_sem.at[plane - 1]
        )

    loads = [
        pltpu.make_async_copy(bond_hbm, bond_in, load_sem.at[0]),
        pltpu.make_async_copy(level_hbm, heat_in.at[0], load_sem.at[1]),
        pltpu.make_async_copy(height_hbm, heat_in.at[1], load_sem.at[2]),
        pltpu.make_async_copy(angle_hbm, heat_in.at[2], load_sem.at[3]),
    ]
    for load in small:
        load.start()
    top_load = pltpu.make_async_copy(bond_hbm.at[2, planes - 1], bond_top, load_sem.at[4])
    top_load.start()
    plane_order = [far_plane, near_plane] + list(range(2, planes))
    for plane in plane_order:
        spin_load(plane).start()
    for load in loads:
        load.start()

    lane = lax.broadcasted_iota(jnp.int32, (half, columns), 1) % 2
    lane_chunk = lax.broadcasted_iota(jnp.int32, (chunk, columns), 1) % 2
    def lane_piece(size):
        return lax.broadcasted_iota(jnp.int32, (size, columns), 1) % 2

    for load in small:
        load.wait()
    swapped = bits_ref[0] != 0

    def order_of(slot):
        other = 1 - slot
        return jnp.where(swapped, order_ref[other], order_ref[slot])

    def beta_of(slot):
        other = 1 - slot
        return jnp.where(swapped, beta_ref[other], beta_ref[slot])

    def parity(slot, plane):
        return lax.rem(me * planes + plane + order_of(slot), 2)

    for slot in (0, 1):
        meta[slot, 0:1] = jnp.full((1, columns), beta_of(slot), jnp.float32)
        meta[slot, 1:2] = jnp.full((1, columns), order_of(slot), jnp.int32).astype(jnp.float32)
        meta[slot, 2:3] = jnp.full((1, columns), bits_ref[1], jnp.int32).astype(jnp.float32)

    def halo(step, slot, down, rows_at, part):
        return pltpu.make_async_remote_copy(
            src_ref=state.at[step, slot, jnp.where(down, 1, planes), :, rows_at],
            dst_ref=state.at[step, slot, jnp.where(down, planes + 1, 0), :, rows_at],
            send_sem=send_sem.at[slot, part],
            recv_sem=recv_sem.at[1 if isinstance(step, int) and step == got else lax.rem(step, 2), slot, part],
            device_id={"gz": jnp.where(down, lower, upper)},
            device_id_type=MESH,
        )

    def far_out(step, slot, part):
        return halo(step, slot, far_low, pl.ds(PAD + part * piece, piece), part)

    def far_in(step, slot, part):
        return halo(step, slot, ~far_low, pl.ds(PAD + part * piece, piece), part)

    def near_out(step, slot):
        return halo(step, slot, ~far_low, main, CHUNKS)

    def near_in(step, slot):
        return halo(step, slot, far_low, main, CHUNKS)

    bond_up = pltpu.make_async_remote_copy(
        src_ref=bond_top,
        dst_ref=bond_halo,
        send_sem=bond_send,
        recv_sem=bond_recv,
        device_id={"gz": upper},
        device_id_type=MESH,
    )

    def along_temp(source, target, send, recv, slot):
        return pltpu.make_async_remote_copy(
            src_ref=source,
            dst_ref=target,
            send_sem=send,
            recv_sem=recv,
            device_id={"temp": temp_towards(slot)},
            device_id_type=MESH,
        )

    def meta_copy(slot):
        return along_temp(
            meta.at[slot], meta_got.at[1 - slot], meta_send.at[slot], meta_recv.at[1 - slot], slot
        )

    def draw_copy(slot, plane):
        return along_temp(
            draws.at[slot, plane],
            draws_got.at[1 - slot, plane],
            draw_send.at[slot],
            draw_recv.at[1 - slot],
            slot,
        )

    def all_draws(slot):
        return along_temp(
            draws.at[slot], draws_got.at[1 - slot], draw_send.at[slot], draw_recv.at[1 - slot], slot
        )

    def swap_copy(slot, plane):
        return along_temp(
            state.at[HALVES, slot, plane, :, main],
            state.at[got, 1 - slot, plane, :, main],
            swap_send.at[slot],
            swap_recv.at[1 - slot, plane - 1],
            slot,
        )

    def all_swaps(slot):
        return along_temp(
            state.at[HALVES, slot, pl.ds(1, planes), :, main],
            state.at[got, 1 - slot, pl.ds(1, planes), :, main],
            swap_send.at[slot],
            swap_recv.at[0, 0],
            slot,
        )

    def total_copy(slot):
        return along_temp(
            total_sum, total_got.at[1 - slot], total_send.at[slot], total_recv.at[1 - slot], slot
        )

    def share_copy(distance):
        return pltpu.make_async_remote_copy(
            src_ref=share_sum,
            dst_ref=share_got.at[distance - 1],
            send_sem=share_send,
            recv_sem=share_recv,
            device_id={"gz": lax.rem(me + distance, count)},
            device_id_type=MESH,
        )

    all_shares = pltpu.make_async_remote_copy(
        src_ref=share_got,
        dst_ref=share_got,
        send_sem=share_send,
        recv_sem=share_recv,
        device_id={"gz": upper},
        device_id_type=MESH,
    )

    def far_signal(index):
        if index < len(distances):
            for move in (distances[index], count - distances[index]):
                pl.semaphore_signal(
                    far_sem.at[index],
                    inc=1,
                    device_id={"gz": lax.rem(me + move, count)},
                    device_id_type=MESH,
                )

    def far_wait(index):
        if index < len(distances):
            pl.semaphore_wait(far_sem.at[index], 2)

    even_rows = pl.ds(0, half, stride=2)
    odd_rows = pl.ds(1, half, stride=2)

    def wrap_rows(step, slot, plane):
        for part in range(3):
            state[step, slot, plane, part, PAD - 1 : PAD] = state[
                step, slot, plane, part, PAD + half - 1 : PAD + half
            ]
            state[step, slot, plane, part, PAD + half : PAD + half + 1] = state[
                step, slot, plane, part, PAD : PAD + 1
            ]

    def pack_spins(plane):
        for part in range(3):
            pairs = [
                (
                    spin_in[r, part, plane - 1, even_rows, :],
                    spin_in[r, part, plane - 1, odd_rows, :],
                )
                for r in (0, 1)
            ]
            for slot in (0, 1):
                even = jnp.where(swapped, pairs[1 - slot][0], pairs[slot][0])
                odd = jnp.where(swapped, pairs[1 - slot][1], pairs[slot][1])
                mask = lane == parity(slot, plane - 1)
                state[0, slot, plane, part, main] = jnp.where(mask, even, odd)
                state[1, slot, plane, part, main] = jnp.where(mask, odd, even)
        for slot in (0, 1):
            wrap_rows(1, slot, plane)

    def first_copy(slot, down, rows_at, part):
        return pltpu.make_async_remote_copy(
            src_ref=state.at[jnp.where(down, 1, 0), slot, jnp.where(down, 1, 0), :, rows_at],
            dst_ref=state.at[1, slot, jnp.where(down, planes + 1, 0), :, rows_at],
            send_sem=send_sem.at[slot, part],
            recv_sem=recv_sem.at[1, slot, part],
            device_id={"gz": jnp.where(down, lower, upper)},
            device_id_type=MESH,
        )

    def stage_products():
        even, odd = bond_top[even_rows, :], bond_top[odd_rows, :]
        for slot in (0, 1):
            bond = jnp.where(lane == parity(slot, planes - 1), odd, even)
            for part in range(3):
                state[0, slot, 0, part, main] = bond * state[1, slot, planes, part, main]

    pl.semaphore_wait(barrier, 2 + has(0).astype(jnp.int32) + has(1).astype(jnp.int32))
    top_load.wait()
    spin_load(far_plane).wait()
    pack_spins(far_plane)

    @pl.when(~far_low)
    def _():
        stage_products()

    for slot in (0, 1):
        for part in range(CHUNKS):
            first_copy(slot, far_low, pl.ds(PAD + part * piece, piece), part).start()
    spin_load(near_plane).wait()
    pack_spins(near_plane)

    @pl.when(far_low)
    def _():
        stage_products()

    for slot in (0, 1):
        first_copy(slot, ~far_low, main, CHUNKS).start()

        @pl.when(has(slot))
        def _(slot=slot):
            meta_copy(slot).start()

        @pl.when(~has(slot))
        def _(slot=slot):
            meta_got[slot] = jnp.zeros((8, columns), jnp.float32)

    bond_up.start()

    def pack_inner(plane, _):
        spin_load(plane).wait()
        pack_spins(plane)
        return 0

    lax.fori_loop(2, planes, pack_inner, 0)
    loads[0].wait()

    def pack_bonds(plane, _):
        even, odd = bond_in[0, plane, even_rows, :], bond_in[0, plane, odd_rows, :]
        first = jnp.where(lane == 0, even, odd)
        second = jnp.where(lane == 0, odd, even)
        bond_x[0, plane, 0] = first
        bond_x[1, plane, 0] = second
        bond_x[0, plane, 1] = pltpu.roll(second, 1, 1)
        bond_x[1, plane, 1] = pltpu.roll(first, 1, 1)
        even, odd = bond_in[1, plane, even_rows, :], bond_in[1, plane, odd_rows, :]
        before = pltpu.roll(odd, 1, 0)
        bond_ys[plane] = even
        bond_yo[0, plane] = jnp.where(lane == 0, before, odd)
        bond_yo[1, plane] = jnp.where(lane == 0, odd, before)
        even, odd = bond_in[2, plane, even_rows, :], bond_in[2, plane, odd_rows, :]
        bond_z[0, plane + 1] = jnp.where(lane == 0, even, odd)
        bond_z[1, plane + 1] = jnp.where(lane == 0, odd, even)
        return 0

    lax.fori_loop(0, planes, pack_bonds, 0)

    def pack_heat(slot, plane):
        side = 1 - slot
        mask = lane_chunk == parity(slot, plane)
        for start in range(0, half, chunk):
            here = pl.ds(start, chunk)
            even_here = pl.ds(2 * start, chunk, stride=2)
            odd_here = pl.ds(2 * start + 1, chunk, stride=2)
            packed = []
            for kind in range(3):
                even = jnp.where(
                    swapped,
                    heat_in[kind, side, plane, even_here, :],
                    heat_in[kind, slot, plane, even_here, :],
                )
                odd = jnp.where(
                    swapped,
                    heat_in[kind, side, plane, odd_here, :],
                    heat_in[kind, slot, plane, odd_here, :],
                )
                packed.append((jnp.where(mask, even, odd), jnp.where(mask, odd, even)))
                draws[slot, plane, kind, here] = packed[kind][1]
            for colour in (0, 1):
                level, height, angle = (draw[colour] for draw in packed)
                across = jnp.sqrt(jnp.maximum(1.0 - height * height, 0.0))
                cosine, sine = cos_sin(angle)
                trial[slot, colour, plane, 0, here] = level
                trial[slot, colour, plane, 1, here] = across * cosine
                trial[slot, colour, plane, 2, here] = across * sine
                trial[slot, colour, plane, 3, here] = height

    def bonds_of(pattern, plane, start, size=chunk):
        here = pl.ds(start, size)
        return (
            bond_x[pattern, plane - 1, 0, here],
            bond_x[pattern, plane - 1, 1, here],
            bond_ys[plane - 1, here],
            bond_yo[pattern, plane - 1, here],
            bond_z[pattern, plane, here],
            bond_z[pattern, plane - 1, here],
        )

    def pulls(step, slot, plane, bonds, mask, start, size=chunk):
        east, west, near, far, above, below = bonds
        at = pl.ds(PAD + start, size)
        out = []
        for part in range(3):
            centre = state[step, slot, plane, part, at]
            other = jnp.where(
                mask,
                state[step, slot, plane, part, pl.ds(PAD + start - 1, size)],
                state[step, slot, plane, part, pl.ds(PAD + start + 1, size)],
            )
            pulled = east * pltpu.roll(centre, columns - 1, 1) + west * pltpu.roll(centre, 1, 1)
            pulled = pulled + near * centre + far * other
            pulled = pulled + above * state[step, slot, plane + 1, part, at]
            pulled = pulled + below * state[step, slot, plane - 1, part, at]
            out.append(pulled)
        return out

    def dot(first, second):
        return first[0] * second[0] + first[1] * second[1] + first[2] * second[2]

    def colour_of(step, slot, plane):
        return lax.rem(parity(slot, plane - 1) + step + 1, 2)

    def relax_rows(step, slot, plane, start, size):
        pattern = colour_of(step, slot, plane)
        at = pl.ds(PAD + start, size)
        bonds = bonds_of(pattern, plane, start, size)
        pulled = pulls(step, slot, plane, bonds, lane_piece(size) == pattern, start, size)
        old = [state[step - 1, slot, plane, part, at] for part in range(3)]
        scale = 2.0 * dot(old, pulled) / jnp.maximum(dot(pulled, pulled), 0.01)
        for part in range(3):
            state[step + 1, slot, plane, part, at] = scale * pulled[part] - old[part]
        return 0

    def heated(pulled, beta, level, draw):
        square = jnp.maximum(dot(pulled, pulled), 0.01)
        inverse = lax.rsqrt(square)
        reach = beta * (square * inverse)
        axis = [part * inverse for part in pulled]
        cosine = 1.0 + jnp.log((1.0 - level) + level * jnp.exp(-2.0 * reach)) / reach
        along = dot(draw, axis)
        tangent = [draw[part] - along * axis[part] for part in range(3)]
        norm = lax.rsqrt(jnp.maximum(dot(tangent, tangent), 0.0001))
        side = jnp.sqrt(jnp.maximum(1.0 - cosine * cosine, 0.0)) * norm
        return [cosine * axis[part] + side * tangent[part] for part in range(3)]

    def heat_rows(step, slot, plane, start, size):
        colour = step - OR_HALVES - 1
        pattern = colour_of(step, slot, plane)
        at = pl.ds(PAD + start, size)
        here = pl.ds(start, size)
        bonds = bonds_of(pattern, plane, start, size)
        pulled = pulls(step, slot, plane, bonds, lane_piece(size) == pattern, start, size)
        level = trial[slot, colour, plane - 1, 0, here]
        draw = [trial[slot, colour, plane - 1, part, here] for part in (1, 2, 3)]
        fresh = heated(pulled, beta_of(slot), level, draw)
        for part in range(3):
            state[step + 1, slot, plane, part, at] = fresh[part]
        return jnp.sum(dot(fresh, pulled).reshape(-1, 8, columns), axis=0)

    def whole_plane(step, slot, plane, rows_of):
        total = 0
        for start in range(0, half, chunk):
            total = total + rows_of(step, slot, plane, start, chunk)
        wrap_rows(step + 1, slot, plane)
        return total

    def swap_start(slot, plane):
        @pl.when(has(slot))
        def _():
            swap_copy(slot, plane).start()

    def far_rows(step, slot, rows_of, send, swap):
        total = 0
        for part in range(CHUNKS):
            far_in(step, slot, part).wait_recv()
            total = total + rows_of(step, slot, far_plane, part * piece, piece)
            if send:
                far_out(step, slot, part).wait_send()
                far_out(step + 1, slot, part).start()
        wrap_rows(step + 1, slot, far_plane)
        if swap:
            swap_start(slot, far_plane)
        return total

    def near_rows(step, slot, rows_of, send, swap):
        near_in(step, slot).wait_recv()
        total = whole_plane(step, slot, near_plane, rows_of)
        if send:
            near_out(step, slot).wait_send()
            near_out(step + 1, slot).start()
        if swap:
            swap_start(slot, near_plane)
        return total

    def both(body):
        def visit(slot, _):
            body(slot)
            return 0

        lax.fori_loop(0, 2, visit, 0)

    def inner_planes(step, slot, rows_of, swap, initial):
        def visit(plane, total):
            total = total + whole_plane(step, slot, plane, rows_of)
            if swap:

                @pl.when(plane == 2)
                def _():
                    swap_start(slot, plane)

            return total

        return lax.fori_loop(2, planes, visit, initial)

    zero = jnp.zeros((8, columns), jnp.float32)

    def first_inner(slot, _):
        inner_planes(1, slot, relax_rows, False, 0)
        return 0

    lax.fori_loop(0, 2, first_inner, 0)
    for load in loads[1:]:
        load.wait()

    def fill(visit, _):
        slot = visit // planes
        plane = lax.rem(visit, planes)
        pack_heat(slot, plane)

        @pl.when(has(slot))
        def _():
            draw_copy(slot, plane).start()

        return 0

    lax.fori_loop(0, 2 * planes, fill, 0)
    bond_z[0, 0] = jnp.ones((half, columns), jnp.float32)
    bond_z[1, 0] = jnp.ones((half, columns), jnp.float32)

    def relax_round(step, _):
        both(lambda slot: far_rows(step, slot, relax_rows, True, False))
        both(lambda slot: near_rows(step, slot, relax_rows, True, False))

        @pl.when(step == 1)
        def _():
            far_signal(0)
            bond_up.wait_recv()
            even, odd = bond_halo[even_rows, :], bond_halo[odd_rows, :]
            bond_z[0, 0] = jnp.where(lane == 0, even, odd)
            bond_z[1, 0] = jnp.where(lane == 0, odd, even)

        @pl.when(step == 2)
        def _():
            far_wait(0)
            far_signal(1)

        both(lambda slot: inner_planes(step + 1, slot, relax_rows, False, 0))
        return 0

    lax.fori_loop(1, OR_HALVES, relax_round, 0)
    both(lambda slot: far_rows(OR_HALVES, slot, relax_rows, True, False))
    both(lambda slot: near_rows(OR_HALVES, slot, relax_rows, True, False))
    far_wait(1)
    far_signal(2)
    both(lambda slot: inner_planes(OR_HALVES + 1, slot, heat_rows, True, zero))

    both(lambda slot: far_rows(OR_HALVES + 1, slot, heat_rows, True, False))
    both(lambda slot: near_rows(OR_HALVES + 1, slot, heat_rows, True, False))
    both(lambda slot: swap_start(slot, far_plane))
    both(lambda slot: swap_start(slot, near_plane))

    def rest_of_swap(visit, _):
        swap_start(lax.rem(visit, 2), visit // 2 + 3)
        return 0

    lax.fori_loop(0, 2 * (planes - 3), rest_of_swap, 0)

    def inner_gain(slot):
        gains[slot] = inner_planes(OR_HALVES + 2, slot, heat_rows, False, zero)

    def far_gain(slot):
        gains[slot] = gains[slot] + far_rows(OR_HALVES + 2, slot, heat_rows, False, False)

    def near_gain(slot):
        gain = gains[slot] + near_rows(OR_HALVES + 2, slot, heat_rows, False, False)
        share_sum[pl.ds(slot, 1), :] = jnp.sum(gain, axis=0, keepdims=True)

    both(inner_gain)
    both(far_gain)
    both(near_gain)
    far_wait(2)

    def pass_far(slot):
        for part in range(CHUNKS):
            far_out(HALVES, slot, part).wait_send()

        @pl.when(has(slot))
        def _():
            swap_copy(1 - slot, far_plane).wait_recv()
            for part in range(CHUNKS):
                far_out(got, slot, part).start()
            wrap_rows(got, slot, far_plane)

    close = min(3, count // 2 - 1)
    sides = [side for step in range(1, close + 1) for side in (step, count - step)]
    sides.append(count // 2)
    for step in range(count // 2 - 1, close, -1):
        sides += [step, count - step]
    for distance in sides:
        share_copy(distance).start()

    def pass_near(slot, _):
        near_out(HALVES, slot).wait_send()

        @pl.when(has(slot))
        def _():
            swap_copy(1 - slot, near_plane).wait_recv()
            near_out(got, slot).start()
            wrap_rows(got, slot, near_plane)

        return 0

    pass_far(1)
    pass_far(0)
    lax.fori_loop(0, 2, pass_near, 0)
    for slot in (0, 1):

        @pl.when(has(slot))
        def _(slot=slot):
            all_draws(1 - slot).wait_recv()
            meta_copy(1 - slot).wait_recv()

    def prepare(visit, _):
        slot = visit // planes
        plane = lax.rem(visit, planes)
        for start in range(0, half, chunk):
            here = pl.ds(start, chunk)
            level, height, angle = (draws_got[slot, plane, kind, here] for kind in range(3))
            across = jnp.sqrt(jnp.maximum(1.0 - height * height, 0.0))
            cosine, sine = cos_sin(angle)
            trial_got[slot, plane, 0, here] = level
            trial_got[slot, plane, 1, here] = across * cosine
            trial_got[slot, plane, 2, here] = across * sine
            trial_got[slot, plane, 3, here] = height
        return 0

    lax.fori_loop(0, 2 * planes, prepare, 0)

    taking = [
        (meta_got[0, 2:3] > 0.5) & (here_temp > 0),
        jnp.full((1, columns), bits_ref[1], jnp.int32) * jnp.where(here_temp < temps - 1, 1, 0) > 0,
    ]

    def finish_plane(slot, plane):
        take = jnp.broadcast_to(taking[slot], (chunk, columns))
        flip = jnp.broadcast_to(meta_got[slot, 1:2] > 0.5, (chunk, columns))
        beta = meta_got[slot, 0:1]
        base = lax.rem(me * planes + plane - 1, 2)
        first_mask = (lane_chunk == base) ^ flip
        own_mask = lane_chunk == parity(slot, plane - 1)
        unpack_mask = jnp.where(take, first_mask.astype(jnp.int32), own_mask.astype(jnp.int32)) > 0
        for start in range(0, half, chunk):
            at = pl.ds(PAD + start, chunk)
            here = pl.ds(start, chunk)
            plain = bonds_of(1 - base, plane, start)
            other = bonds_of(base, plane, start)
            bonds = [jnp.where(flip, b, a) for a, b in zip(plain, other)]
            pulled = pulls(got, slot, plane, bonds, ~first_mask, start)
            level = trial_got[slot, plane - 1, 0, here]
            draw = [trial_got[slot, plane - 1, part, here] for part in (1, 2, 3)]
            fresh = heated(pulled, beta, level, draw)
            for part in range(3):
                first = jnp.where(
                    take, state[got, slot, plane, part, at], state[HALVES, slot, plane, part, at]
                )
                second = jnp.where(take, fresh[part], state[HALVES + 1, slot, plane, part, at])
                out_ref[slot, part, plane - 1, pl.ds(2 * start, chunk, stride=2), :] = jnp.where(
                    unpack_mask, first, second
                )
                out_ref[slot, part, plane - 1, pl.ds(2 * start + 1, chunk, stride=2), :] = jnp.where(
                    unpack_mask, second, first
                )

    all_shares.wait_recv()
    total_sum[...] = share_sum[...] + jnp.sum(share_got[...], axis=0)
    for slot in (0, 1):

        @pl.when(has(slot))
        def _(slot=slot):
            total_copy(slot).start()

    def arrive(visit, _):
        slot = visit // (planes - 2)
        plane = lax.rem(visit, planes - 2) + 2

        @pl.when(has(slot))
        def _():
            swap_copy(1 - slot, plane).wait_recv()
            wrap_rows(got, slot, plane)

        return 0

    lax.fori_loop(0, 2 * (planes - 2), arrive, 0)

    def finish_inner(plane, _):
        for slot in (0, 1):
            finish_plane(slot, plane)
        return 0

    lax.fori_loop(2, planes, finish_inner, 0)

    def finish_outer(index, _):
        for slot in (0, 1):

            @pl.when((index == 0) & has(slot))
            def _(slot=slot):
                near_in(got, slot).wait_recv()

            @pl.when((index == 1) & has(slot))
            def _(slot=slot):
                for part in range(CHUNKS):
                    far_in(got, slot, part).wait_recv()

        plane = jnp.where(index == 0, near_plane, far_plane)
        for slot in (0, 1):
            finish_plane(slot, plane)
        return 0

    lax.fori_loop(0, 2, finish_outer, 0)

    bond_up.wait_send()
    all_shares.wait_send()
    for slot in (0, 1):

        @pl.when(has(slot))
        def _(slot=slot):
            meta_copy(slot).wait_send()
            all_draws(slot).wait_send()
            all_swaps(slot).wait_send()
            for part in range(CHUNKS):
                far_out(got, slot, part).wait_send()
            near_out(got, slot).wait_send()

    for slot in (0, 1):

        @pl.when(has(slot))
        def _(slot=slot):
            total_copy(1 - slot).wait_recv()

    sites = float(columns * rows * planes * count)
    values = [
        jnp.where(taking[slot], total_got[slot, 1 - slot : 2 - slot], total_sum[slot : slot + 1])
        for slot in (0, 1)
    ]
    sums = [-jnp.sum(value, axis=1, keepdims=True) / sites for value in values]
    spot = lax.broadcasted_iota(jnp.int32, (1, columns), 1)
    energy_ref[...] = jnp.where(spot == 0, sums[0], sums[1])

    for slot in (0, 1):

        @pl.when(has(slot))
        def _(slot=slot):
            total_copy(slot).wait_send()


def on_device(
    spin_state,
    couplings,
    inverse_temps,
    colour_order,
    heat_level,
    heat_height,
    heat_angle,
    swap_bits,
):
    slots, parts, planes, rows, columns = spin_state.shape
    half = rows // 2
    count = lax.axis_size("gz")
    f32 = jnp.float32
    dma = pltpu.SemaphoreType.DMA
    any_space = pl.BlockSpec(memory_space=pl.ANY)
    vmem = pl.BlockSpec(memory_space=pltpu.VMEM)
    steps = HALVES + 3
    spins, energies = pl.pallas_call(
        step_kernel,
        out_shape=(
            pltpu.VMEM(spin_state.shape, f32),
            pltpu.VMEM((1, columns), f32),
        ),
        in_specs=[any_space] * 8,
        out_specs=(vmem, vmem),
        scratch_shapes=[
            pltpu.SMEM((slots,), f32),
            pltpu.SMEM((slots,), jnp.int32),
            pltpu.SMEM((slots,), jnp.int32),
            pltpu.VMEM(spin_state.shape, f32),
            pltpu.VMEM(couplings.shape, f32),
            pltpu.VMEM((3,) + heat_level.shape, f32),
            pltpu.VMEM((steps, slots, planes + 2, 3, half + 2 * PAD, columns), f32),
            pltpu.VMEM((2, planes, 2, half, columns), f32),
            pltpu.VMEM((2, planes, half, columns), f32),
            pltpu.VMEM((planes, half, columns), f32),
            pltpu.VMEM((2, planes + 1, half, columns), f32),
            pltpu.VMEM((rows, columns), f32),
            pltpu.VMEM((rows, columns), f32),
            pltpu.VMEM((slots, 2, planes, 4, half, columns), f32),
            pltpu.VMEM((slots, 8, columns), f32),
            pltpu.VMEM((slots, 8, columns), f32),
            pltpu.VMEM((slots, planes, 3, half, columns), f32),
            pltpu.VMEM((slots, planes, 3, half, columns), f32),
            pltpu.VMEM((slots, planes, 4, half, columns), f32),
            pltpu.VMEM((2, columns), f32),
            pltpu.VMEM((count - 1, 2, columns), f32),
            pltpu.VMEM((2, columns), f32),
            pltpu.VMEM((slots, 2, columns), f32),
            pltpu.VMEM((slots, 8, columns), f32),
            dma((3,)),
            dma((planes,)),
            dma((5,)),
            dma,
            dma,
            dma((slots, CHUNKS + 1)),
            dma((2, slots, CHUNKS + 1)),
            dma((slots,)),
            dma((slots,)),
            dma((slots,)),
            dma((slots,)),
            dma((slots,)),
            dma((slots, planes)),
            dma,
            dma,
            dma((slots,)),
            dma((slots,)),
            pltpu.SemaphoreType.REGULAR((max(1, len(far_distances(count))),)),
        ],
        compiler_params=pltpu.CompilerParams(
            collective_id=0, has_side_effects=True, vmem_limit_bytes=56 * 1024 * 1024
        ),
        name="replica_step",
    )(
        spin_state,
        couplings,
        heat_level,
        heat_height,
        heat_angle,
        inverse_temps,
        colour_order,
        swap_bits,
    )
    return (spins, energies[0, :slots])


def solution(mesh):
    return jax.shard_map(
        on_device,
        mesh=mesh,
        in_specs=(
            P(("group", "temp"), None, "gz", None, None),
            P(None, ("group", "gz"), None, None),
            P(("group", "temp")),
            P(("group", "temp")),
            P(("group", "temp"), "gz", None, None),
            P(("group", "temp"), "gz", None, None),
            P(("group", "temp"), "gz", None, None),
            P(("group", "temp")),
        ),
        out_specs=(P(("group", "temp"), None, "gz", None, None), P(("group", "temp"))),
        check_vma=False,
    )
```
